16 devices in a mesh: dp: 2 (over y, z), sp: 8 (over x, core).
Axes of the slice: x: 4, y: 2, z: 1, core: 2. Of those that a mesh axis runs over, the one named last changes fastest.
The devices are a block of a 4x4x8 slice.
Arguments:
- x_in: bfloat16 [16, 1024, 2048], P('dp', 'sp'), parts along dimension 0
- grad_y: bfloat16 [16, 1024, 2048], P('dp', 'sp'), parts along dimension 0
- positions: int32 [16, 1024], P('dp', 'sp'), parts along dimension 0
- g_norm: bfloat16 [2048], replicated
- w_query: bfloat16 [2048, 2048], replicated
- w_key: bfloat16 [2048, 2048], replicated
- w_value: bfloat16 [2048, 2048], replicated
- w_out: bfloat16 [2048, 2048], replicated
- g_query: bfloat16 [2048], replicated
- g_key: bfloat16 [2048], replicated
Outputs:
- output 1: bfloat16 [16, 1024, 2048], P('dp', 'sp'), parts along dimension 0
- output 2: bfloat16 [16, 1024, 2048], P('dp', 'sp'), parts along dimension 0
- output 3: float32 [4096], P(('dp', 'sp')), parts along dimension 0
- output 4: float32 [4096, 2048], P(('dp', 'sp')), parts along dimension 0
- output 5: float32 [4096, 2048], P(('dp', 'sp')), parts along dimension 0
- output 6: float32 [4096, 2048], P(('dp', 'sp')), parts along dimension 0
- output 7: float32 [4096, 2048], P(('dp', 'sp')), parts along dimension 0
- output 8: float32 [4096], P(('dp', 'sp')), parts along dimension 0
- output 9: float32 [4096], P(('dp', 'sp')), parts along dimension 0
There are 2 independent parts. The reference program is written for one: setup_inputs(seed, part) draws one part's arguments, and reference() takes and returns one part's arrays. A program takes and returns all parts, laid end to end along the dimension named above; an argument that names none is the same for every part.
All inputs are finite; a program needn't handle non-finite values.
Results may differ from the reference program's by a relative error of at most 0.0114602.
Values are sent between devices in bfloat16 or wider.
A program may use at most 768 MiB of HBM per device.

```python
import jax
import jax.numpy as jnp
from jax import lax

N_BATCH = 8
SEQ_LEN = 1024
D_MODEL = 2048
N_HEADS = 16
HEAD_DIM = 128
QUERY_BLOCK = min(128, SEQ_LEN)
NORM_EPS = 1e-5
ROPE_BASE = 10000.0
NEG_BIG = -1e30


def setup_inputs(seed: int = 0, part: int = 0) -> dict:
    part_key = jax.random.fold_in(jax.random.key(seed), part)
    key_x, key_dy, key_pos = jax.random.split(part_key, 3)
    weight_keys = jax.random.split(jax.random.key(seed + 1), 9)
    act_shape = (N_BATCH, SEQ_LEN, D_MODEL)
    x_in = jax.random.normal(key_x, act_shape, jnp.float32).astype(jnp.bfloat16)
    grad_y = jax.random.normal(key_dy, act_shape, jnp.float32).astype(jnp.bfloat16)
    tok_idx = jnp.arange(SEQ_LEN, dtype=jnp.int32)
    restart = jax.random.randint(key_pos, (N_BATCH, SEQ_LEN), 0, 256) == 0
    doc_start = lax.cummax(jnp.where(restart, tok_idx[None, :], 0), axis=1)
    positions = (tok_idx[None, :] - doc_start).astype(jnp.int32)
    fan_scale = D_MODEL ** -0.5
    head_q = jnp.repeat(jax.random.uniform(weight_keys[0], (N_HEADS,), jnp.float32, 0.5, 1.5), HEAD_DIM)
    head_k = jnp.repeat(jax.random.uniform(weight_keys[1], (N_HEADS,), jnp.float32, 0.5, 1.5), HEAD_DIM)
    w_shape = (D_MODEL, D_MODEL)
    w_query = (jax.random.normal(weight_keys[2], w_shape, jnp.float32) * fan_scale * head_q[None, :]).astype(jnp.bfloat16)
    w_key = (jax.random.normal(weight_keys[3], w_shape, jnp.float32) * fan_scale * head_k[None, :]).astype(jnp.bfloat16)
    w_value = (jax.random.normal(weight_keys[4], w_shape, jnp.float32) * fan_scale).astype(jnp.bfloat16)
    w_out = (jax.random.normal(weight_keys[5], w_shape, jnp.float32) * fan_scale).astype(jnp.bfloat16)
    g_norm = (1.0 + 0.3 * jax.random.normal(weight_keys[6], (D_MODEL,), jnp.float32)).astype(jnp.bfloat16)
    g_query = (1.7 + 0.4 * jax.random.normal(weight_keys[7], (D_MODEL,), jnp.float32)).astype(jnp.bfloat16)
    g_key = (1.7 + 0.4 * jax.random.normal(weight_keys[8], (D_MODEL,), jnp.float32)).astype(jnp.bfloat16)
    return {'x_in': x_in, 'grad_y': grad_y, 'positions': positions, 'g_norm': g_norm, 'w_query': w_query, 'w_key': w_key, 'w_value': w_value, 'w_out': w_out, 'g_query': g_query, 'g_key': g_key}


def rms_scale(values, gain_vec):
    inv_rms = lax.rsqrt(jnp.mean(values * values, axis=-1, keepdims=True) + NORM_EPS)
    return values * inv_rms * gain_vec


def rope_tables(positions):
    half_dim = HEAD_DIM // 2
    inv_freq = ROPE_BASE ** (-jnp.arange(half_dim, dtype=jnp.float32) * (2.0 / HEAD_DIM))
    angles = positions.astype(jnp.float32)[..., None] * inv_freq
    return jnp.cos(angles)[:, :, None, :], jnp.sin(angles)[:, :, None, :]


def rope_apply(values, cos_t, sin_t):
    half_dim = values.shape[-1] // 2
    first_half = values[..., :half_dim]
    second_half = values[..., half_dim:]
    return jnp.concatenate([first_half * cos_t - second_half * sin_t, second_half * cos_t + first_half * sin_t], axis=-1)


def mat_f32(left_op, right_op):
    return jnp.dot(left_op, right_op, precision=lax.Precision.HIGHEST)


def causal_attention(q_bf, k_bf, v_bf):
    q_f = q_bf.astype(jnp.float32)
    k_f = k_bf.astype(jnp.float32)
    v_f = v_bf.astype(jnp.float32)
    key_pos = jnp.arange(SEQ_LEN)
    qk_scale = HEAD_DIM ** -0.5

    def one_block(q_start):
        q_blk = lax.dynamic_slice_in_dim(q_f, q_start, QUERY_BLOCK, axis=1)
        scores = jnp.einsum('bqhd,bkhd->bhqk', q_blk, k_f, precision=lax.Precision.HIGHEST) * qk_scale
        q_pos = q_start + jnp.arange(QUERY_BLOCK)
        scores = jnp.where(q_pos[:, None] >= key_pos[None, :], scores, NEG_BIG)
        prob_f = jax.nn.softmax(scores, axis=-1)
        return jnp.einsum('bhqk,bkhd->bqhd', prob_f, v_f, precision=lax.Precision.HIGHEST)

    starts = jnp.arange(SEQ_LEN // QUERY_BLOCK) * QUERY_BLOCK
    blocks = lax.map(jax.checkpoint(one_block), starts)
    merged = jnp.moveaxis(blocks, 0, 1).reshape(q_bf.shape)
    return merged.astype(jnp.bfloat16)


def reference(x_in, grad_y, positions, g_norm, w_query, w_key, w_value, w_out, g_query, g_key):
    cos_t, sin_t = rope_tables(positions)
    head_shape = (N_BATCH, SEQ_LEN, N_HEADS, HEAD_DIM)
    flat_shape = (N_BATCH, SEQ_LEN, D_MODEL)

    def forward(x_f, gain_n, wq_f, wk_f, wv_f, wo_f, gain_q, gain_k):
        hidden = rms_scale(x_f, gain_n).astype(jnp.bfloat16).astype(jnp.float32)
        q_raw = mat_f32(hidden, wq_f)
        k_raw = mat_f32(hidden, wk_f)
        v_val = mat_f32(hidden, wv_f).astype(jnp.bfloat16)
        q_rot = rope_apply(rms_scale(q_raw, gain_q).reshape(head_shape), cos_t, sin_t).astype(jnp.bfloat16)
        k_rot = rope_apply(rms_scale(k_raw, gain_k).reshape(head_shape), cos_t, sin_t).astype(jnp.bfloat16)
        attended = causal_attention(q_rot, k_rot, v_val.reshape(head_shape))
        o_proj = mat_f32(attended.reshape(flat_shape).astype(jnp.float32), wo_f)
        return (x_f + o_proj).astype(jnp.bfloat16)

    y_out, pullback = jax.vjp(forward, x_in.astype(jnp.float32), g_norm.astype(jnp.float32), w_query.astype(jnp.float32), w_key.astype(jnp.float32), w_value.astype(jnp.float32), w_out.astype(jnp.float32), g_query.astype(jnp.float32), g_key.astype(jnp.float32))
    cotangents = pullback(grad_y)
    return (y_out, cotangents[0].astype(jnp.bfloat16), cotangents[1], cotangents[2], cotangents[3], cotangents[4], cotangents[5], cotangents[6], cotangents[7])
```

```python
import functools
import math
import jax
import jax.numpy as jnp
from jax import lax
from jax.experimental import pallas as pl
from jax.experimental.pallas import tpu as pltpu
from jax.sharding import PartitionSpec as P

HEAD_DIM = 128
NORM_EPS = 1e-5
ROPE_BASE = 10000.0
NEG_BIG = -1e30
LOG2E = math.log2(math.e)
Q_BLOCK = 256


def rope_tables(positions):
    half_dim = HEAD_DIM // 2
    inv_freq = ROPE_BASE ** (-jnp.arange(half_dim, dtype=jnp.float32) * (2.0 / HEAD_DIM))
    angles = positions.astype(jnp.float32)[..., None] * inv_freq
    return jnp.cos(angles)[:, None, :], jnp.sin(angles)[:, None, :]


def rope_apply(values, cos_t, sin_t):
    half_dim = values.shape[-1] // 2
    first_half = values[..., :half_dim]
    second_half = values[..., half_dim:]
    return jnp.concatenate([first_half * cos_t - second_half * sin_t, second_half * cos_t + first_half * sin_t], axis=-1)


def rope_revert(grads_in, cos_t, sin_t):
    half_dim = grads_in.shape[-1] // 2
    first_half = grads_in[..., :half_dim]
    second_half = grads_in[..., half_dim:]
    return jnp.concatenate([first_half * cos_t + second_half * sin_t, second_half * cos_t - first_half * sin_t], axis=-1)


def rms_forward(values, gain_vec):
    inv_rms = lax.rsqrt(jnp.mean(values * values, axis=-1, keepdims=True) + NORM_EPS)
    normed = values * inv_rms
    return normed * gain_vec.astype(jnp.float32), normed, inv_rms


def rms_backward(d_out, normed, inv_rms, gain_vec):
    d_normed = d_out * gain_vec.astype(jnp.float32)
    d_in = inv_rms * (d_normed - normed * jnp.mean(d_normed * normed, axis=-1, keepdims=True))
    return d_in, d_out * normed


def dot_nn(a, b):
    return lax.dot_general(a, b, (((1,), (0,)), ((), ())), preferred_element_type=jnp.float32)


def dot_nt(a, b):
    return lax.dot_general(a, b, (((1,), (1,)), ((), ())), preferred_element_type=jnp.float32)


def dot_tn(a, b):
    return lax.dot_general(a, b, (((0,), (0,)), ((), ())), preferred_element_type=jnp.float32)


def attn_fwd_kernel(seq_len, q_ref, k_ref, v_ref, o_ref, lse_ref):
    scale2 = LOG2E * HEAD_DIM ** -0.5
    for start in range(0, seq_len, Q_BLOCK):
        stop = start + Q_BLOCK
        q_blk = q_ref[start:stop, :]
        s_diag = dot_nt(k_ref[start:stop, :], q_blk)
        key_i = lax.broadcasted_iota(jnp.int32, s_diag.shape, 0)
        qry_i = lax.broadcasted_iota(jnp.int32, s_diag.shape, 1)
        s_diag = jnp.where(key_i <= qry_i, s_diag, NEG_BIG)
        m = jnp.max(s_diag, axis=0, keepdims=True)
        if start:
            s_past = dot_nt(k_ref[0:start, :], q_blk)
            m = jnp.maximum(m, jnp.max(s_past, axis=0, keepdims=True))
        m2 = m * scale2
        p_diag = jnp.exp2(s_diag * scale2 - m2)
        l = jnp.sum(p_diag, axis=0, keepdims=True)
        acc = dot_tn(v_ref[start:stop, :], p_diag.astype(jnp.bfloat16))
        if start:
            p_past = jnp.exp2(s_past * scale2 - m2)
            l = l + jnp.sum(p_past, axis=0, keepdims=True)
            acc = acc + dot_tn(v_ref[0:start, :], p_past.astype(jnp.bfloat16))
        o_ref[start:stop, :] = (acc / l).T.astype(o_ref.dtype)
        lse_ref[0, :, start:stop] = m2 + jnp.log2(l)


def attn_bwd_kernel(seq_len, q_ref, k_ref, v_ref, do_ref, lse_ref, dq_ref, dk_ref, dv_ref, dk_acc, dv_acc):
    scale = HEAD_DIM ** -0.5
    scale2 = LOG2E * scale
    dk_acc[...] = jnp.zeros_like(dk_acc)
    dv_acc[...] = jnp.zeros_like(dv_acc)
    for start in range(0, seq_len, Q_BLOCK):
        stop = start + Q_BLOCK
        q_blk = q_ref[start:stop, :]
        do_blk = do_ref[start:stop, :]
        lse = lse_ref[0, :, start:stop]
        k_all = k_ref[0:stop, :]
        s = dot_nt(k_all, q_blk)
        p = jnp.exp2(s * scale2 - lse)
        key_i = lax.broadcasted_iota(jnp.int32, (Q_BLOCK, Q_BLOCK), 0)
        qry_i = lax.broadcasted_iota(jnp.int32, (Q_BLOCK, Q_BLOCK), 1)
        p_diag = jnp.where(key_i <= qry_i, p[start:stop, :], 0.0)
        p = jnp.concatenate([p[0:start, :], p_diag], axis=0) if start else p_diag
        dp = dot_nt(v_ref[0:stop, :], do_blk)
        delta = jnp.sum(p * dp, axis=0, keepdims=True)
        ds = (p * (dp - delta) * scale).astype(jnp.bfloat16)
        dv_acc[0:stop, :] += dot_nn(p.astype(jnp.bfloat16), do_blk)
        dk_acc[0:stop, :] += dot_nn(ds, q_blk)
        dq_ref[start:stop, :] = dot_tn(k_all, ds).T.astype(dq_ref.dtype)
    dk_ref[...] = dk_acc[...].astype(dk_ref.dtype)
    dv_ref[...] = dv_acc[...].astype(dv_ref.dtype)


def attend_forward(q, k, v):
    seq_len, d_model = q.shape
    n_heads = d_model // HEAD_DIM
    head_spec = pl.BlockSpec((seq_len, HEAD_DIM), lambda h: (0, h))
    flops = 2 * 2 * seq_len * seq_len * d_model
    return pl.pallas_call(
        functools.partial(attn_fwd_kernel, seq_len),
        grid=(n_heads,),
        out_shape=(jax.ShapeDtypeStruct(q.shape, jnp.bfloat16), jax.ShapeDtypeStruct((n_heads, 1, seq_len), jnp.float32)),
        in_specs=[head_spec] * 3,
        out_specs=(head_spec, pl.BlockSpec((1, 1, seq_len), lambda h: (h, 0, 0))),
        cost_estimate=pl.CostEstimate(flops=flops, bytes_accessed=4 * q.size * 2, transcendentals=seq_len * seq_len * n_heads),
        name="attn_fwd",
    )(q, k, v)


def attend_backward(q, k, v, d_out, lse):
    seq_len, d_model = q.shape
    n_heads = d_model // HEAD_DIM
    head_spec = pl.BlockSpec((seq_len, HEAD_DIM), lambda h: (0, h))
    flops = 5 * 2 * seq_len * seq_len * d_model
    return pl.pallas_call(
        functools.partial(attn_bwd_kernel, seq_len),
        grid=(n_heads,),
        out_shape=(jax.ShapeDtypeStruct(q.shape, jnp.bfloat16),) * 3,
        in_specs=[head_spec] * 4 + [pl.BlockSpec((1, 1, seq_len), lambda h: (h, 0, 0))],
        out_specs=(head_spec,) * 3,
        scratch_shapes=[pltpu.VMEM((seq_len, HEAD_DIM), jnp.float32)] * 2,
        cost_estimate=pl.CostEstimate(flops=flops, bytes_accessed=7 * q.size * 2, transcendentals=seq_len * seq_len * n_heads),
        name="attn_bwd",
    )(q, k, v, d_out, lse)


def solution(mesh):
    to_seqs = functools.partial(lax.all_to_all, axis_name='sp', split_axis=0, concat_axis=1, tiled=True)
    to_tokens = functools.partial(lax.all_to_all, axis_name='sp', split_axis=1, concat_axis=0, tiled=True)

    def sum_rows(partial_sum):
        return lax.psum_scatter(partial_sum, 'sp', scatter_dimension=0, tiled=True)

    def device_step(x_loc, gy_loc, pos_loc, g_norm, w_query, w_key, w_value, w_out, g_query, g_key):
        d_model = x_loc.shape[-1]
        x_seq = to_seqs(x_loc)
        pos_seq = to_seqs(pos_loc)
        gy_seq = to_seqs(gy_loc)
        n_seq, seq_len = pos_seq.shape
        rows = n_seq * seq_len
        cos_t, sin_t = rope_tables(pos_seq.reshape(rows))
        x_bf = x_seq.reshape(rows, d_model)
        gy = gy_seq.reshape(rows, d_model)
        heads = (rows, d_model // HEAD_DIM, HEAD_DIM)

        hid_f, x_hat, x_inv = rms_forward(x_bf.astype(jnp.float32), g_norm)
        hidden = hid_f.astype(jnp.bfloat16)
        q_nrm, q_hat, q_inv = rms_forward(dot_nn(hidden, w_query), g_query)
        k_nrm, k_hat, k_inv = rms_forward(dot_nn(hidden, w_key), g_key)
        q_rot = rope_apply(q_nrm.reshape(heads), cos_t, sin_t).astype(jnp.bfloat16).reshape(rows, d_model)
        k_rot = rope_apply(k_nrm.reshape(heads), cos_t, sin_t).astype(jnp.bfloat16).reshape(rows, d_model)
        v_val = dot_nn(hidden, w_value).astype(jnp.bfloat16)

        outs = [attend_forward(q_rot[i:i + seq_len], k_rot[i:i + seq_len], v_val[i:i + seq_len]) for i in range(0, rows, seq_len)]
        attended = outs[0][0] if n_seq == 1 else jnp.concatenate([o[0] for o in outs])
        grad_wo = sum_rows(dot_tn(attended, gy))
        y_seq = (x_bf.astype(jnp.float32) + dot_nn(attended, w_out)).astype(jnp.bfloat16)
        y_out = to_tokens(y_seq.reshape(n_seq, seq_len, d_model))
        d_attn = dot_nt(gy, w_out).astype(jnp.bfloat16)

        bwd = [attend_backward(q_rot[i:i + seq_len], k_rot[i:i + seq_len], v_val[i:i + seq_len], d_attn[i:i + seq_len], outs[i // seq_len][1]) for i in range(0, rows, seq_len)]
        d_q, d_k, d_v = bwd[0] if n_seq == 1 else [jnp.concatenate([b[j] for b in bwd]) for j in range(3)]

        dq_rot = rope_revert(d_q.astype(jnp.float32).reshape(heads), cos_t, sin_t).reshape(rows, d_model)
        dk_rot = rope_revert(d_k.astype(jnp.float32).reshape(heads), cos_t, sin_t).reshape(rows, d_model)
        dq_raw, q_terms = rms_backward(dq_rot, q_hat, q_inv, g_query)
        dk_raw, k_terms = rms_backward(dk_rot, k_hat, k_inv, g_key)
        dq_bf = dq_raw.astype(jnp.bfloat16)
        dk_bf = dk_raw.astype(jnp.bfloat16)
        grad_wv = sum_rows(dot_tn(hidden, d_v))
        grad_wk = sum_rows(dot_tn(hidden, dk_bf))
        grad_wq = sum_rows(dot_tn(hidden, dq_bf))
        d_hidden = dot_nt(dq_bf, w_query) + dot_nt(dk_bf, w_key) + dot_nt(d_v, w_value)
        d_hidden = d_hidden.astype(jnp.bfloat16).astype(jnp.float32)
        dx_norm, n_terms = rms_backward(d_hidden, x_hat, x_inv, g_norm)
        gx_seq = (gy.astype(jnp.float32) + dx_norm).astype(jnp.bfloat16)
        grad_x = to_tokens(gx_seq.reshape(n_seq, seq_len, d_model))
        gains = [sum_rows(jnp.sum(t, axis=0)) for t in (n_terms, q_terms, k_terms)]
        return y_out, grad_x, gains[0], grad_wq, grad_wk, grad_wv, grad_wo, gains[1], gains[2]

    seq_spec = P('dp', 'sp', None)
    mat_rep = P(None, None)
    vec_rep = P(None)
    row_spec = P(('dp', 'sp'), None)
    vec_spec = P(('dp', 'sp'))
    return jax.shard_map(device_step, mesh=mesh, in_specs=(seq_spec, seq_spec, P('dp', 'sp'), vec_rep, mat_rep, mat_rep, mat_rep, mat_rep, vec_rep, vec_rep), out_specs=(seq_spec, seq_spec, vec_spec, row_spec, row_spec, row_spec, row_spec, vec_spec, vec_spec), check_vma=False)
```

```python
import functools
import math
import jax
import jax.numpy as jnp
from jax import lax
from jax.experimental import pallas as pl
from jax.experimental.pallas import tpu as pltpu
from jax.sharding import PartitionSpec as P

HEAD_DIM = 128
NORM_EPS = 1e-5
ROPE_BASE = 10000.0
NEG_BIG = -1e30
LOG2E = math.log2(math.e)
Q_BLOCK = 256


def rope_tables(positions):
    half_dim = HEAD_DIM // 2
    inv_freq = ROPE_BASE ** (-jnp.arange(half_dim, dtype=jnp.float32) * (2.0 / HEAD_DIM))
    angles = positions.astype(jnp.float32)[:, None] * inv_freq
    cos_h, sin_h = jnp.cos(angles), jnp.sin(angles)
    return jnp.concatenate([cos_h, cos_h], axis=1), jnp.concatenate([-sin_h, sin_h], axis=1)


def dot_nn(a, b):
    return lax.dot_general(a, b, (((1,), (0,)), ((), ())), preferred_element_type=jnp.float32)


def dot_nt(a, b):
    return lax.dot_general(a, b, (((1,), (1,)), ((), ())), preferred_element_type=jnp.float32)


def dot_tn(a, b):
    return lax.dot_general(a, b, (((0,), (0,)), ((), ())), preferred_element_type=jnp.float32)


def attn_fwd_kernel(seq_len, q_ref, k_ref, v_ref, o_ref, lse_ref):
    scale2 = LOG2E * HEAD_DIM ** -0.5
    for start in range(0, seq_len, Q_BLOCK):
        stop = start + Q_BLOCK
        q_blk = q_ref[start:stop, :]
        s_diag = dot_nt(k_ref[start:stop, :], q_blk)
        key_i = lax.broadcasted_iota(jnp.int32, s_diag.shape, 0)
        qry_i = lax.broadcasted_iota(jnp.int32, s_diag.shape, 1)
        s_diag = jnp.where(key_i <= qry_i, s_diag, NEG_BIG)
        m = jnp.max(s_diag, axis=0, keepdims=True)
        if start:
            s_past = dot_nt(k_ref[0:start, :], q_blk)
            m = jnp.maximum(m, jnp.max(s_past, axis=0, keepdims=True))
        m2 = m * scale2
        p_diag = jnp.exp2(s_diag * scale2 - m2)
        l = jnp.sum(p_diag, axis=0, keepdims=True)
        acc = dot_tn(v_ref[start:stop, :], p_diag.astype(jnp.bfloat16))
        if start:
            p_past = jnp.exp2(s_past * scale2 - m2)
            l = l + jnp.sum(p_past, axis=0, keepdims=True)
            acc = acc + dot_tn(v_ref[0:start, :], p_past.astype(jnp.bfloat16))
        o_ref[start:stop, :] = (acc / l).T.astype(o_ref.dtype)
        lse_ref[0, :, start:stop] = m2 + jnp.log2(l)


def attn_bwd_kernel(seq_len, q_ref, k_ref, v_ref, do_ref, lse_ref, dq_ref, dk_ref, dv_ref, dk_acc, dv_acc):
    scale = HEAD_DIM ** -0.5
    scale2 = LOG2E * scale
    dk_acc[...] = jnp.zeros_like(dk_acc)
    dv_acc[...] = jnp.zeros_like(dv_acc)
    for start in range(0, seq_len, Q_BLOCK):
        stop = start + Q_BLOCK
        q_blk = q_ref[start:stop, :]
        do_blk = do_ref[start:stop, :]
        lse = lse_ref[0, :, start:stop]
        k_all = k_ref[0:stop, :]
        s = dot_nt(k_all, q_blk)
        p = jnp.exp2(s * scale2 - lse)
        key_i = lax.broadcasted_iota(jnp.int32, (Q_BLOCK, Q_BLOCK), 0)
        qry_i = lax.broadcasted_iota(jnp.int32, (Q_BLOCK, Q_BLOCK), 1)
        p_diag = jnp.where(key_i <= qry_i, p[start:stop, :], 0.0)
        p = jnp.concatenate([p[0:start, :], p_diag], axis=0) if start else p_diag
        dp = dot_nt(v_ref[0:stop, :], do_blk)
        delta = jnp.sum(p * dp, axis=0, keepdims=True)
        ds = (p * (dp - delta) * scale).astype(jnp.bfloat16)
        dv_acc[0:stop, :] += dot_nn(p.astype(jnp.bfloat16), do_blk)
        dk_acc[0:stop, :] += dot_nn(ds, q_blk)
        dq_ref[start:stop, :] = dot_tn(k_all, ds).T.astype(dq_ref.dtype)
    dk_ref[...] = dk_acc[...].astype(dk_ref.dtype)
    dv_ref[...] = dv_acc[...].astype(dv_ref.dtype)


def attend_forward(q, k, v):
    seq_len, d_model = q.shape
    n_heads = d_model // HEAD_DIM
    head_spec = pl.BlockSpec((seq_len, HEAD_DIM), lambda h: (0, h))
    flops = 2 * 2 * seq_len * seq_len * d_model
    return pl.pallas_call(
        functools.partial(attn_fwd_kernel, seq_len),
        grid=(n_heads,),
        out_shape=(jax.ShapeDtypeStruct(q.shape, jnp.bfloat16), jax.ShapeDtypeStruct((n_heads, 1, seq_len), jnp.float32)),
        in_specs=[head_spec] * 3,
        out_specs=(head_spec, pl.BlockSpec((1, 1, seq_len), lambda h: (h, 0, 0))),
        cost_estimate=pl.CostEstimate(flops=flops, bytes_accessed=4 * q.size * 2, transcendentals=seq_len * seq_len * n_heads),
        name="attn_fwd",
    )(q, k, v)


def attend_backward(q, k, v, d_out, lse):
    seq_len, d_model = q.shape
    n_heads = d_model // HEAD_DIM
    head_spec = pl.BlockSpec((seq_len, HEAD_DIM), lambda h: (0, h))
    flops = 5 * 2 * seq_len * seq_len * d_model
    return pl.pallas_call(
        functools.partial(attn_bwd_kernel, seq_len),
        grid=(n_heads,),
        out_shape=(jax.ShapeDtypeStruct(q.shape, jnp.bfloat16),) * 3,
        in_specs=[head_spec] * 4 + [pl.BlockSpec((1, 1, seq_len), lambda h: (h, 0, 0))],
        out_specs=(head_spec,) * 3,
        scratch_shapes=[pltpu.VMEM((seq_len, HEAD_DIM), jnp.float32)] * 2,
        cost_estimate=pl.CostEstimate(flops=flops, bytes_accessed=7 * q.size * 2, transcendentals=seq_len * seq_len * n_heads),
        name="attn_bwd",
    )(q, k, v, d_out, lse)


MESH = pl.DeviceIdType.MESH
ROW_BLOCK = 256


def row_inv(values):
    return lax.rsqrt(jnp.mean(values * values, axis=-1, keepdims=True) + NORM_EPS)


def qkv_kernel(x_ref, cos_ref, sin_ref, gn_ref, gq_ref, gk_ref, wq_ref, wk_ref, wv_ref,
               q_ref, k_ref, v_ref, ht_ref, q1_ref, k1_ref):
    x_f = x_ref[...].astype(jnp.float32)
    hidden_f = x_f * row_inv(x_f) * gn_ref[...].astype(jnp.float32)
    hidden = hidden_f.astype(jnp.bfloat16)
    ht_ref[...] = hidden.T
    v_ref[...] = dot_nn(hidden, wv_ref[...]).astype(jnp.bfloat16)
    cos_t, sin_t = cos_ref[...], sin_ref[...]
    for w_ref, g_ref, raw_ref, out_ref in ((wq_ref, gq_ref, q1_ref, q_ref), (wk_ref, gk_ref, k1_ref, k_ref)):
        raw_ref[...] = dot_nn(hidden, w_ref[...])
        raw = raw_ref[...]
        inv = row_inv(raw)
        for at in range(0, raw.shape[1], HEAD_DIM):
            u = raw_ref[:, at:at + HEAD_DIM] * inv * g_ref[:, at:at + HEAD_DIM].astype(jnp.float32)
            out_ref[:, at:at + HEAD_DIM] = (u * cos_t + pltpu.roll(u, HEAD_DIM // 2, 1) * sin_t).astype(jnp.bfloat16)


def project_qkv(x_bf, cos_t, sin_t, g_norm, g_query, g_key, w_query, w_key, w_value):
    rows, d_model = x_bf.shape
    blk = ROW_BLOCK
    row_spec = pl.BlockSpec((blk, d_model), lambda i: (i, 0))
    tab_spec = pl.BlockSpec((blk, HEAD_DIM), lambda i: (i, 0))
    vec_spec = pl.BlockSpec((1, d_model), lambda i: (0, 0))
    mat_spec = pl.BlockSpec((d_model, d_model), lambda i: (0, 0), pipeline_mode=pl.Buffered(1))
    act = jax.ShapeDtypeStruct((rows, d_model), jnp.bfloat16)
    raw = jax.ShapeDtypeStruct((rows, d_model), jnp.float32)
    return pl.pallas_call(
        qkv_kernel,
        grid=(rows // blk,),
        out_shape=(act, act, act, jax.ShapeDtypeStruct((d_model, rows), jnp.bfloat16), raw, raw),
        in_specs=[row_spec, tab_spec, tab_spec, vec_spec, vec_spec, vec_spec, mat_spec, mat_spec, mat_spec],
        out_specs=(row_spec, row_spec, row_spec, pl.BlockSpec((d_model, blk), lambda i: (0, i)), row_spec, row_spec),
        compiler_params=pltpu.CompilerParams(vmem_limit_bytes=62 * 1024 * 1024),
        cost_estimate=pl.CostEstimate(flops=6 * rows * d_model * d_model, bytes_accessed=60 * 1024 * 1024, transcendentals=0),
        name="qkv_proj",
    )(x_bf, cos_t, sin_t, g_norm[None], g_query[None], g_key[None], w_query, w_key, w_value)


def norm_back_kernel(dq_ref, dk_ref, q1_ref, k1_ref, cos_ref, sin_ref, gq_ref, gk_ref,
                     oq_ref, ok_ref, tq_ref, tk_ref, tmp_ref, nrm_ref):
    cos_t, sin_t = cos_ref[...], sin_ref[...]
    for d_ref, raw_ref, g_ref, out_ref, t_ref in ((dq_ref, q1_ref, gq_ref, oq_ref, tq_ref), (dk_ref, k1_ref, gk_ref, ok_ref, tk_ref)):
        raw = raw_ref[...]
        inv = row_inv(raw)
        total = jnp.zeros((raw.shape[0], HEAD_DIM), jnp.float32)
        for at in range(0, raw.shape[1], HEAD_DIM):
            d_u = d_ref[:, at:at + HEAD_DIM].astype(jnp.float32)
            d_n = d_u * cos_t - pltpu.roll(d_u, HEAD_DIM // 2, 1) * sin_t
            hat = raw_ref[:, at:at + HEAD_DIM] * inv
            terms = jnp.sum(d_n * hat, axis=0, keepdims=True)

            @pl.when(pl.program_id(0) == 0)
            def _():
                t_ref[:, at:at + HEAD_DIM] = terms

            @pl.when(pl.program_id(0) > 0)
            def _():
                t_ref[:, at:at + HEAD_DIM] += terms

            d_n = d_n * g_ref[:, at:at + HEAD_DIM].astype(jnp.float32)
            total = total + d_n * hat
            tmp_ref[:, at:at + HEAD_DIM] = d_n
            nrm_ref[:, at:at + HEAD_DIM] = hat
        mean = jnp.sum(total, axis=-1, keepdims=True) * (1.0 / raw.shape[1])
        out_ref[...] = (inv * (tmp_ref[...] - nrm_ref[...] * mean)).astype(jnp.bfloat16)


def norm_back(d_q, d_k, q1, k1, cos_t, sin_t, g_query, g_key):
    rows, d_model = d_q.shape
    blk = ROW_BLOCK
    row_spec = pl.BlockSpec((blk, d_model), lambda i: (i, 0))
    tab_spec = pl.BlockSpec((blk, HEAD_DIM), lambda i: (i, 0))
    vec_spec = pl.BlockSpec((1, d_model), lambda i: (0, 0))
    act = jax.ShapeDtypeStruct((rows, d_model), jnp.bfloat16)
    vec = jax.ShapeDtypeStruct((1, d_model), jnp.float32)
    return pl.pallas_call(
        norm_back_kernel,
        grid=(rows // blk,),
        out_shape=(act, act, vec, vec),
        in_specs=[row_spec] * 4 + [tab_spec] * 2 + [vec_spec] * 2,
        out_specs=(row_spec, row_spec, vec_spec, vec_spec),
        scratch_shapes=[pltpu.VMEM((blk, d_model), jnp.float32)] * 2,
        cost_estimate=pl.CostEstimate(flops=40 * rows * d_model, bytes_accessed=24 * rows * d_model, transcendentals=0),
        name="norm_back",
    )(d_q, d_k, q1, k1, cos_t, sin_t, g_query[None], g_key[None])


N_SLOTS = 4


def tail_kernel(n_dev, ht_ref, dy_v, dy_k, dy_q, w_v, w_k, w_q, x_ref, gy_ref, gn_ref, tq_ref, tk_ref,
                gw_v, gw_k, gw_q, gx_ref, gain_ref,
                ht_own, ht_par, dy_own, dy_par, rs, dh, wbuf, xbuf, gybuf, n_acc, gsend, grecv,
                load_sem, part_send, part_recv, rs_send, rs_recv, w_sem, xy_sem, gx_send, gx_recv, gx_loc,
                gain_send, gain_recv, fin_loc, fin_send, fin_recv):
    me = lax.axis_index('sp')
    chip, core = me // 2, me % 2
    n_chips = n_dev // 2
    step_dir = 1 - 2 * core
    partner = me + step_dir
    right = 2 * lax.rem(chip + step_dir + n_chips, n_chips) + core
    rows, d_model = x_ref.shape
    half = d_model // 2
    piece = rows // n_dev
    chunk = d_model // n_chips
    own_rows = d_model // n_dev
    dys, ws, gws = (dy_v, dy_k, dy_q), (w_v, w_k, w_q), (gw_v, gw_k, gw_q)
    mine = pl.ds(pl.multiple_of(core * half, half), half)
    other = pl.ds(pl.multiple_of((1 - core) * half, half), half)

    loads = [pltpu.make_async_copy(ht_ref, ht_own, load_sem.at[0])]
    loads += [pltpu.make_async_copy(dys[i], dy_own.at[i], load_sem.at[1 + i]) for i in range(3)]
    for cp in loads:
        cp.start()

    barrier = pltpu.get_barrier_semaphore()
    for off in range(1, n_dev):
        pl.semaphore_signal(barrier, inc=1, device_id={'sp': lax.rem(me + off, n_dev)}, device_id_type=MESH)
    pl.semaphore_wait(barrier, n_dev - 1)

    def to_partner(src, dst, idx):
        return pltpu.make_async_remote_copy(src_ref=src, dst_ref=dst, send_sem=part_send.at[idx], recv_sem=part_recv.at[idx],
                                            device_id={'sp': partner}, device_id_type=MESH)

    parts = [to_partner(ht_ref, ht_par, 0)]
    parts += [to_partner(dys[i].at[:, other], dy_par.at[i], 1 + i) for i in range(3)]
    for cp in parts:
        cp.start()

    def rs_copy(w, s):
        return pltpu.make_async_remote_copy(src_ref=rs.at[w, s], dst_ref=rs.at[w, s + 1], send_sem=rs_send.at[w, s], recv_sem=rs_recv.at[w, s],
                                            device_id={'sp': right}, device_id_type=MESH)

    n_tile = 256

    def ring_step(w, s):
        owner = lax.rem(chip - step_dir * (1 + s) + 2 * n_chips, n_chips)
        row_at = pl.multiple_of(owner * chunk, chunk)

        def tile(t, carry):
            col = pl.multiple_of(t * n_tile, n_tile)
            term = dot_nn(ht_own[pl.ds(row_at, chunk), :], dy_own[w, :, pl.ds(pl.multiple_of(core * half + col, n_tile), n_tile)])
            term = term + dot_nn(ht_par[pl.ds(row_at, chunk), :], dy_par[w, :, pl.ds(col, n_tile)])

            @pl.when(s == 0)
            def _():
                rs[w, s, :, pl.ds(col, n_tile)] = term

            @pl.when(s > 0)
            def _():
                rs[w, s, :, pl.ds(col, n_tile)] += term

            return carry

        lax.fori_loop(0, half // n_tile, tile, 0)

    def w_copy(i, n, slot):
        return pltpu.make_async_copy(ws[i].at[pl.ds(pl.multiple_of(n * n_tile, n_tile), n_tile), :], wbuf.at[slot, i], w_sem.at[slot, i])

    def dh_block(n):
        slot = lax.rem(n, 2)
        for i in range(3):
            w_copy(i, n, slot).wait()

        @pl.when(n + 1 < d_model // n_tile)
        def _():
            for i in range(3):
                w_copy(i, n + 1, 1 - slot).start()

        m_tile = 256

        def tile(t, carry):
            at = pl.ds(pl.multiple_of(t * m_tile, m_tile), m_tile)
            total = dot_nt(dy_own[0, at, :], wbuf[slot, 0]) + dot_nt(dy_own[1, at, :], wbuf[slot, 1]) + dot_nt(dy_own[2, at, :], wbuf[slot, 2])
            dh[at, pl.ds(pl.multiple_of(n * n_tile, n_tile), n_tile)] = total.astype(jnp.bfloat16)
            return carry

        lax.fori_loop(0, rows // m_tile, tile, 0)

    def xy_copies(p, slot):
        at = pl.ds(pl.multiple_of(p * piece, piece), piece)
        return (pltpu.make_async_copy(x_ref.at[at, :], xbuf.at[slot], xy_sem.at[slot, 0]),
                pltpu.make_async_copy(gy_ref.at[at, :], gybuf.at[slot], xy_sem.at[slot, 1]))

    def gx_remote(off):
        dest = lax.rem(me + off, n_dev)
        at = pl.ds(pl.multiple_of(dest * piece, piece), piece)
        return pltpu.make_async_remote_copy(src_ref=dh.at[at, :], dst_ref=gx_ref.at[me], send_sem=gx_send.at[off], recv_sem=gx_recv.at[off],
                                            device_id={'sp': dest}, device_id_type=MESH)

    def gx_own():
        at = pl.ds(pl.multiple_of(me * piece, piece), piece)
        return pltpu.make_async_copy(dh.at[at, :], gx_ref.at[me], gx_loc)

    def gain_copy(off):
        dest = lax.rem(me + off, n_dev)
        return pltpu.make_async_remote_copy(src_ref=gsend.at[dest], dst_ref=grecv.at[off], send_sem=gain_send.at[off], recv_sem=gain_recv.at[off],
                                            device_id={'sp': dest}, device_id_type=MESH)

    def grad_x_pieces():
        n_acc[...] = jnp.zeros_like(n_acc)
        for cp in xy_copies(0, 0):
            cp.start()

        def one(p, carry):
            slot = lax.rem(p, 2)
            for cp in xy_copies(p, slot):
                cp.wait()

            @pl.when(p + 1 < n_dev)
            def _():
                for cp in xy_copies(p + 1, 1 - slot):
                    cp.start()

            at = pl.ds(pl.multiple_of(p * piece, piece), piece)
            sub = 32

            def rows_of(j, c2):
                ra = pl.ds(pl.multiple_of(j * sub, sub), sub)
                rb = pl.ds(pl.multiple_of(p * piece + j * sub, sub), sub)
                x_f = xbuf[slot, ra, :].astype(jnp.float32)
                inv = row_inv(x_f)
                hat = x_f * inv
                d_h = dh[rb, :].astype(jnp.float32)
                n_acc[...] += jnp.sum(d_h * hat, axis=0, keepdims=True)
                d_n = d_h * gn_ref[...].astype(jnp.float32)
                mean = jnp.mean(d_n * hat, axis=-1, keepdims=True)
                out = gybuf[slot, ra, :].astype(jnp.float32) + inv * (d_n - hat * mean)
                dh[rb, :] = out.astype(jnp.bfloat16)
                return c2

            lax.fori_loop(0, piece // sub, rows_of, 0)
            return carry

        lax.fori_loop(0, n_dev, one, 0)
        for off in range(1, n_dev):
            gx_remote(off).start()
        gx_own().start()
        for d in range(n_dev):
            gsend[d] = jnp.zeros(gsend.shape[1:], jnp.float32)
            cols = slice(d * own_rows, (d + 1) * own_rows)
            gsend[d, 0:1, :] = n_acc[:, cols]
            gsend[d, 1:2, :] = tq_ref[:, cols]
            gsend[d, 2:3, :] = tk_ref[:, cols]
        for off in range(1, n_dev):
            gain_copy(off).start()

    def finish_out(w):
        keep = pl.ds(pl.multiple_of(core * own_rows, own_rows), own_rows)
        give = pl.ds(pl.multiple_of((1 - core) * own_rows, own_rows), own_rows)
        loc = pltpu.make_async_copy(rs.at[w, N_SLOTS - 1, keep, :], gws[w].at[:, mine], fin_loc.at[w])
        rem = pltpu.make_async_remote_copy(src_ref=rs.at[w, N_SLOTS - 1, give, :], dst_ref=gws[w].at[:, mine], send_sem=fin_send.at[w], recv_sem=fin_recv.at[w],
                                           device_id={'sp': partner}, device_id_type=MESH)
        return loc, rem

    for cp in loads:
        cp.wait()
    for i in range(3):
        w_copy(i, 0, 0).start()
    parts[0].wait_recv()
    n_blocks = d_model // n_tile
    dh_from = 2

    def main(it, carry):
        s, w = it // 3, lax.rem(it, 3)

        @pl.when(s == 0)
        def _():
            pltpu.make_async_remote_copy(src_ref=dy_v.at[:, other], dst_ref=dy_par.at[w], send_sem=part_send.at[1 + w], recv_sem=part_recv.at[1 + w],
                                         device_id={'sp': partner}, device_id_type=MESH).wait_recv()

        @pl.when(s > 0)
        def _():
            rs_copy(w, s - 1).wait_recv()

        ring_step(w, s)

        @pl.when(s < N_SLOTS - 1)
        def _():
            rs_copy(w, s).start()

        for j in range(2):
            blk_i = 2 * (it - dh_from) + j

            @pl.when(jnp.logical_and(blk_i >= 0, blk_i < n_blocks))
            def _():
                dh_block(blk_i)

        @pl.when(it == dh_from + n_blocks // 2)
        def _():
            grad_x_pieces()

        for i in range(3):
            @pl.when(jnp.logical_and(s == N_SLOTS - 1, w == i))
            def _():
                for cp in finish_out(i):
                    cp.start()

        return carry

    lax.fori_loop(0, 3 * N_SLOTS, main, 0)

    for cp in parts:
        cp.wait_send()

    def drain(it, carry):
        rs_copy(lax.rem(it, 3), it // 3).wait_send()
        return carry

    lax.fori_loop(0, 3 * (N_SLOTS - 1), drain, 0)
    for off in range(1, n_dev):
        gain_copy(off).wait()
    total = gsend[me]
    for off in range(1, n_dev):
        total = total + grecv[off]
    gain_ref[...] = total
    for off in range(1, n_dev):
        gx_remote(off).wait()
    gx_own().wait()
    for i in range(3):
        loc, rem = finish_out(i)
        loc.wait()
        rem.wait()


def tail(n_dev, ht, dys, ws, x_bf, gy, g_norm, t_q, t_k):
    rows, d_model = x_bf.shape
    half, chunk, own_rows, piece = d_model // 2, d_model // (n_dev // 2), d_model // n_dev, rows // n_dev
    hbm = pl.BlockSpec(memory_space=pl.ANY)
    vmem = pl.BlockSpec(memory_space=pltpu.VMEM)
    f32, bf16 = jnp.float32, jnp.bfloat16
    gw = jax.ShapeDtypeStruct((own_rows, d_model), f32)
    dma = pltpu.SemaphoreType.DMA
    return pl.pallas_call(
        functools.partial(tail_kernel, n_dev),
        out_shape=(gw, gw, gw, jax.ShapeDtypeStruct((n_dev, piece, d_model), bf16), jax.ShapeDtypeStruct((8, own_rows), f32)),
        in_specs=[hbm] * 9 + [vmem] * 3,
        out_specs=(hbm,) * 4 + (vmem,),
        scratch_shapes=[
            pltpu.VMEM((d_model, rows), bf16), pltpu.VMEM((d_model, rows), bf16),
            pltpu.VMEM((3, rows, d_model), bf16), pltpu.VMEM((3, rows, half), bf16),
            pltpu.VMEM((3, N_SLOTS, chunk, half), f32),
            pltpu.VMEM((rows, d_model), bf16),
            pltpu.VMEM((2, 3, 256, d_model), bf16),
            pltpu.VMEM((2, piece, d_model), bf16), pltpu.VMEM((2, piece, d_model), bf16),
            pltpu.VMEM((1, d_model), f32), pltpu.VMEM((n_dev, 8, own_rows), f32), pltpu.VMEM((n_dev, 8, own_rows), f32),
            dma((4,)), dma((4,)), dma((4,)), dma((3, 3)), dma((3, 3)), dma((2, 3)), dma((2, 2)),
            dma((n_dev,)), dma((n_dev,)), dma, dma((n_dev,)), dma((n_dev,)), dma((3,)), dma((3,)), dma((3,)),
        ],
        compiler_params=pltpu.CompilerParams(collective_id=0, has_side_effects=True, vmem_limit_bytes=67043328),
        cost_estimate=pl.CostEstimate(flops=12 * rows * d_model * d_model, bytes_accessed=64 * 1024 * 1024, transcendentals=0),
        name="tail",
    )(ht, *dys, *ws, x_bf, gy, g_norm[None], t_q, t_k)


def solution(mesh):
    n_dev = mesh.shape['sp']
    exchange = functools.partial(lax.all_to_all, axis_name='sp', split_axis=0, concat_axis=0, tiled=True)

    def sum_rows(partial_sum):
        return lax.psum_scatter(partial_sum, 'sp', scatter_dimension=0, tiled=True)

    def device_step(x_loc, gy_loc, pos_loc, g_norm, w_query, w_key, w_value, w_out, g_query, g_key):
        n_batch, loc_len, d_model = x_loc.shape
        rows = n_batch * loc_len
        x_bf = exchange(x_loc).reshape(rows, d_model)
        pos_seq = exchange(pos_loc).reshape(rows)
        gy = exchange(gy_loc).reshape(rows, d_model)
        cos_t, sin_t = rope_tables(pos_seq)
        q_rot, k_rot, v_val, h_t, q1, k1 = project_qkv(x_bf, cos_t, sin_t, g_norm, g_query, g_key, w_query, w_key, w_value)
        attended, lse = attend_forward(q_rot, k_rot, v_val)
        grad_wo = sum_rows(dot_tn(attended, gy))
        y_seq = (x_bf.astype(jnp.float32) + dot_nn(attended, w_out)).astype(jnp.bfloat16)
        y_out = exchange(y_seq.reshape(n_batch, loc_len, d_model))
        d_attn = dot_nt(gy, w_out).astype(jnp.bfloat16)
        d_q, d_k, d_v = attend_backward(q_rot, k_rot, v_val, d_attn, lse)
        dq_bf, dk_bf, t_q, t_k = norm_back(d_q, d_k, q1, k1, cos_t, sin_t, g_query, g_key)
        grad_wv, grad_wk, grad_wq, grad_x, gains = tail(n_dev, h_t, (d_v, dk_bf, dq_bf), (w_value, w_key, w_query), x_bf, gy, g_norm, t_q, t_k)
        return y_out, grad_x, gains[0], grad_wq, grad_wk, grad_wv, grad_wo, gains[1], gains[2]

    seq_spec = P('dp', 'sp', None)
    mat_rep = P(None, None)
    vec_rep = P(None)
    row_spec = P(('dp', 'sp'), None)
    vec_spec = P(('dp', 'sp'))
    return jax.shard_map(device_step, mesh=mesh, in_specs=(seq_spec, seq_spec, P('dp', 'sp'), vec_rep, mat_rep, mat_rep, mat_rep, mat_rep, vec_rep, vec_rep), out_specs=(seq_spec, seq_spec, vec_spec, row_spec, row_spec, row_spec, row_spec, vec_spec, vec_spec), check_vma=False)
```

```python
import functools
import math
import jax
import jax.numpy as jnp
from jax import lax
from jax.experimental import pallas as pl
from jax.experimental.pallas import tpu as pltpu
from jax.sharding import PartitionSpec as P

HEAD_DIM = 128
NORM_EPS = 1e-5
ROPE_BASE = 10000.0
NEG_BIG = -1e30
LOG2E = math.log2(math.e)
Q_BLOCK = 256


def rope_table(n_pos):
    half_dim = HEAD_DIM // 2
    inv_freq = ROPE_BASE ** (-jnp.arange(half_dim, dtype=jnp.float32) * (2.0 / HEAD_DIM))
    angles = jnp.arange(n_pos, dtype=jnp.float32)[:, None] * inv_freq
    cos_h, sin_h = jnp.cos(angles), jnp.sin(angles)
    table = jnp.concatenate([cos_h, cos_h, -sin_h, sin_h], axis=1)
    parts = []
    for _ in range(3):
        part = lax.reduce_precision(table, 8, 7)
        parts.append(part.astype(jnp.bfloat16))
        table = table - part
    return jnp.stack(parts)


def dot_nn(a, b):
    return lax.dot_general(a, b, (((1,), (0,)), ((), ())), preferred_element_type=jnp.float32)


def dot_nt(a, b):
    return lax.dot_general(a, b, (((1,), (1,)), ((), ())), preferred_element_type=jnp.float32)


def dot_tn(a, b):
    return lax.dot_general(a, b, (((0,), (0,)), ((), ())), preferred_element_type=jnp.float32)


def attn_fwd_kernel(seq_len, q_ref, k_ref, v_ref, o_ref, lse_ref):
    scale2 = LOG2E * HEAD_DIM ** -0.5
    for start in range(0, seq_len, Q_BLOCK):
        stop = start + Q_BLOCK
        q_blk = q_ref[start:stop, :]
        s_diag = dot_nt(k_ref[start:stop, :], q_blk)
        key_i = lax.broadcasted_iota(jnp.int32, s_diag.shape, 0)
        qry_i = lax.broadcasted_iota(jnp.int32, s_diag.shape, 1)
        s_diag = jnp.where(key_i <= qry_i, s_diag, NEG_BIG)
        m = jnp.max(s_diag, axis=0, keepdims=True)
        if start:
            s_past = dot_nt(k_ref[0:start, :], q_blk)
            m = jnp.maximum(m, jnp.max(s_past, axis=0, keepdims=True))
        m2 = m * scale2
        p_diag = jnp.exp2(s_diag * scale2 - m2)
        l = jnp.sum(p_diag, axis=0, keepdims=True)
        acc = dot_tn(v_ref[start:stop, :], p_diag.astype(jnp.bfloat16))
        if start:
            p_past = jnp.exp2(s_past * scale2 - m2)
            l = l + jnp.sum(p_past, axis=0, keepdims=True)
            acc = acc + dot_tn(v_ref[0:start, :], p_past.astype(jnp.bfloat16))
        o_ref[start:stop, :] = (acc / l).T.astype(o_ref.dtype)
        lse_ref[0, :, start:stop] = m2 + jnp.log2(l)


def attn_bwd_kernel(seq_len, q_ref, k_ref, v_ref, do_ref, lse_ref, dq_ref, dk_ref, dv_ref, dk_acc, dv_acc):
    scale = HEAD_DIM ** -0.5
    scale2 = LOG2E * scale
    dk_acc[...] = jnp.zeros_like(dk_acc)
    dv_acc[...] = jnp.zeros_like(dv_acc)
    for start in range(0, seq_len, Q_BLOCK):
        stop = start + Q_BLOCK
        q_blk = q_ref[start:stop, :]
        do_blk = do_ref[start:stop, :]
        lse = lse_ref[0, :, start:stop]
        k_all = k_ref[0:stop, :]
        s = dot_nt(k_all, q_blk)
        p = jnp.exp2(s * scale2 - lse)
        key_i = lax.broadcasted_iota(jnp.int32, (Q_BLOCK, Q_BLOCK), 0)
        qry_i = lax.broadcasted_iota(jnp.int32, (Q_BLOCK, Q_BLOCK), 1)
        p_diag = jnp.where(key_i <= qry_i, p[start:stop, :], 0.0)
        p = jnp.concatenate([p[0:start, :], p_diag], axis=0) if start else p_diag
        dp = dot_nt(v_ref[0:stop, :], do_blk)
        delta = jnp.sum(p * dp, axis=0, keepdims=True)
        ds = (p * (dp - delta) * scale).astype(jnp.bfloat16)
        dv_acc[0:stop, :] += dot_nn(p.astype(jnp.bfloat16), do_blk)
        dk_acc[0:stop, :] += dot_nn(ds, q_blk)
        dq_ref[start:stop, :] = dot_tn(k_all, ds).T.astype(dq_ref.dtype)
    dk_ref[...] = dk_acc[...].astype(dk_ref.dtype)
    dv_ref[...] = dv_acc[...].astype(dv_ref.dtype)


def attend_forward(q, k, v):
    seq_len, d_model = q.shape
    n_heads = d_model // HEAD_DIM
    head_spec = pl.BlockSpec((seq_len, HEAD_DIM), lambda h: (0, h))
    flops = 2 * 2 * seq_len * seq_len * d_model
    return pl.pallas_call(
        functools.partial(attn_fwd_kernel, seq_len),
        grid=(n_heads,),
        out_shape=(jax.ShapeDtypeStruct(q.shape, jnp.bfloat16), jax.ShapeDtypeStruct((n_heads, 1, seq_len), jnp.float32)),
        in_specs=[head_spec] * 3,
        out_specs=(head_spec, pl.BlockSpec((1, 1, seq_len), lambda h: (h, 0, 0))),
        cost_estimate=pl.CostEstimate(flops=flops, bytes_accessed=4 * q.size * 2, transcendentals=seq_len * seq_len * n_heads),
        name="attn_fwd",
    )(q, k, v)


def attend_backward(q, k, v, d_out, lse):
    seq_len, d_model = q.shape
    n_heads = d_model // HEAD_DIM
    head_spec = pl.BlockSpec((seq_len, HEAD_DIM), lambda h: (0, h))
    flops = 5 * 2 * seq_len * seq_len * d_model
    return pl.pallas_call(
        functools.partial(attn_bwd_kernel, seq_len),
        grid=(n_heads,),
        out_shape=(jax.ShapeDtypeStruct(q.shape, jnp.bfloat16),) * 3,
        in_specs=[head_spec] * 4 + [pl.BlockSpec((1, 1, seq_len), lambda h: (h, 0, 0))],
        out_specs=(head_spec,) * 3,
        scratch_shapes=[pltpu.VMEM((seq_len, HEAD_DIM), jnp.float32)] * 2,
        cost_estimate=pl.CostEstimate(flops=flops, bytes_accessed=7 * q.size * 2, transcendentals=seq_len * seq_len * n_heads),
        name="attn_bwd",
    )(q, k, v, d_out, lse)


MESH = pl.DeviceIdType.MESH
ROW_BLOCK = 256


def row_inv(values):
    return lax.rsqrt(jnp.mean(values * values, axis=-1, keepdims=True) + NORM_EPS)


def front_kernel(n_dev, x_loc, pos_loc, tab_ref, gn_ref, gq_ref, gk_ref, wq_ref, wk_ref, wv_ref,
                 x_seq, cs_ref, q_ref, k_ref, v_ref, ht_ref, q1_ref, k1_ref,
                 xv, posv, wbuf, csb, qb, kb, vb, htb, q1b, k1b,
                 w_sem, x_send, x_recv, p_send, p_recv, own_sem, xs_sem, out_sem):
    me = lax.axis_index('sp')
    chip, core = me // 2, me % 2
    n_chips = n_dev // 2
    piece = x_loc.shape[1]
    blk = 2 * piece
    n_pos = tab_ref.shape[1]
    d_model = x_loc.shape[2]

    for cp in [pltpu.make_async_copy(w, wbuf.at[i], w_sem.at[i]) for i, w in enumerate((wv_ref, wq_ref, wk_ref))]:
        cp.start()
    mine = pl.ds(pl.multiple_of(me * piece, piece), piece)
    own = [pltpu.make_async_copy(x_loc.at[me], xv.at[mine, :], own_sem.at[0]), pltpu.make_async_copy(pos_loc.at[me], posv.at[me], own_sem.at[1])]
    for cp in own:
        cp.start()

    barrier = pltpu.get_barrier_semaphore()
    for off in range(1, n_dev):
        pl.semaphore_signal(barrier, inc=1, device_id={'sp': lax.rem(me + off, n_dev)}, device_id_type=MESH)
    pl.semaphore_wait(barrier, n_dev - 1)

    sends = []
    dests = [2 * chip + 1 - core]
    for hop in (1, n_chips - 1, 2):
        dests += [2 * lax.rem(chip + hop, n_chips) + lax.rem(core + flip, 2) for flip in range(2)]
    for i, dest in enumerate(dests):
        sends.append(pltpu.make_async_remote_copy(src_ref=pos_loc.at[dest], dst_ref=posv.at[me], send_sem=p_send.at[i], recv_sem=p_recv.at[me],
                                                  device_id={'sp': dest}, device_id_type=MESH))
        sends.append(pltpu.make_async_remote_copy(src_ref=x_loc.at[dest], dst_ref=xv.at[mine, :], send_sem=x_send.at[i], recv_sem=x_recv.at[me],
                                                  device_id={'sp': dest}, device_id_type=MESH))
    for cp in sends:
        cp.start()

    def arrival(src):
        at = pl.ds(pl.multiple_of(src * piece, piece), piece)
        return (pltpu.make_async_remote_copy(src_ref=x_loc.at[src], dst_ref=xv.at[at, :], send_sem=x_send.at[0], recv_sem=x_recv.at[src],
                                             device_id={'sp': src}, device_id_type=MESH),
                pltpu.make_async_remote_copy(src_ref=pos_loc.at[src], dst_ref=posv.at[src], send_sem=p_send.at[0], recv_sem=p_recv.at[src],
                                             device_id={'sp': src}, device_id_type=MESH))

    def outs(at, slot):
        rows = pl.ds(pl.multiple_of(at, blk), blk)
        pairs = [(csb.at[slot], cs_ref.at[rows, :]), (qb.at[slot], q_ref.at[rows, :]), (kb.at[slot], k_ref.at[rows, :]), (vb.at[slot], v_ref.at[rows, :]),
                 (htb.at[slot], ht_ref.at[:, rows]), (q1b.at[slot], q1_ref.at[rows, :]), (k1b.at[slot], k1_ref.at[rows, :])]
        return [pltpu.make_async_copy(s, d, out_sem.at[slot, i]) for i, (s, d) in enumerate(pairs)]

    def x_out(src_chip):
        rows = pl.ds(pl.multiple_of(src_chip * blk, blk), blk)
        return pltpu.make_async_copy(xv.at[rows, :], x_seq.at[rows, :], xs_sem.at[src_chip])

    def block(b, carry):
        hop = b + (b // 2) * (5 - 2 * b)
        src_chip = lax.rem(chip + hop, n_chips)
        at = pl.multiple_of(src_chip * blk, blk)
        slot = lax.rem(b, 2)

        @pl.when(b == 0)
        def _():
            for cp in own:
                cp.wait()
            for cp in arrival(2 * chip + 1 - core):
                cp.wait_recv()

        @pl.when(b > 0)
        def _():
            for e in range(2):
                for cp in arrival(2 * src_chip + e):
                    cp.wait_recv()

        x_out(src_chip).start()

        @pl.when(b >= 2)
        def _():
            for cp in outs(at, slot):
                cp.wait()

        for e in range(2):
            hot = (lax.broadcasted_iota(jnp.int32, (n_pos, piece), 0) == posv[2 * src_chip + e]).astype(jnp.bfloat16)
            csb[slot, e * piece:(e + 1) * piece, :] = (dot_tn(hot, tab_ref[0]) + dot_tn(hot, tab_ref[1])) + dot_tn(hot, tab_ref[2])
        x_f = xv[pl.ds(at, blk), :].astype(jnp.float32)
        hidden = (x_f * row_inv(x_f) * gn_ref[...].astype(jnp.float32)).astype(jnp.bfloat16)
        htb[slot] = hidden.T

        @pl.when(b == 0)
        def _():
            for i, w in enumerate((wv_ref, wq_ref, wk_ref)):
                pltpu.make_async_copy(w, wbuf.at[i], w_sem.at[i]).wait()

        vb[slot] = dot_nn(hidden, wbuf[0]).astype(jnp.bfloat16)
        cos_t, sin_t = csb[slot, :, 0:HEAD_DIM], csb[slot, :, HEAD_DIM:2 * HEAD_DIM]
        for i, g_ref, raw_ref, out_ref in ((1, gq_ref, q1b, qb), (2, gk_ref, k1b, kb)):
            raw_ref[slot] = dot_nn(hidden, wbuf[i])
            inv = row_inv(raw_ref[slot])
            for c in range(0, d_model, HEAD_DIM):
                u = raw_ref[slot, :, c:c + HEAD_DIM] * inv * g_ref[:, c:c + HEAD_DIM].astype(jnp.float32)
                out_ref[slot, :, c:c + HEAD_DIM] = (u * cos_t + pltpu.roll(u, HEAD_DIM // 2, 1) * sin_t).astype(jnp.bfloat16)
        for cp in outs(at, slot):
            cp.start()
        return carry

    lax.fori_loop(0, n_chips, block, 0)
    for slot in range(2):
        for cp in outs(0, slot):
            cp.wait()
    for i in range(n_chips):
        x_out(i).wait()
    for cp in sends:
        cp.wait_send()


def front(n_dev, x_loc, pos_loc, g_norm, g_query, g_key, w_query, w_key, w_value):
    n_batch, piece, d_model = x_loc.shape
    rows, blk = n_batch * piece, 2 * piece
    hbm = pl.BlockSpec(memory_space=pl.ANY)
    vmem = pl.BlockSpec(memory_space=pltpu.VMEM)
    bf16, f32 = jnp.bfloat16, jnp.float32
    act = jax.ShapeDtypeStruct((rows, d_model), bf16)
    raw = jax.ShapeDtypeStruct((rows, d_model), f32)
    dma = pltpu.SemaphoreType.DMA
    stage = pltpu.VMEM((2, blk, d_model), bf16)
    return pl.pallas_call(
        functools.partial(front_kernel, n_dev),
        out_shape=(act, jax.ShapeDtypeStruct((rows, 2 * HEAD_DIM), f32), act, act, act, jax.ShapeDtypeStruct((d_model, rows), bf16), raw, raw),
        in_specs=[hbm, hbm] + [vmem] * 4 + [hbm] * 3,
        out_specs=(hbm,) * 8,
        scratch_shapes=[
            pltpu.VMEM((rows, d_model), bf16), pltpu.VMEM((n_dev, 1, piece), jnp.int32), pltpu.VMEM((3, d_model, d_model), bf16),
            pltpu.VMEM((2, blk, 2 * HEAD_DIM), f32), stage, stage, stage, pltpu.VMEM((2, d_model, blk), bf16),
            pltpu.VMEM((2, blk, d_model), f32), pltpu.VMEM((2, blk, d_model), f32),
            dma((3,)), dma((n_dev,)), dma((n_dev,)), dma((n_dev,)), dma((n_dev,)), dma((2,)), dma((n_dev // 2,)), dma((2, 7)),
        ],
        compiler_params=pltpu.CompilerParams(collective_id=1, has_side_effects=True, vmem_limit_bytes=62 * 1024 * 1024),
        cost_estimate=pl.CostEstimate(flops=6 * rows * d_model * d_model, bytes_accessed=60 * 1024 * 1024, transcendentals=0),
        name="front",
    )(x_loc, pos_loc[:, None, :], rope_table(rows), g_norm[None], g_query[None], g_key[None], w_query, w_key, w_value)


def norm_back_kernel(dq_ref, dk_ref, q1_ref, k1_ref, cs_ref, gq_ref, gk_ref,
                     oq_ref, ok_ref, tq_ref, tk_ref, tmp_ref, nrm_ref):
    cos_t, sin_t = cs_ref[:, 0:HEAD_DIM], cs_ref[:, HEAD_DIM:2 * HEAD_DIM]
    for d_ref, raw_ref, g_ref, out_ref, t_ref in ((dq_ref, q1_ref, gq_ref, oq_ref, tq_ref), (dk_ref, k1_ref, gk_ref, ok_ref, tk_ref)):
        raw = raw_ref[...]
        inv = row_inv(raw)
        total = jnp.zeros((raw.shape[0], HEAD_DIM), jnp.float32)
        for at in range(0, raw.shape[1], HEAD_DIM):
            d_u = d_ref[:, at:at + HEAD_DIM].astype(jnp.float32)
            d_n = d_u * cos_t - pltpu.roll(d_u, HEAD_DIM // 2, 1) * sin_t
            hat = raw_ref[:, at:at + HEAD_DIM] * inv
            terms = jnp.sum(d_n * hat, axis=0, keepdims=True)

            @pl.when(pl.program_id(0) == 0)
            def _():
                t_ref[:, at:at + HEAD_DIM] = terms

            @pl.when(pl.program_id(0) > 0)
            def _():
                t_ref[:, at:at + HEAD_DIM] += terms

            d_n = d_n * g_ref[:, at:at + HEAD_DIM].astype(jnp.float32)
            total = total + d_n * hat
            tmp_ref[:, at:at + HEAD_DIM] = d_n
            nrm_ref[:, at:at + HEAD_DIM] = hat
        mean = jnp.sum(total, axis=-1, keepdims=True) * (1.0 / raw.shape[1])
        out_ref[...] = (inv * (tmp_ref[...] - nrm_ref[...] * mean)).astype(jnp.bfloat16)


def norm_back(d_q, d_k, q1, k1, cos_sin, g_query, g_key):
    rows, d_model = d_q.shape
    blk = ROW_BLOCK
    row_spec = pl.BlockSpec((blk, d_model), lambda i: (i, 0))
    tab_spec = pl.BlockSpec((blk, 2 * HEAD_DIM), lambda i: (i, 0))
    vec_spec = pl.BlockSpec((1, d_model), lambda i: (0, 0))
    act = jax.ShapeDtypeStruct((rows, d_model), jnp.bfloat16)
    vec = jax.ShapeDtypeStruct((1, d_model), jnp.float32)
    return pl.pallas_call(
        norm_back_kernel,
        grid=(rows // blk,),
        out_shape=(act, act, vec, vec),
        in_specs=[row_spec] * 4 + [tab_spec] + [vec_spec] * 2,
        out_specs=(row_spec, row_spec, vec_spec, vec_spec),
        scratch_shapes=[pltpu.VMEM((blk, d_model), jnp.float32)] * 2,
        cost_estimate=pl.CostEstimate(flops=40 * rows * d_model, bytes_accessed=24 * rows * d_model, transcendentals=0),
        name="norm_back",
    )(d_q, d_k, q1, k1, cos_sin, g_query[None], g_key[None])


N_SLOTS = 4


def tail_kernel(n_dev, ht_ref, dy_v, dy_k, dy_q, w_v, w_k, w_q, x_ref, gy_ref, gn_ref, tq_ref, tk_ref,
                gw_v, gw_k, gw_q, gx_ref, gain_ref,
                ht_own, ht_par, dy_own, dy_par, rs, dh, wbuf, xbuf, gybuf, n_acc, gsend, grecv,
                load_sem, part_send, part_recv, rs_send, rs_recv, w_sem, xy_sem, gx_send, gx_recv, gx_loc,
                gain_send, gain_recv, fin_loc, fin_send, fin_recv):
    me = lax.axis_index('sp')
    chip, core = me // 2, me % 2
    n_chips = n_dev // 2
    step_dir = 1 - 2 * core
    partner = me + step_dir
    right = 2 * lax.rem(chip + step_dir + n_chips, n_chips) + core
    rows, d_model = x_ref.shape
    half = d_model // 2
    piece = rows // n_dev
    chunk = d_model // n_chips
    own_rows = d_model // n_dev
    dys, ws, gws = (dy_v, dy_k, dy_q), (w_v, w_k, w_q), (gw_v, gw_k, gw_q)
    mine = pl.ds(pl.multiple_of(core * half, half), half)
    other = pl.ds(pl.multiple_of((1 - core) * half, half), half)

    loads = [pltpu.make_async_copy(ht_ref, ht_own, load_sem.at[0])]
    loads += [pltpu.make_async_copy(dys[i], dy_own.at[i], load_sem.at[1 + i]) for i in range(3)]
    for cp in loads:
        cp.start()

    barrier = pltpu.get_barrier_semaphore()
    for off in range(1, n_dev):
        pl.semaphore_signal(barrier, inc=1, device_id={'sp': lax.rem(me + off, n_dev)}, device_id_type=MESH)
    pl.semaphore_wait(barrier, n_dev - 1)

    def to_partner(src, dst, idx):
        return pltpu.make_async_remote_copy(src_ref=src, dst_ref=dst, send_sem=part_send.at[idx], recv_sem=part_recv.at[idx],
                                            device_id={'sp': partner}, device_id_type=MESH)

    parts = [to_partner(ht_ref, ht_par, 0)]
    parts += [to_partner(dys[i].at[:, other], dy_par.at[i], 1 + i) for i in range(3)]
    for cp in parts:
        cp.start()

    def rs_copy(w, s):
        return pltpu.make_async_remote_copy(src_ref=rs.at[w, s], dst_ref=rs.at[w, s + 1], send_sem=rs_send.at[w, s], recv_sem=rs_recv.at[w, s],
                                            device_id={'sp': right}, device_id_type=MESH)

    n_tile = 256

    def ring_step(w, s):
        owner = lax.rem(chip - step_dir * (1 + s) + 2 * n_chips, n_chips)
        row_at = pl.multiple_of(owner * chunk, chunk)

        def tile(t, carry):
            col = pl.multiple_of(t * n_tile, n_tile)
            term = dot_nn(ht_own[pl.ds(row_at, chunk), :], dy_own[w, :, pl.ds(pl.multiple_of(core * half + col, n_tile), n_tile)])
            term = term + dot_nn(ht_par[pl.ds(row_at, chunk), :], dy_par[w, :, pl.ds(col, n_tile)])

            @pl.when(s == 0)
            def _():
                rs[w, s, :, pl.ds(col, n_tile)] = term

            @pl.when(s > 0)
            def _():
                rs[w, s, :, pl.ds(col, n_tile)] += term

            return carry

        lax.fori_loop(0, half // n_tile, tile, 0)

    def w_copy(i, n, slot):
        return pltpu.make_async_copy(ws[i].at[pl.ds(pl.multiple_of(n * n_tile, n_tile), n_tile), :], wbuf.at[slot, i], w_sem.at[slot, i])

    def dh_block(n):
        slot = lax.rem(n, 2)
        for i in range(3):
            w_copy(i, n, slot).wait()

        @pl.when(n + 1 < d_model // n_tile)
        def _():
            for i in range(3):
                w_copy(i, n + 1, 1 - slot).start()

        m_tile = 256

        def tile(t, carry):
            at = pl.ds(pl.multiple_of(t * m_tile, m_tile), m_tile)
            total = dot_nt(dy_own[0, at, :], wbuf[slot, 0]) + dot_nt(dy_own[1, at, :], wbuf[slot, 1]) + dot_nt(dy_own[2, at, :], wbuf[slot, 2])
            dh[at, pl.ds(pl.multiple_of(n * n_tile, n_tile), n_tile)] = total.astype(jnp.bfloat16)
            return carry

        lax.fori_loop(0, rows // m_tile, tile, 0)

    def xy_copies(p, slot):
        at = pl.ds(pl.multiple_of(p * piece, piece), piece)
        return (pltpu.make_async_copy(x_ref.at[at, :], xbuf.at[slot], xy_sem.at[slot, 0]),
                pltpu.make_async_copy(gy_ref.at[at, :], gybuf.at[slot], xy_sem.at[slot, 1]))

    def gx_remote(off):
        dest = lax.rem(me + off, n_dev)
        at = pl.ds(pl.multiple_of(dest * piece, piece), piece)
        return pltpu.make_async_remote_copy(src_ref=dh.at[at, :], dst_ref=gx_ref.at[me], send_sem=gx_send.at[off], recv_sem=gx_recv.at[off],
                                            device_id={'sp': dest}, device_id_type=MESH)

    def gx_own():
        at = pl.ds(pl.multiple_of(me * piece, piece), piece)
        return pltpu.make_async_copy(dh.at[at, :], gx_ref.at[me], gx_loc)

    def gain_copy(off):
        dest = lax.rem(me + off, n_dev)
        return pltpu.make_async_remote_copy(src_ref=gsend.at[dest], dst_ref=grecv.at[off], send_sem=gain_send.at[off], recv_sem=gain_recv.at[off],
                                            device_id={'sp': dest}, device_id_type=MESH)

    def grad_x_pieces():
        n_acc[...] = jnp.zeros_like(n_acc)
        for cp in xy_copies(0, 0):
            cp.start()

        def one(p, carry):
            slot = lax.rem(p, 2)
            for cp in xy_copies(p, slot):
                cp.wait()

            @pl.when(p + 1 < n_dev)
            def _():
                for cp in xy_copies(p + 1, 1 - slot):
                    cp.start()

            at = pl.ds(pl.multiple_of(p * piece, piece), piece)
            sub = 32

            def rows_of(j, c2):
                ra = pl.ds(pl.multiple_of(j * sub, sub), sub)
                rb = pl.ds(pl.multiple_of(p * piece + j * sub, sub), sub)
                x_f = xbuf[slot, ra, :].astype(jnp.float32)
                inv = row_inv(x_f)
                hat = x_f * inv
                d_h = dh[rb, :].astype(jnp.float32)
                n_acc[...] += jnp.sum(d_h * hat, axis=0, keepdims=True)
                d_n = d_h * gn_ref[...].astype(jnp.float32)
                mean = jnp.mean(d_n * hat, axis=-1, keepdims=True)
                out = gybuf[slot, ra, :].astype(jnp.float32) + inv * (d_n - hat * mean)
                dh[rb, :] = out.astype(jnp.bfloat16)
                return c2

            lax.fori_loop(0, piece // sub, rows_of, 0)
            return carry

        lax.fori_loop(0, n_dev, one, 0)
        for off in range(1, n_dev):
            gx_remote(off).start()
        gx_own().start()
        for d in range(n_dev):
            gsend[d] = jnp.zeros(gsend.shape[1:], jnp.float32)
            cols = slice(d * own_rows, (d + 1) * own_rows)
            gsend[d, 0:1, :] = n_acc[:, cols]
            gsend[d, 1:2, :] = tq_ref[:, cols]
            gsend[d, 2:3, :] = tk_ref[:, cols]
        for off in range(1, n_dev):
            gain_copy(off).start()

    def finish_out(w):
        keep = pl.ds(pl.multiple_of(core * own_rows, own_rows), own_rows)
        give = pl.ds(pl.multiple_of((1 - core) * own_rows, own_rows), own_rows)
        loc = pltpu.make_async_copy(rs.at[w, N_SLOTS - 1, keep, :], gws[w].at[:, mine], fin_loc.at[w])
        rem = pltpu.make_async_remote_copy(src_ref=rs.at[w, N_SLOTS - 1, give, :], dst_ref=gws[w].at[:, mine], send_sem=fin_send.at[w], recv_sem=fin_recv.at[w],
                                           device_id={'sp': partner}, device_id_type=MESH)
        return loc, rem

    for cp in loads:
        cp.wait()
    for i in range(3):
        w_copy(i, 0, 0).start()
    parts[0].wait_recv()
    n_blocks = d_model // n_tile
    dh_from = 2

    def main(it, carry):
        s, w = it // 3, lax.rem(it, 3)

        @pl.when(s == 0)
        def _():
            pltpu.make_async_remote_copy(src_ref=dy_v.at[:, other], dst_ref=dy_par.at[w], send_sem=part_send.at[1 + w], recv_sem=part_recv.at[1 + w],
                                         device_id={'sp': partner}, device_id_type=MESH).wait_recv()

        @pl.when(s > 0)
        def _():
            rs_copy(w, s - 1).wait_recv()

        ring_step(w, s)

        @pl.when(s < N_SLOTS - 1)
        def _():
            rs_copy(w, s).start()

        for j in range(2):
            blk_i = 2 * (it - dh_from) + j

            @pl.when(jnp.logical_and(blk_i >= 0, blk_i < n_blocks))
            def _():
                dh_block(blk_i)

        @pl.when(it == dh_from + n_blocks // 2)
        def _():
            grad_x_pieces()

        for i in range(3):
            @pl.when(jnp.logical_and(s == N_SLOTS - 1, w == i))
            def _():
                for cp in finish_out(i):
                    cp.start()

        return carry

    lax.fori_loop(0, 3 * N_SLOTS, main, 0)

    for cp in parts:
        cp.wait_send()

    def drain(it, carry):
        rs_copy(lax.rem(it, 3), it // 3).wait_send()
        return carry

    lax.fori_loop(0, 3 * (N_SLOTS - 1), drain, 0)
    for off in range(1, n_dev):
        gain_copy(off).wait()
    total = gsend[me]
    for off in range(1, n_dev):
        total = total + grecv[off]
    gain_ref[...] = total
    for off in range(1, n_dev):
        gx_remote(off).wait()
    gx_own().wait()
    for i in range(3):
        loc, rem = finish_out(i)
        loc.wait()
        rem.wait()


def tail(n_dev, ht, dys, ws, x_bf, gy, g_norm, t_q, t_k):
    rows, d_model = x_bf.shape
    half, chunk, own_rows, piece = d_model // 2, d_model // (n_dev // 2), d_model // n_dev, rows // n_dev
    hbm = pl.BlockSpec(memory_space=pl.ANY)
    vmem = pl.BlockSpec(memory_space=pltpu.VMEM)
    f32, bf16 = jnp.float32, jnp.bfloat16
    gw = jax.ShapeDtypeStruct((own_rows, d_model), f32)
    dma = pltpu.SemaphoreType.DMA
    return pl.pallas_call(
        functools.partial(tail_kernel, n_dev),
        out_shape=(gw, gw, gw, jax.ShapeDtypeStruct((n_dev, piece, d_model), bf16), jax.ShapeDtypeStruct((8, own_rows), f32)),
        in_specs=[hbm] * 9 + [vmem] * 3,
        out_specs=(hbm,) * 4 + (vmem,),
        scratch_shapes=[
            pltpu.VMEM((d_model, rows), bf16), pltpu.VMEM((d_model, rows), bf16),
            pltpu.VMEM((3, rows, d_model), bf16), pltpu.VMEM((3, rows, half), bf16),
            pltpu.VMEM((3, N_SLOTS, chunk, half), f32),
            pltpu.VMEM((rows, d_model), bf16),
            pltpu.VMEM((2, 3, 256, d_model), bf16),
            pltpu.VMEM((2, piece, d_model), bf16), pltpu.VMEM((2, piece, d_model), bf16),
            pltpu.VMEM((1, d_model), f32), pltpu.VMEM((n_dev, 8, own_rows), f32), pltpu.VMEM((n_dev, 8, own_rows), f32),
            dma((4,)), dma((4,)), dma((4,)), dma((3, 3)), dma((3, 3)), dma((2, 3)), dma((2, 2)),
            dma((n_dev,)), dma((n_dev,)), dma, dma((n_dev,)), dma((n_dev,)), dma((3,)), dma((3,)), dma((3,)),
        ],
        compiler_params=pltpu.CompilerParams(collective_id=0, has_side_effects=True, vmem_limit_bytes=67043328),
        cost_estimate=pl.CostEstimate(flops=12 * rows * d_model * d_model, bytes_accessed=64 * 1024 * 1024, transcendentals=0),
        name="tail",
    )(ht, *dys, *ws, x_bf, gy, g_norm[None], t_q, t_k)


def solution(mesh):
    n_dev = mesh.shape['sp']
    exchange = functools.partial(lax.all_to_all, axis_name='sp', split_axis=0, concat_axis=0, tiled=True)

    def sum_rows(partial_sum):
        return lax.psum_scatter(partial_sum, 'sp', scatter_dimension=0, tiled=True)

    def device_step(x_loc, gy_loc, pos_loc, g_norm, w_query, w_key, w_value, w_out, g_query, g_key):
        n_batch, loc_len, d_model = x_loc.shape
        rows = n_batch * loc_len
        x_bf, cos_sin, q_rot, k_rot, v_val, h_t, q1, k1 = front(n_dev, x_loc, pos_loc, g_norm, g_query, g_key, w_query, w_key, w_value)
        gy_late, q_rot = lax.optimization_barrier((gy_loc, q_rot))
        gy = exchange(gy_late).reshape(rows, d_model)
        attended, lse = attend_forward(q_rot, k_rot, v_val)
        grad_wo = sum_rows(dot_tn(attended, gy))
        y_seq = (x_bf.astype(jnp.float32) + dot_nn(attended, w_out)).astype(jnp.bfloat16)
        y_out = exchange(y_seq.reshape(n_batch, loc_len, d_model))
        d_attn = dot_nt(gy, w_out).astype(jnp.bfloat16)
        d_q, d_k, d_v = attend_backward(q_rot, k_rot, v_val, d_attn, lse)
        dq_bf, dk_bf, t_q, t_k = norm_back(d_q, d_k, q1, k1, cos_sin, g_query, g_key)
        grad_wv, grad_wk, grad_wq, grad_x, gains = tail(n_dev, h_t, (d_v, dk_bf, dq_bf), (w_value, w_key, w_query), x_bf, gy, g_norm, t_q, t_k)
        return y_out, grad_x, gains[0], grad_wq, grad_wk, grad_wv, grad_wo, gains[1], gains[2]

    seq_spec = P('dp', 'sp', None)
    mat_rep = P(None, None)
    vec_rep = P(None)
    row_spec = P(('dp', 'sp'), None)
    vec_spec = P(('dp', 'sp'))
    return jax.shard_map(device_step, mesh=mesh, in_specs=(seq_spec, seq_spec, P('dp', 'sp'), vec_rep, mat_rep, mat_rep, mat_rep, mat_rep, vec_rep, vec_rep), out_specs=(seq_spec, seq_spec, vec_spec, row_spec, row_spec, row_spec, row_spec, vec_spec, vec_spec), check_vma=False)
```

```python
import functools
import math
import jax
import jax.numpy as jnp
from jax import lax
from jax.experimental import pallas as pl
from jax.experimental.pallas import tpu as pltpu
from jax.sharding import PartitionSpec as P

HEAD_DIM = 128
NORM_EPS = 1e-5
ROPE_BASE = 10000.0
NEG_BIG = -1e30
LOG2E = math.log2(math.e)
Q_BLOCK = 256


def rope_table(n_pos):
    half_dim = HEAD_DIM // 2
    inv_freq = ROPE_BASE ** (-jnp.arange(half_dim, dtype=jnp.float32) * (2.0 / HEAD_DIM))
    angles = jnp.arange(n_pos, dtype=jnp.float32)[:, None] * inv_freq
    cos_h, sin_h = jnp.cos(angles), jnp.sin(angles)
    table = jnp.concatenate([cos_h, cos_h, -sin_h, sin_h], axis=1)
    parts = []
    for _ in range(3):
        part = lax.reduce_precision(table, 8, 7)
        parts.append(part.astype(jnp.bfloat16))
        table = table - part
    return jnp.stack(parts)


def dot_nn(a, b):
    return lax.dot_general(a, b, (((1,), (0,)), ((), ())), preferred_element_type=jnp.float32)


def dot_nt(a, b):
    return lax.dot_general(a, b, (((1,), (1,)), ((), ())), preferred_element_type=jnp.float32)


def dot_tn(a, b):
    return lax.dot_general(a, b, (((0,), (0,)), ((), ())), preferred_element_type=jnp.float32)


def attn_fwd_kernel(seq_len, q_ref, k_ref, v_ref, o_ref, ot_ref, lse_ref):
    scale2 = LOG2E * HEAD_DIM ** -0.5
    for start in range(0, seq_len, Q_BLOCK):
        stop = start + Q_BLOCK
        q_blk = q_ref[start:stop, :]
        s_diag = dot_nt(k_ref[start:stop, :], q_blk)
        key_i = lax.broadcasted_iota(jnp.int32, s_diag.shape, 0)
        qry_i = lax.broadcasted_iota(jnp.int32, s_diag.shape, 1)
        s_diag = jnp.where(key_i <= qry_i, s_diag, NEG_BIG)
        m = jnp.max(s_diag, axis=0, keepdims=True)
        if start:
            s_past = dot_nt(k_ref[0:start, :], q_blk)
            m = jnp.maximum(m, jnp.max(s_past, axis=0, keepdims=True))
        m2 = m * scale2
        p_diag = jnp.exp2(s_diag * scale2 - m2)
        l = jnp.sum(p_diag, axis=0, keepdims=True)
        acc = dot_tn(v_ref[start:stop, :], p_diag.astype(jnp.bfloat16))
        if start:
            p_past = jnp.exp2(s_past * scale2 - m2)
            l = l + jnp.sum(p_past, axis=0, keepdims=True)
            acc = acc + dot_tn(v_ref[0:start, :], p_past.astype(jnp.bfloat16))
        out = acc / l
        ot_ref[:, start:stop] = out.astype(ot_ref.dtype)
        o_ref[start:stop, :] = out.T.astype(o_ref.dtype)
        lse_ref[0, :, start:stop] = m2 + jnp.log2(l)


def attend_forward(q, k, v):
    seq_len, d_model = q.shape
    n_heads = d_model // HEAD_DIM
    head_spec = pl.BlockSpec((seq_len, HEAD_DIM), lambda h: (0, h))
    flops = 2 * 2 * seq_len * seq_len * d_model
    return pl.pallas_call(
        functools.partial(attn_fwd_kernel, seq_len),
        grid=(n_heads,),
        out_shape=(jax.ShapeDtypeStruct(q.shape, jnp.bfloat16), jax.ShapeDtypeStruct((d_model, seq_len), jnp.bfloat16), jax.ShapeDtypeStruct((n_heads, 1, seq_len), jnp.float32)),
        in_specs=[head_spec] * 3,
        out_specs=(head_spec, pl.BlockSpec((HEAD_DIM, seq_len), lambda h: (h, 0)), pl.BlockSpec((1, 1, seq_len), lambda h: (h, 0, 0))),
        cost_estimate=pl.CostEstimate(flops=flops, bytes_accessed=4 * q.size * 2, transcendentals=seq_len * seq_len * n_heads),
        name="attn_fwd",
    )(q, k, v)


MESH = pl.DeviceIdType.MESH
ROW_BLOCK = 256


def row_inv(values):
    return lax.rsqrt(jnp.mean(values * values, axis=-1, keepdims=True) + NORM_EPS)


def front_kernel(n_dev, x_loc, pos_loc, tab_ref, gn_ref, gq_ref, gk_ref, wq_ref, wk_ref, wv_ref,
                 x_seq, cs_ref, q_ref, k_ref, v_ref, ht_ref, q1_ref, k1_ref,
                 xv, posv, wbuf, csb, qb, kb, vb, htb, q1b, k1b,
                 w_sem, x_send, x_recv, p_send, p_recv, own_sem, xs_sem, out_sem):
    me = lax.axis_index('sp')
    chip, core = me // 2, me % 2
    n_chips = n_dev // 2
    piece = x_loc.shape[1]
    blk = 2 * piece
    n_pos = tab_ref.shape[1]
    d_model = x_loc.shape[2]

    for cp in [pltpu.make_async_copy(w, wbuf.at[i], w_sem.at[i]) for i, w in enumerate((wv_ref, wq_ref, wk_ref))]:
        cp.start()
    mine = pl.ds(pl.multiple_of(me * piece, piece), piece)
    own = [pltpu.make_async_copy(x_loc.at[me], xv.at[mine, :], own_sem.at[0]), pltpu.make_async_copy(pos_loc.at[me], posv.at[me], own_sem.at[1])]
    for cp in own:
        cp.start()

    barrier = pltpu.get_barrier_semaphore()
    for off in range(1, n_dev):
        pl.semaphore_signal(barrier, inc=1, device_id={'sp': lax.rem(me + off, n_dev)}, device_id_type=MESH)
    pl.semaphore_wait(barrier, n_dev - 1)

    sends = []
    dests = [2 * chip + 1 - core]
    for hop in (1, n_chips - 1, 2):
        dests += [2 * lax.rem(chip + hop, n_chips) + lax.rem(core + flip, 2) for flip in range(2)]
    for i, dest in enumerate(dests):
        sends.append(pltpu.make_async_remote_copy(src_ref=pos_loc.at[dest], dst_ref=posv.at[me], send_sem=p_send.at[i], recv_sem=p_recv.at[me],
                                                  device_id={'sp': dest}, device_id_type=MESH))
        sends.append(pltpu.make_async_remote_copy(src_ref=x_loc.at[dest], dst_ref=xv.at[mine, :], send_sem=x_send.at[i], recv_sem=x_recv.at[me],
                                                  device_id={'sp': dest}, device_id_type=MESH))
    for cp in sends:
        cp.start()

    def arrival(src):
        at = pl.ds(pl.multiple_of(src * piece, piece), piece)
        return (pltpu.make_async_remote_copy(src_ref=x_loc.at[src], dst_ref=xv.at[at, :], send_sem=x_send.at[0], recv_sem=x_recv.at[src],
                                             device_id={'sp': src}, device_id_type=MESH),
                pltpu.make_async_remote_copy(src_ref=pos_loc.at[src], dst_ref=posv.at[src], send_sem=p_send.at[0], recv_sem=p_recv.at[src],
                                             device_id={'sp': src}, device_id_type=MESH))

    def outs(at, slot):
        rows = pl.ds(pl.multiple_of(at, blk), blk)
        pairs = [(csb.at[slot], cs_ref.at[rows, :]), (qb.at[slot], q_ref.at[rows, :]), (kb.at[slot], k_ref.at[rows, :]), (vb.at[slot], v_ref.at[rows, :]),
                 (htb.at[slot], ht_ref.at[:, rows]), (q1b.at[slot], q1_ref.at[rows, :]), (k1b.at[slot], k1_ref.at[rows, :])]
        return [pltpu.make_async_copy(s, d, out_sem.at[slot, i]) for i, (s, d) in enumerate(pairs)]

    def x_out(src_chip):
        rows = pl.ds(pl.multiple_of(src_chip * blk, blk), blk)
        return pltpu.make_async_copy(xv.at[rows, :], x_seq.at[rows, :], xs_sem.at[src_chip])

    def block(b, carry):
        hop = b + (b // 2) * (5 - 2 * b)
        src_chip = lax.rem(chip + hop, n_chips)
        at = pl.multiple_of(src_chip * blk, blk)
        slot = lax.rem(b, 2)

        @pl.when(b == 0)
        def _():
            for cp in own:
                cp.wait()
            for cp in arrival(2 * chip + 1 - core):
                cp.wait_recv()

        @pl.when(b > 0)
        def _():
            for e in range(2):
                for cp in arrival(2 * src_chip + e):
                    cp.wait_recv()

        x_out(src_chip).start()

        @pl.when(b >= 2)
        def _():
            for cp in outs(at, slot):
                cp.wait()

        for e in range(2):
            hot = (lax.broadcasted_iota(jnp.int32, (n_pos, piece), 0) == posv[2 * src_chip + e]).astype(jnp.bfloat16)
            csb[slot, e * piece:(e + 1) * piece, :] = (dot_tn(hot, tab_ref[0]) + dot_tn(hot, tab_ref[1])) + dot_tn(hot, tab_ref[2])
        x_f = xv[pl.ds(at, blk), :].astype(jnp.float32)
        hidden = (x_f * row_inv(x_f) * gn_ref[...].astype(jnp.float32)).astype(jnp.bfloat16)
        htb[slot] = hidden.T

        @pl.when(b == 0)
        def _():
            for i, w in enumerate((wv_ref, wq_ref, wk_ref)):
                pltpu.make_async_copy(w, wbuf.at[i], w_sem.at[i]).wait()

        vb[slot] = dot_nn(hidden, wbuf[0]).astype(jnp.bfloat16)
        cos_t, sin_t = csb[slot, :, 0:HEAD_DIM], csb[slot, :, HEAD_DIM:2 * HEAD_DIM]
        for i, g_ref, raw_ref, out_ref in ((1, gq_ref, q1b, qb), (2, gk_ref, k1b, kb)):
            raw_ref[slot] = dot_nn(hidden, wbuf[i])
            inv = row_inv(raw_ref[slot])
            for c in range(0, d_model, HEAD_DIM):
                u = raw_ref[slot, :, c:c + HEAD_DIM] * inv * g_ref[:, c:c + HEAD_DIM].astype(jnp.float32)
                out_ref[slot, :, c:c + HEAD_DIM] = (u * cos_t + pltpu.roll(u, HEAD_DIM // 2, 1) * sin_t).astype(jnp.bfloat16)
        for cp in outs(at, slot):
            cp.start()
        return carry

    lax.fori_loop(0, n_chips, block, 0)
    for slot in range(2):
        for cp in outs(0, slot):
            cp.wait()
    for i in range(n_chips):
        x_out(i).wait()
    for cp in sends:
        cp.wait_send()


def front(n_dev, x_loc, pos_loc, g_norm, g_query, g_key, w_query, w_key, w_value):
    n_batch, piece, d_model = x_loc.shape
    rows, blk = n_batch * piece, 2 * piece
    hbm = pl.BlockSpec(memory_space=pl.ANY)
    vmem = pl.BlockSpec(memory_space=pltpu.VMEM)
    bf16, f32 = jnp.bfloat16, jnp.float32
    act = jax.ShapeDtypeStruct((rows, d_model), bf16)
    raw = jax.ShapeDtypeStruct((rows, d_model), f32)
    dma = pltpu.SemaphoreType.DMA
    stage = pltpu.VMEM((2, blk, d_model), bf16)
    return pl.pallas_call(
        functools.partial(front_kernel, n_dev),
        out_shape=(act, jax.ShapeDtypeStruct((rows, 2 * HEAD_DIM), f32), act, act, act, jax.ShapeDtypeStruct((d_model, rows), bf16), raw, raw),
        in_specs=[hbm, hbm] + [vmem] * 4 + [hbm] * 3,
        out_specs=(hbm,) * 8,
        scratch_shapes=[
            pltpu.VMEM((rows, d_model), bf16), pltpu.VMEM((n_dev, 1, piece), jnp.int32), pltpu.VMEM((3, d_model, d_model), bf16),
            pltpu.VMEM((2, blk, 2 * HEAD_DIM), f32), stage, stage, stage, pltpu.VMEM((2, d_model, blk), bf16),
            pltpu.VMEM((2, blk, d_model), f32), pltpu.VMEM((2, blk, d_model), f32),
            dma((3,)), dma((n_dev,)), dma((n_dev,)), dma((n_dev,)), dma((n_dev,)), dma((2,)), dma((n_dev // 2,)), dma((2, 7)),
        ],
        compiler_params=pltpu.CompilerParams(collective_id=1, has_side_effects=True, vmem_limit_bytes=62 * 1024 * 1024),
        cost_estimate=pl.CostEstimate(flops=6 * rows * d_model * d_model, bytes_accessed=60 * 1024 * 1024, transcendentals=0),
        name="front",
    )(x_loc, pos_loc[:, None, :], rope_table(rows), g_norm[None], g_query[None], g_key[None], w_query, w_key, w_value)


def middle_kernel(n_dev, y_seq, at_ref, gy_ref, wo_ref, q_ref, k_ref, v_ref, q1_ref, k1_ref, cs_ref, lse_ref, gq_ref, gk_ref,
                  y_out, gw_ref, dq_ref, dk_ref, dv_ref, tq_ref, tk_ref,
                  wo, at_own, at_par, gy_own, gy_par, rs, dqk, hbuf, dvb, dob, dk_acc, dv_acc, rawb, tmp, nrm,
                  load_sem, y_send, y_recv, y_loc, part_send, part_recv, rs_send, rs_recv, h_sem, dv_sem, raw_sem, dqk_sem,
                  fin_loc, fin_send, fin_recv):
    me = lax.axis_index('sp')
    chip, core = me // 2, me % 2
    n_chips = n_dev // 2
    step_dir = 1 - 2 * core
    partner = me + step_dir
    right = 2 * lax.rem(chip + step_dir + n_chips, n_chips) + core
    rows, d_model = gy_ref.shape
    n_heads = d_model // HEAD_DIM
    half, sub = d_model // 2, d_model // 4
    piece, chunk, own_rows = rows // n_dev, d_model // n_chips, d_model // n_dev
    other = pl.ds(pl.multiple_of((1 - core) * half, half), half)

    loads = [pltpu.make_async_copy(s, d, load_sem.at[i]) for i, (s, d) in enumerate(((at_ref, at_own), (gy_ref, gy_own), (wo_ref, wo)))]
    for cp in loads:
        cp.start()

    def head_copies(h, slot):
        cols = pl.ds(pl.multiple_of(h * HEAD_DIM, HEAD_DIM), HEAD_DIM)
        return [pltpu.make_async_copy(r.at[:, cols], hbuf.at[slot, i], h_sem.at[slot, i]) for i, r in enumerate((q_ref, k_ref, v_ref))]

    for cp in head_copies(0, 0):
        cp.start()

    barrier = pltpu.get_barrier_semaphore()
    for off in range(1, n_dev):
        pl.semaphore_signal(barrier, inc=1, device_id={'sp': lax.rem(me + off, n_dev)}, device_id_type=MESH)
    pl.semaphore_wait(barrier, n_dev - 1)

    parts = [pltpu.make_async_remote_copy(src_ref=s, dst_ref=d, send_sem=part_send.at[i], recv_sem=part_recv.at[i], device_id={'sp': partner}, device_id_type=MESH)
             for i, (s, d) in enumerate(((at_ref, at_par), (gy_ref.at[:, other], gy_par)))]
    for cp in parts:
        cp.start()

    def rs_copy(ch, s):
        return pltpu.make_async_remote_copy(src_ref=rs.at[ch, s], dst_ref=rs.at[ch, s + 1], send_sem=rs_send.at[ch, s], recv_sem=rs_recv.at[ch, s],
                                            device_id={'sp': right}, device_id_type=MESH)

    n_tile = 256

    def ring_step(ch, s):
        owner = lax.rem(chip - step_dir * (1 + s) + 2 * n_chips, n_chips)
        row_at = pl.ds(pl.multiple_of(owner * chunk, chunk), chunk)

        def tile(t, carry):
            col = pl.multiple_of(t * n_tile, n_tile)
            in_half = pl.multiple_of(ch * sub + col, n_tile)
            term = dot_nn(at_own[row_at, :], gy_own[:, pl.ds(pl.multiple_of(core * half + in_half, n_tile), n_tile)])
            term = term + dot_nn(at_par[row_at, :], gy_par[:, pl.ds(in_half, n_tile)])

            @pl.when(s == 0)
            def _():
                rs[ch, s, :, pl.ds(col, n_tile)] = term

            @pl.when(s > 0)
            def _():
                rs[ch, s, :, pl.ds(col, n_tile)] += term

            return carry

        lax.fori_loop(0, sub // n_tile, tile, 0)

    def ring(i):
        ch, s = lax.rem(i, 2), i // 2

        @pl.when(s > 0)
        def _():
            rs_copy(ch, s - 1).wait_recv()

        ring_step(ch, s)

        @pl.when(s < N_SLOTS - 1)
        def _():
            rs_copy(ch, s).start()

    def y_remote(off):
        dest = lax.rem(me + off, n_dev)
        return pltpu.make_async_remote_copy(src_ref=y_seq.at[dest], dst_ref=y_out.at[me], send_sem=y_send.at[off], recv_sem=y_recv.at[off],
                                            device_id={'sp': dest}, device_id_type=MESH)

    y_own = pltpu.make_async_copy(y_seq.at[me], y_out.at[me], y_loc)
    for off in range(1, n_dev):
        y_remote(off).start()
    y_own.start()

    def finish_out(ch):
        keep = pl.ds(pl.multiple_of(core * own_rows, own_rows), own_rows)
        give = pl.ds(pl.multiple_of((1 - core) * own_rows, own_rows), own_rows)
        cols = pl.ds(pl.multiple_of(core * half + ch * sub, sub), sub)
        loc = pltpu.make_async_copy(rs.at[ch, N_SLOTS - 1, keep, :], gw_ref.at[:, cols], fin_loc.at[ch])
        rem = pltpu.make_async_remote_copy(src_ref=rs.at[ch, N_SLOTS - 1, give, :], dst_ref=gw_ref.at[:, cols], send_sem=fin_send.at[ch], recv_sem=fin_recv.at[ch],
                                           device_id={'sp': partner}, device_id_type=MESH)
        return loc, rem

    scale = HEAD_DIM ** -0.5
    scale2 = LOG2E * scale

    def dv_copy(h, slot):
        cols = pl.ds(pl.multiple_of(h * HEAD_DIM, HEAD_DIM), HEAD_DIM)
        return pltpu.make_async_copy(dvb.at[slot], dv_ref.at[:, cols], dv_sem.at[slot])

    def head(h, carry):
        slot = lax.rem(h, 2)
        cols = pl.ds(pl.multiple_of(h * HEAD_DIM, HEAD_DIM), HEAD_DIM)
        in_pair = pl.ds(pl.multiple_of(slot * HEAD_DIM, HEAD_DIM), HEAD_DIM)

        @pl.when(slot == 0)
        def _():
            def do_tile(t, c2):
                ra = pl.ds(pl.multiple_of(t * 256, 256), 256)
                dob[ra, :] = dot_nt(gy_own[ra, :], wo[pl.ds(pl.multiple_of(h * HEAD_DIM, 2 * HEAD_DIM), 2 * HEAD_DIM), :]).astype(jnp.bfloat16)
                return c2

            lax.fori_loop(0, rows // 256, do_tile, 0)

        for cp in head_copies(h, slot):
            cp.wait()

        @pl.when(h + 1 < n_heads)
        def _():
            for cp in head_copies(h + 1, 1 - slot):
                cp.start()

        dk_acc[...] = jnp.zeros_like(dk_acc)
        dv_acc[...] = jnp.zeros_like(dv_acc)
        for start in range(0, rows, Q_BLOCK):
            stop = start + Q_BLOCK
            q_blk = hbuf[slot, 0, start:stop, :]
            do_blk = dob[start:stop, in_pair]
            lse = lse_ref[h, :, start:stop]
            k_all = hbuf[slot, 1, 0:stop, :]
            p = jnp.exp2(dot_nt(k_all, q_blk) * scale2 - lse)
            key_i = lax.broadcasted_iota(jnp.int32, (Q_BLOCK, Q_BLOCK), 0)
            qry_i = lax.broadcasted_iota(jnp.int32, (Q_BLOCK, Q_BLOCK), 1)
            p_diag = jnp.where(key_i <= qry_i, p[start:stop, :], 0.0)
            p = jnp.concatenate([p[0:start, :], p_diag], axis=0) if start else p_diag
            dp = dot_nt(hbuf[slot, 2, 0:stop, :], do_blk)
            delta = jnp.sum(p * dp, axis=0, keepdims=True)
            ds = (p * (dp - delta) * scale).astype(jnp.bfloat16)
            dv_acc[0:stop, :] += dot_nn(p.astype(jnp.bfloat16), do_blk)
            dk_acc[0:stop, :] += dot_nn(ds, q_blk)
            dqk[0, start:stop, cols] = dot_tn(k_all, ds).T.astype(jnp.bfloat16)
        dqk[1, :, cols] = dk_acc[...].astype(jnp.bfloat16)

        @pl.when(h >= 2)
        def _():
            dv_copy(h, slot).wait()

        dvb[slot] = dv_acc[...].astype(jnp.bfloat16)
        dv_copy(h, slot).start()

        ring_from = n_heads - 6

        @pl.when(jnp.logical_and(h >= ring_from, lax.rem(h - ring_from, 2) == 1))
        def _():
            ring(2 + (h - ring_from) // 2)

        return carry

    loads[0].wait()
    loads[1].wait()
    for cp in parts:
        cp.wait_recv()
    for i in range(2):
        ring(i)
    loads[2].wait()
    lax.fori_loop(0, n_heads, head, 0)
    for slot in range(2):
        dv_copy(0, slot).wait()

    def raw_copy(i, b, slot):
        src = (q1_ref, k1_ref)[i]
        return pltpu.make_async_copy(src.at[pl.ds(pl.multiple_of(b * piece, piece), piece), :], rawb.at[slot], raw_sem.at[slot])

    for i, g_ref, t_ref in ((0, gq_ref, tq_ref), (1, gk_ref, tk_ref)):
        t_ref[...] = jnp.zeros_like(t_ref)
        raw_copy(i, 0, 0).start()

        def norm_rows(b, carry):
            slot = lax.rem(b, 2)
            raw_copy(i, b, slot).wait()

            @pl.when(b + 1 < n_dev)
            def _():
                raw_copy(i, b + 1, 1 - slot).start()

            at = pl.ds(pl.multiple_of(b * piece, piece), piece)
            inv = row_inv(rawb[slot])
            cos_t, sin_t = cs_ref[at, 0:HEAD_DIM], cs_ref[at, HEAD_DIM:2 * HEAD_DIM]
            total = jnp.zeros((piece, HEAD_DIM), jnp.float32)
            for c in range(0, d_model, HEAD_DIM):
                d_u = dqk[i, at, c:c + HEAD_DIM].astype(jnp.float32)
                d_n = d_u * cos_t - pltpu.roll(d_u, HEAD_DIM // 2, 1) * sin_t
                hat = rawb[slot, :, c:c + HEAD_DIM] * inv
                t_ref[:, c:c + HEAD_DIM] += jnp.sum(d_n * hat, axis=0, keepdims=True)
                d_n = d_n * g_ref[:, c:c + HEAD_DIM].astype(jnp.float32)
                total = total + d_n * hat
                tmp[:, c:c + HEAD_DIM] = d_n
                nrm[:, c:c + HEAD_DIM] = hat
            mean = jnp.sum(total, axis=-1, keepdims=True) * (1.0 / d_model)
            for c in range(0, d_model, HEAD_DIM):
                dqk[i, at, c:c + HEAD_DIM] = (inv * (tmp[:, c:c + HEAD_DIM] - nrm[:, c:c + HEAD_DIM] * mean)).astype(jnp.bfloat16)
            return carry

        lax.fori_loop(0, n_dev, norm_rows, 0)
        pltpu.make_async_copy(dqk.at[i], (dq_ref, dk_ref)[i], dqk_sem.at[i]).start()
        if i == 0:
            ring(jnp.int32(5))

    for ch in range(2):
        ring(jnp.int32(6 + ch))
        for cp in finish_out(ch):
            cp.start()
    for cp in parts:
        cp.wait_send()
    for ch in range(2):
        for s in range(N_SLOTS - 1):
            rs_copy(ch, s).wait_send()
    for off in range(1, n_dev):
        y_remote(off).wait()
    y_own.wait()
    for i in range(2):
        pltpu.make_async_copy(dqk.at[i], (dq_ref, dk_ref)[i], dqk_sem.at[i]).wait()
    for ch in range(2):
        loc, rem = finish_out(ch)
        loc.wait()
        rem.wait()


def middle(n_dev, y_seq, a_t, gy, w_out, q_rot, k_rot, v_val, q1, k1, cos_sin, lse, g_query, g_key):
    rows, d_model = gy.shape
    piece, chunk, own_rows, sub = rows // n_dev, d_model // (n_dev // 2), d_model // n_dev, d_model // 4
    hbm = pl.BlockSpec(memory_space=pl.ANY)
    vmem = pl.BlockSpec(memory_space=pltpu.VMEM)
    f32, bf16 = jnp.float32, jnp.bfloat16
    act = jax.ShapeDtypeStruct((rows, d_model), bf16)
    vec = jax.ShapeDtypeStruct((1, d_model), f32)
    dma = pltpu.SemaphoreType.DMA
    return pl.pallas_call(
        functools.partial(middle_kernel, n_dev),
        out_shape=(jax.ShapeDtypeStruct((n_dev, piece, d_model), bf16), jax.ShapeDtypeStruct((own_rows, d_model), f32), act, act, act, vec, vec),
        in_specs=[hbm] * 9 + [vmem] * 4,
        out_specs=(hbm,) * 5 + (vmem,) * 2,
        scratch_shapes=[
            pltpu.VMEM((d_model, d_model), bf16), pltpu.VMEM((d_model, rows), bf16), pltpu.VMEM((d_model, rows), bf16),
            pltpu.VMEM((rows, d_model), bf16), pltpu.VMEM((rows, d_model // 2), bf16),
            pltpu.VMEM((2, N_SLOTS, chunk, sub), f32), pltpu.VMEM((2, rows, d_model), bf16),
            pltpu.VMEM((2, 3, rows, HEAD_DIM), bf16), pltpu.VMEM((2, rows, HEAD_DIM), bf16), pltpu.VMEM((rows, 2 * HEAD_DIM), bf16),
            pltpu.VMEM((rows, HEAD_DIM), f32), pltpu.VMEM((rows, HEAD_DIM), f32),
            pltpu.VMEM((2, piece, d_model), f32), pltpu.VMEM((piece, d_model), f32), pltpu.VMEM((piece, d_model), f32),
            dma((3,)), dma((n_dev,)), dma((n_dev,)), dma, dma((2,)), dma((2,)), dma((2, 3)), dma((2, 3)), dma((2, 3)), dma((2,)), dma((2,)), dma((2,)),
            dma((2,)), dma((2,)), dma((2,)),
        ],
        compiler_params=pltpu.CompilerParams(collective_id=2, has_side_effects=True, vmem_limit_bytes=67043328),
        cost_estimate=pl.CostEstimate(flops=12 * rows * rows * d_model, bytes_accessed=64 * 1024 * 1024, transcendentals=0),
        name="middle",
    )(y_seq.reshape(n_dev, piece, d_model), a_t, gy, w_out, q_rot, k_rot, v_val, q1, k1, cos_sin, lse, g_query[None], g_key[None])


N_SLOTS = 4


def tail_kernel(n_dev, ht_ref, dy_v, dy_k, dy_q, w_v, w_k, w_q, x_ref, gy_ref, gn_ref, tq_ref, tk_ref,
                gw_v, gw_k, gw_q, gx_ref, gain_ref,
                ht_own, ht_par, dy_own, dy_par, rs, dh, wbuf, xbuf, gybuf, n_acc, gsend, grecv,
                load_sem, part_send, part_recv, rs_send, rs_recv, w_sem, xy_sem, gx_send, gx_recv, gx_loc,
                gain_send, gain_recv, fin_loc, fin_send, fin_recv):
    me = lax.axis_index('sp')
    chip, core = me // 2, me % 2
    n_chips = n_dev // 2
    step_dir = 1 - 2 * core
    partner = me + step_dir
    right = 2 * lax.rem(chip + step_dir + n_chips, n_chips) + core
    rows, d_model = x_ref.shape
    half = d_model // 2
    piece = rows // n_dev
    chunk = d_model // n_chips
    own_rows = d_model // n_dev
    dys, ws, gws = (dy_v, dy_k, dy_q), (w_v, w_k, w_q), (gw_v, gw_k, gw_q)
    mine = pl.ds(pl.multiple_of(core * half, half), half)
    other = pl.ds(pl.multiple_of((1 - core) * half, half), half)

    loads = [pltpu.make_async_copy(ht_ref, ht_own, load_sem.at[0])]
    loads += [pltpu.make_async_copy(dys[i], dy_own.at[i], load_sem.at[1 + i]) for i in range(3)]
    for cp in loads:
        cp.start()

    barrier = pltpu.get_barrier_semaphore()
    for off in range(1, n_dev):
        pl.semaphore_signal(barrier, inc=1, device_id={'sp': lax.rem(me + off, n_dev)}, device_id_type=MESH)
    pl.semaphore_wait(barrier, n_dev - 1)

    def to_partner(src, dst, idx):
        return pltpu.make_async_remote_copy(src_ref=src, dst_ref=dst, send_sem=part_send.at[idx], recv_sem=part_recv.at[idx],
                                            device_id={'sp': partner}, device_id_type=MESH)

    parts = [to_partner(ht_ref, ht_par, 0)]
    parts += [to_partner(dys[i].at[:, other], dy_par.at[i], 1 + i) for i in range(3)]
    for cp in parts:
        cp.start()

    def rs_copy(w, s):
        return pltpu.make_async_remote_copy(src_ref=rs.at[w, s], dst_ref=rs.at[w, s + 1], send_sem=rs_send.at[w, s], recv_sem=rs_recv.at[w, s],
                                            device_id={'sp': right}, device_id_type=MESH)

    n_tile = 256

    def ring_step(w, s):
        owner = lax.rem(chip - step_dir * (1 + s) + 2 * n_chips, n_chips)
        row_at = pl.multiple_of(owner * chunk, chunk)

        def tile(t, carry):
            col = pl.multiple_of(t * n_tile, n_tile)
            term = dot_nn(ht_own[pl.ds(row_at, chunk), :], dy_own[w, :, pl.ds(pl.multiple_of(core * half + col, n_tile), n_tile)])
            term = term + dot_nn(ht_par[pl.ds(row_at, chunk), :], dy_par[w, :, pl.ds(col, n_tile)])

            @pl.when(s == 0)
            def _():
                rs[w, s, :, pl.ds(col, n_tile)] = term

            @pl.when(s > 0)
            def _():
                rs[w, s, :, pl.ds(col, n_tile)] += term

            return carry

        lax.fori_loop(0, half // n_tile, tile, 0)

    def w_copy(i, n, slot):
        return pltpu.make_async_copy(ws[i].at[pl.ds(pl.multiple_of(n * n_tile, n_tile), n_tile), :], wbuf.at[slot, i], w_sem.at[slot, i])

    def dh_block(n):
        slot = lax.rem(n, 2)
        for i in range(3):
            w_copy(i, n, slot).wait()

        @pl.when(n + 1 < d_model // n_tile)
        def _():
            for i in range(3):
                w_copy(i, n + 1, 1 - slot).start()

        m_tile = 256

        def tile(t, carry):
            at = pl.ds(pl.multiple_of(t * m_tile, m_tile), m_tile)
            total = dot_nt(dy_own[0, at, :], wbuf[slot, 0]) + dot_nt(dy_own[1, at, :], wbuf[slot, 1]) + dot_nt(dy_own[2, at, :], wbuf[slot, 2])
            dh[at, pl.ds(pl.multiple_of(n * n_tile, n_tile), n_tile)] = total.astype(jnp.bfloat16)
            return carry

        lax.fori_loop(0, rows // m_tile, tile, 0)

    def xy_copies(p, slot):
        at = pl.ds(pl.multiple_of(p * piece, piece), piece)
        return (pltpu.make_async_copy(x_ref.at[at, :], xbuf.at[slot], xy_sem.at[slot, 0]),
                pltpu.make_async_copy(gy_ref.at[at, :], gybuf.at[slot], xy_sem.at[slot, 1]))

    def gx_remote(off):
        dest = lax.rem(me + off, n_dev)
        at = pl.ds(pl.multiple_of(dest * piece, piece), piece)
        return pltpu.make_async_remote_copy(src_ref=dh.at[at, :], dst_ref=gx_ref.at[me], send_sem=gx_send.at[off], recv_sem=gx_recv.at[off],
                                            device_id={'sp': dest}, device_id_type=MESH)

    def gx_own():
        at = pl.ds(pl.multiple_of(me * piece, piece), piece)
        return pltpu.make_async_copy(dh.at[at, :], gx_ref.at[me], gx_loc)

    def gain_copy(off):
        dest = lax.rem(me + off, n_dev)
        return pltpu.make_async_remote_copy(src_ref=gsend.at[dest], dst_ref=grecv.at[off], send_sem=gain_send.at[off], recv_sem=gain_recv.at[off],
                                            device_id={'sp': dest}, device_id_type=MESH)

    def grad_x_pieces():
        n_acc[...] = jnp.zeros_like(n_acc)
        for cp in xy_copies(0, 0):
            cp.start()

        def one(p, carry):
            slot = lax.rem(p, 2)
            for cp in xy_copies(p, slot):
                cp.wait()

            @pl.when(p + 1 < n_dev)
            def _():
                for cp in xy_copies(p + 1, 1 - slot):
                    cp.start()

            at = pl.ds(pl.multiple_of(p * piece, piece), piece)
            sub = 32

            def rows_of(j, c2):
                ra = pl.ds(pl.multiple_of(j * sub, sub), sub)
                rb = pl.ds(pl.multiple_of(p * piece + j * sub, sub), sub)
                x_f = xbuf[slot, ra, :].astype(jnp.float32)
                inv = row_inv(x_f)
                hat = x_f * inv
                d_h = dh[rb, :].astype(jnp.float32)
                n_acc[...] += jnp.sum(d_h * hat, axis=0, keepdims=True)
                d_n = d_h * gn_ref[...].astype(jnp.float32)
                mean = jnp.mean(d_n * hat, axis=-1, keepdims=True)
                out = gybuf[slot, ra, :].astype(jnp.float32) + inv * (d_n - hat * mean)
                dh[rb, :] = out.astype(jnp.bfloat16)
                return c2

            lax.fori_loop(0, piece // sub, rows_of, 0)
            return carry

        lax.fori_loop(0, n_dev, one, 0)
        for off in range(1, n_dev):
            gx_remote(off).start()
        gx_own().start()
        for d in range(n_dev):
            gsend[d] = jnp.zeros(gsend.shape[1:], jnp.float32)
            cols = slice(d * own_rows, (d + 1) * own_rows)
            gsend[d, 0:1, :] = n_acc[:, cols]
            gsend[d, 1:2, :] = tq_ref[:, cols]
            gsend[d, 2:3, :] = tk_ref[:, cols]
        for off in range(1, n_dev):
            gain_copy(off).start()

    def finish_out(w):
        keep = pl.ds(pl.multiple_of(core * own_rows, own_rows), own_rows)
        give = pl.ds(pl.multiple_of((1 - core) * own_rows, own_rows), own_rows)
        loc = pltpu.make_async_copy(rs.at[w, N_SLOTS - 1, keep, :], gws[w].at[:, mine], fin_loc.at[w])
        rem = pltpu.make_async_remote_copy(src_ref=rs.at[w, N_SLOTS - 1, give, :], dst_ref=gws[w].at[:, mine], send_sem=fin_send.at[w], recv_sem=fin_recv.at[w],
                                           device_id={'sp': partner}, device_id_type=MESH)
        return loc, rem

    for cp in loads:
        cp.wait()
    for i in range(3):
        w_copy(i, 0, 0).start()
    parts[0].wait_recv()
    n_blocks = d_model // n_tile
    dh_from = 2

    def main(it, carry):
        s, w = it // 3, lax.rem(it, 3)

        @pl.when(s == 0)
        def _():
            pltpu.make_async_remote_copy(src_ref=dy_v.at[:, other], dst_ref=dy_par.at[w], send_sem=part_send.at[1 + w], recv_sem=part_recv.at[1 + w],
                                         device_id={'sp': partner}, device_id_type=MESH).wait_recv()

        @pl.when(s > 0)
        def _():
            rs_copy(w, s - 1).wait_recv()

        ring_step(w, s)

        @pl.when(s < N_SLOTS - 1)
        def _():
            rs_copy(w, s).start()

        for j in range(2):
            blk_i = 2 * (it - dh_from) + j

            @pl.when(jnp.logical_and(blk_i >= 0, blk_i < n_blocks))
            def _():
                dh_block(blk_i)

        @pl.when(it == dh_from + n_blocks // 2)
        def _():
            grad_x_pieces()

        for i in range(3):
            @pl.when(jnp.logical_and(s == N_SLOTS - 1, w == i))
            def _():
                for cp in finish_out(i):
                    cp.start()

        return carry

    lax.fori_loop(0, 3 * N_SLOTS, main, 0)

    for cp in parts:
        cp.wait_send()

    def drain(it, carry):
        rs_copy(lax.rem(it, 3), it // 3).wait_send()
        return carry

    lax.fori_loop(0, 3 * (N_SLOTS - 1), drain, 0)
    for off in range(1, n_dev):
        gain_copy(off).wait()
    total = gsend[me]
    for off in range(1, n_dev):
        total = total + grecv[off]
    gain_ref[...] = total
    for off in range(1, n_dev):
        gx_remote(off).wait()
    gx_own().wait()
    for i in range(3):
        loc, rem = finish_out(i)
        loc.wait()
        rem.wait()


def tail(n_dev, ht, dys, ws, x_bf, gy, g_norm, t_q, t_k):
    rows, d_model = x_bf.shape
    half, chunk, own_rows, piece = d_model // 2, d_model // (n_dev // 2), d_model // n_dev, rows // n_dev
    hbm = pl.BlockSpec(memory_space=pl.ANY)
    vmem = pl.BlockSpec(memory_space=pltpu.VMEM)
    f32, bf16 = jnp.float32, jnp.bfloat16
    gw = jax.ShapeDtypeStruct((own_rows, d_model), f32)
    dma = pltpu.SemaphoreType.DMA
    return pl.pallas_call(
        functools.partial(tail_kernel, n_dev),
        out_shape=(gw, gw, gw, jax.ShapeDtypeStruct((n_dev, piece, d_model), bf16), jax.ShapeDtypeStruct((8, own_rows), f32)),
        in_specs=[hbm] * 9 + [vmem] * 3,
        out_specs=(hbm,) * 4 + (vmem,),
        scratch_shapes=[
            pltpu.VMEM((d_model, rows), bf16), pltpu.VMEM((d_model, rows), bf16),
            pltpu.VMEM((3, rows, d_model), bf16), pltpu.VMEM((3, rows, half), bf16),
            pltpu.VMEM((3, N_SLOTS, chunk, half), f32),
            pltpu.VMEM((rows, d_model), bf16),
            pltpu.VMEM((2, 3, 256, d_model), bf16),
            pltpu.VMEM((2, piece, d_model), bf16), pltpu.VMEM((2, piece, d_model), bf16),
            pltpu.VMEM((1, d_model), f32), pltpu.VMEM((n_dev, 8, own_rows), f32), pltpu.VMEM((n_dev, 8, own_rows), f32),
            dma((4,)), dma((4,)), dma((4,)), dma((3, 3)), dma((3, 3)), dma((2, 3)), dma((2, 2)),
            dma((n_dev,)), dma((n_dev,)), dma, dma((n_dev,)), dma((n_dev,)), dma((3,)), dma((3,)), dma((3,)),
        ],
        compiler_params=pltpu.CompilerParams(collective_id=0, has_side_effects=True, vmem_limit_bytes=67043328),
        cost_estimate=pl.CostEstimate(flops=12 * rows * d_model * d_model, bytes_accessed=64 * 1024 * 1024, transcendentals=0),
        name="tail",
    )(ht, *dys, *ws, x_bf, gy, g_norm[None], t_q, t_k)


def solution(mesh):
    n_dev = mesh.shape['sp']
    exchange = functools.partial(lax.all_to_all, axis_name='sp', split_axis=0, concat_axis=0, tiled=True)

    def device_step(x_loc, gy_loc, pos_loc, g_norm, w_query, w_key, w_value, w_out, g_query, g_key):
        n_batch, loc_len, d_model = x_loc.shape
        rows = n_batch * loc_len
        x_bf, cos_sin, q_rot, k_rot, v_val, h_t, q1, k1 = front(n_dev, x_loc, pos_loc, g_norm, g_query, g_key, w_query, w_key, w_value)
        gy_late, q_rot = lax.optimization_barrier((gy_loc, q_rot))
        gy = exchange(gy_late).reshape(rows, d_model)
        attended, a_t, lse = attend_forward(q_rot, k_rot, v_val)
        y_seq = (x_bf.astype(jnp.float32) + dot_nn(attended, w_out)).astype(jnp.bfloat16)
        y_out, grad_wo, dq_bf, dk_bf, d_v, t_q, t_k = middle(n_dev, y_seq, a_t, gy, w_out, q_rot, k_rot, v_val, q1, k1, cos_sin, lse, g_query, g_key)
        grad_wv, grad_wk, grad_wq, grad_x, gains = tail(n_dev, h_t, (d_v, dk_bf, dq_bf), (w_value, w_key, w_query), x_bf, gy, g_norm, t_q, t_k)
        return y_out, grad_x, gains[0], grad_wq, grad_wk, grad_wv, grad_wo, gains[1], gains[2]

    seq_spec = P('dp', 'sp', None)
    mat_rep = P(None, None)
    vec_rep = P(None)
    row_spec = P(('dp', 'sp'), None)
    vec_spec = P(('dp', 'sp'))
    return jax.shard_map(device_step, mesh=mesh, in_specs=(seq_spec, seq_spec, P('dp', 'sp'), vec_rep, mat_rep, mat_rep, mat_rep, mat_rep, vec_rep, vec_rep), out_specs=(seq_spec, seq_spec, vec_spec, row_spec, row_spec, row_spec, row_spec, vec_spec, vec_spec), check_vma=False)
```

```python
import functools
import math
import jax
import jax.numpy as jnp
from jax import lax
from jax.experimental import pallas as pl
from jax.experimental.pallas import tpu as pltpu
from jax.sharding import PartitionSpec as P

HEAD_DIM = 128
NORM_EPS = 1e-5
ROPE_BASE = 10000.0
NEG_BIG = -1e30
LOG2E = math.log2(math.e)
Q_BLOCK = 256


def rope_table(n_pos):
    half_dim = HEAD_DIM // 2
    inv_freq = ROPE_BASE ** (-jnp.arange(half_dim, dtype=jnp.float32) * (2.0 / HEAD_DIM))
    angles = jnp.arange(n_pos, dtype=jnp.float32)[:, None] * inv_freq
    cos_h, sin_h = jnp.cos(angles), jnp.sin(angles)
    table = jnp.concatenate([cos_h, cos_h, -sin_h, sin_h], axis=1)
    parts = []
    for _ in range(3):
        part = lax.reduce_precision(table, 8, 7)
        parts.append(part.astype(jnp.bfloat16))
        table = table - part
    return jnp.stack(parts)


def dot_nn(a, b):
    return lax.dot_general(a, b, (((1,), (0,)), ((), ())), preferred_element_type=jnp.float32)


def dot_nt(a, b):
    return lax.dot_general(a, b, (((1,), (1,)), ((), ())), preferred_element_type=jnp.float32)


def dot_tn(a, b):
    return lax.dot_general(a, b, (((0,), (0,)), ((), ())), preferred_element_type=jnp.float32)


def attend_head(seq_len, load_q, load_k, load_v, store):
    scale2 = LOG2E * HEAD_DIM ** -0.5
    for start in range(0, seq_len, Q_BLOCK):
        stop = start + Q_BLOCK
        q_blk = load_q(start, stop)
        s_diag = dot_nt(load_k(start, stop), q_blk)
        key_i = lax.broadcasted_iota(jnp.int32, s_diag.shape, 0)
        qry_i = lax.broadcasted_iota(jnp.int32, s_diag.shape, 1)
        s_diag = jnp.where(key_i <= qry_i, s_diag, NEG_BIG)
        m = jnp.max(s_diag, axis=0, keepdims=True)
        if start:
            s_past = dot_nt(load_k(0, start), q_blk)
            m = jnp.maximum(m, jnp.max(s_past, axis=0, keepdims=True))
        m2 = m * scale2
        p_diag = jnp.exp2(s_diag * scale2 - m2)
        l = jnp.sum(p_diag, axis=0, keepdims=True)
        acc = dot_tn(load_v(start, stop), p_diag.astype(jnp.bfloat16))
        if start:
            p_past = jnp.exp2(s_past * scale2 - m2)
            l = l + jnp.sum(p_past, axis=0, keepdims=True)
            acc = acc + dot_tn(load_v(0, start), p_past.astype(jnp.bfloat16))
        store(start, stop, acc / l, m2 + jnp.log2(l))


MESH = pl.DeviceIdType.MESH
ROW_BLOCK = 256


def row_inv(values):
    return lax.rsqrt(jnp.mean(values * values, axis=-1, keepdims=True) + NORM_EPS)


def front_kernel(n_dev, x_loc, gy_loc, pos_loc, tab_ref, g_ref, wq_ref, wk_ref, wv_ref,
                 x_seq, gy_seq, cs_ref, q_ref, k_ref, v_ref, ht_ref, ht_par, q1_ref, k1_ref, a_ref, at_ref, lse_ref,
                 xv, posv, wbuf, csb, qb, kb, vb, htb, q1b, k1b, ab, atb,
                 w_sem, x_send, x_recv, g_send, g_recv, p_send, p_recv, own_sem, xs_sem, out_sem, hp_send, hp_recv, a_sem):
    me = lax.axis_index('sp')
    chip, core = me // 2, me % 2
    n_chips = n_dev // 2
    piece = x_loc.shape[1]
    blk = 2 * piece
    n_pos = tab_ref.shape[1]
    d_model = x_loc.shape[2]

    for cp in [pltpu.make_async_copy(w, wbuf.at[i], w_sem.at[i]) for i, w in enumerate((wv_ref, wq_ref, wk_ref))]:
        cp.start()
    mine = pl.ds(pl.multiple_of(me * piece, piece), piece)
    own = [pltpu.make_async_copy(x_loc.at[me], xv.at[mine, :], own_sem.at[0]), pltpu.make_async_copy(pos_loc.at[me], posv.at[me], own_sem.at[1])]
    own_gy = pltpu.make_async_copy(gy_loc.at[me], gy_seq.at[me], own_sem.at[2])
    for cp in own + [own_gy]:
        cp.start()

    barrier = pltpu.get_barrier_semaphore()
    for off in range(1, n_dev):
        pl.semaphore_signal(barrier, inc=1, device_id={'sp': lax.rem(me + off, n_dev)}, device_id_type=MESH)
    pl.semaphore_wait(barrier, n_dev - 1)

    sends = []
    dests = [2 * chip + 1 - core]
    for hop in (1, n_chips - 1, 2):
        dests += [2 * lax.rem(chip + hop, n_chips) + lax.rem(core + flip, 2) for flip in range(2)]
    for i, dest in enumerate(dests):
        sends.append(pltpu.make_async_remote_copy(src_ref=pos_loc.at[dest], dst_ref=posv.at[me], send_sem=p_send.at[i], recv_sem=p_recv.at[me],
                                                  device_id={'sp': dest}, device_id_type=MESH))
        sends.append(pltpu.make_async_remote_copy(src_ref=x_loc.at[dest], dst_ref=xv.at[mine, :], send_sem=x_send.at[i], recv_sem=x_recv.at[me],
                                                  device_id={'sp': dest}, device_id_type=MESH))
    gy_sends = [pltpu.make_async_remote_copy(src_ref=gy_loc.at[dest], dst_ref=gy_seq.at[me], send_sem=g_send.at[i], recv_sem=g_recv.at[me],
                                             device_id={'sp': dest}, device_id_type=MESH) for i, dest in enumerate(dests)]
    for cp in sends + gy_sends:
        cp.start()

    def arrival(src):
        at = pl.ds(pl.multiple_of(src * piece, piece), piece)
        return (pltpu.make_async_remote_copy(src_ref=x_loc.at[src], dst_ref=xv.at[at, :], send_sem=x_send.at[0], recv_sem=x_recv.at[src],
                                             device_id={'sp': src}, device_id_type=MESH),
                pltpu.make_async_remote_copy(src_ref=pos_loc.at[src], dst_ref=posv.at[src], send_sem=p_send.at[0], recv_sem=p_recv.at[src],
                                             device_id={'sp': src}, device_id_type=MESH))

    def outs(at, slot):
        rows = pl.ds(pl.multiple_of(at, blk), blk)
        pairs = [(csb.at[slot], cs_ref.at[rows, :]), (qb.at[rows, :], q_ref.at[rows, :]), (kb.at[rows, :], k_ref.at[rows, :]), (vb.at[rows, :], v_ref.at[rows, :]),
                 (htb.at[slot], ht_ref.at[:, rows]), (q1b.at[slot], q1_ref.at[rows, :]), (k1b.at[slot], k1_ref.at[rows, :])]
        return [pltpu.make_async_copy(s, d, out_sem.at[slot, i]) for i, (s, d) in enumerate(pairs)]

    def ht_send(at, slot, b):
        cols = pl.ds(pl.multiple_of(at, blk), blk)
        return pltpu.make_async_remote_copy(src_ref=htb.at[slot], dst_ref=ht_par.at[:, cols], send_sem=hp_send.at[slot], recv_sem=hp_recv.at[b],
                                            device_id={'sp': 2 * chip + 1 - core}, device_id_type=MESH)

    def x_out(src_chip):
        rows = pl.ds(pl.multiple_of(src_chip * blk, blk), blk)
        return pltpu.make_async_copy(xv.at[rows, :], x_seq.at[rows, :], xs_sem.at[src_chip])

    def block(b, carry):
        hop = b + (b // 2) * (5 - 2 * b)
        src_chip = lax.rem(chip + hop, n_chips)
        at = pl.multiple_of(src_chip * blk, blk)
        slot = lax.rem(b, 2)

        @pl.when(b == 0)
        def _():
            for cp in own:
                cp.wait()
            for cp in arrival(2 * chip + 1 - core):
                cp.wait_recv()

        @pl.when(b > 0)
        def _():
            for e in range(2):
                for cp in arrival(2 * src_chip + e):
                    cp.wait_recv()

        x_out(src_chip).start()

        @pl.when(b >= 2)
        def _():
            for cp in outs(at, slot):
                cp.wait()
            ht_send(at, slot, b).wait_send()

        for e in range(2):
            hot = (lax.broadcasted_iota(jnp.int32, (n_pos, piece), 0) == posv[2 * src_chip + e]).astype(jnp.bfloat16)
            csb[slot, e * piece:(e + 1) * piece, :] = (dot_tn(hot, tab_ref[0]) + dot_tn(hot, tab_ref[1])) + dot_tn(hot, tab_ref[2])
        x_f = xv[pl.ds(at, blk), :].astype(jnp.float32)
        hidden = (x_f * row_inv(x_f) * g_ref[0:1, :].astype(jnp.float32)).astype(jnp.bfloat16)
        htb[slot] = hidden.T

        @pl.when(b == 0)
        def _():
            for i, w in enumerate((wv_ref, wq_ref, wk_ref)):
                pltpu.make_async_copy(w, wbuf.at[i], w_sem.at[i]).wait()

        vb[pl.ds(at, blk), :] = dot_nn(hidden, wbuf[0]).astype(jnp.bfloat16)
        cos_t, sin_t = csb[slot, :, 0:HEAD_DIM], csb[slot, :, HEAD_DIM:2 * HEAD_DIM]
        for i, raw_ref, out_ref in ((1, q1b, qb), (2, k1b, kb)):
            raw_ref[slot] = dot_nn(hidden, wbuf[i])
            inv = row_inv(raw_ref[slot])
            for c in range(0, d_model, HEAD_DIM):
                u = raw_ref[slot, :, c:c + HEAD_DIM] * inv * g_ref[i:i + 1, c:c + HEAD_DIM].astype(jnp.float32)
                out_ref[pl.ds(at, blk), c:c + HEAD_DIM] = (u * cos_t + pltpu.roll(u, HEAD_DIM // 2, 1) * sin_t).astype(jnp.bfloat16)
        for cp in outs(at, slot):
            cp.start()
        ht_send(at, slot, b).start()
        return carry

    lax.fori_loop(0, n_chips, block, 0)

    def a_copies(h, slot):
        cols = pl.ds(pl.multiple_of(h * HEAD_DIM, HEAD_DIM), HEAD_DIM)
        return (pltpu.make_async_copy(ab.at[slot], a_ref.at[:, cols], a_sem.at[slot, 0]), pltpu.make_async_copy(atb.at[slot], at_ref.at[cols, :], a_sem.at[slot, 1]))

    def head(h, carry):
        slot = lax.rem(h, 2)
        cols = pl.ds(pl.multiple_of(h * HEAD_DIM, HEAD_DIM), HEAD_DIM)

        @pl.when(h >= 2)
        def _():
            for cp in a_copies(h, slot):
                cp.wait()

        def store(start, stop, out, lse):
            atb[slot, :, start:stop] = out.astype(jnp.bfloat16)
            ab[slot, start:stop, :] = out.T.astype(jnp.bfloat16)
            lse_ref[h, :, start:stop] = lse

        attend_head(n_dev * piece, lambda i, j: qb[i:j, cols], lambda i, j: kb[i:j, cols], lambda i, j: vb[i:j, cols], store)
        for cp in a_copies(h, slot):
            cp.start()
        return carry

    lax.fori_loop(0, d_model // HEAD_DIM, head, 0)
    for slot in range(2):
        for cp in outs(0, slot) + list(a_copies(0, slot)):
            cp.wait()
        ht_send(0, slot, 0).wait_send()
    for i in range(n_chips):
        x_out(i).wait()
        ht_send(0, 0, i).wait_recv()
    for cp in sends:
        cp.wait_send()
    own_gy.wait()
    for i, cp in enumerate(gy_sends):
        cp.wait_send()
        src = dests[i]
        pltpu.make_async_remote_copy(src_ref=gy_loc.at[src], dst_ref=gy_seq.at[src], send_sem=g_send.at[0], recv_sem=g_recv.at[src],
                                     device_id={'sp': src}, device_id_type=MESH).wait_recv()


def front(n_dev, x_loc, gy_loc, pos_loc, gains, w_query, w_key, w_value):
    n_batch, piece, d_model = x_loc.shape
    rows, blk = n_batch * piece, 2 * piece
    hbm = pl.BlockSpec(memory_space=pl.ANY)
    vmem = pl.BlockSpec(memory_space=pltpu.VMEM)
    bf16, f32 = jnp.bfloat16, jnp.float32
    act = jax.ShapeDtypeStruct((rows, d_model), bf16)
    raw = jax.ShapeDtypeStruct((rows, d_model), f32)
    turned = jax.ShapeDtypeStruct((d_model, rows), bf16)
    dma = pltpu.SemaphoreType.DMA
    whole = pltpu.VMEM((rows, d_model), bf16)
    return pl.pallas_call(
        functools.partial(front_kernel, n_dev),
        out_shape=(act, jax.ShapeDtypeStruct(x_loc.shape, bf16), jax.ShapeDtypeStruct((rows, 2 * HEAD_DIM), f32), act, act, act, turned, turned, raw, raw, act, turned,
                   jax.ShapeDtypeStruct((d_model // HEAD_DIM, 1, rows), f32)),
        in_specs=[hbm] * 3 + [vmem] * 2 + [hbm] * 3,
        out_specs=(hbm,) * 12 + (vmem,),
        scratch_shapes=[
            pltpu.VMEM((rows, d_model), bf16), pltpu.VMEM((n_dev, 1, piece), jnp.int32), pltpu.VMEM((3, d_model, d_model), bf16),
            pltpu.VMEM((2, blk, 2 * HEAD_DIM), f32), whole, whole, whole, pltpu.VMEM((2, d_model, blk), bf16),
            pltpu.VMEM((2, blk, d_model), f32), pltpu.VMEM((2, blk, d_model), f32),
            pltpu.VMEM((2, rows, HEAD_DIM), bf16), pltpu.VMEM((2, HEAD_DIM, rows), bf16),
            dma((3,)), dma((n_dev,)), dma((n_dev,)), dma((n_dev,)), dma((n_dev,)), dma((n_dev,)), dma((n_dev,)), dma((3,)), dma((n_dev // 2,)), dma((2, 7)), dma((2,)), dma((n_dev // 2,)), dma((2, 2)),
        ],
        compiler_params=pltpu.CompilerParams(collective_id=1, has_side_effects=True, vmem_limit_bytes=67043328),
        cost_estimate=pl.CostEstimate(flops=6 * rows * d_model * d_model, bytes_accessed=60 * 1024 * 1024, transcendentals=0),
        name="front",
    )(x_loc, gy_loc, pos_loc[:, None, :], rope_table(rows), gains, w_query, w_key, w_value)


def middle_kernel(n_dev, a_seq, x_home, at_ref, gy_ref, wo_ref, q_ref, k_ref, v_ref, q1_ref, k1_ref, cs_ref, lse_ref, g_ref,
                  y_out, a_home, gw_ref, dq_ref, dk_ref, dv_ref, tq_ref, tk_ref,
                  wo, at_own, at_par, gy_own, gy_par, rs, dqk, hbuf, dvb, dob, dk_acc, dv_acc, rawb, tmp, nrm, ahb, xhb, yb,
                  load_sem, y_send, y_recv, y_loc, part_send, part_recv, rs_send, rs_recv, h_sem, dv_sem, raw_sem, dqk_sem,
                  fin_loc, fin_send, fin_recv, ax_sem, yo_sem):
    me = lax.axis_index('sp')
    chip, core = me // 2, me % 2
    n_chips = n_dev // 2
    step_dir = 1 - 2 * core
    partner = me + step_dir
    right = 2 * lax.rem(chip + step_dir + n_chips, n_chips) + core
    rows, d_model = gy_ref.shape
    n_heads = d_model // HEAD_DIM
    half, sub = d_model // 2, d_model // 4
    piece, chunk, own_rows = rows // n_dev, d_model // n_chips, d_model // n_dev
    other = pl.ds(pl.multiple_of((1 - core) * half, half), half)

    loads = [pltpu.make_async_copy(s, d, load_sem.at[i]) for i, (s, d) in enumerate(((at_ref, at_own), (gy_ref, gy_own), (wo_ref, wo)))]
    for cp in loads:
        cp.start()

    def head_copies(h, slot):
        cols = pl.ds(pl.multiple_of(h * HEAD_DIM, HEAD_DIM), HEAD_DIM)
        return [pltpu.make_async_copy(r.at[:, cols], hbuf.at[slot, i], h_sem.at[slot, i]) for i, r in enumerate((q_ref, k_ref, v_ref))]

    for cp in head_copies(0, 0):
        cp.start()

    barrier = pltpu.get_barrier_semaphore()
    for off in range(1, n_dev):
        pl.semaphore_signal(barrier, inc=1, device_id={'sp': lax.rem(me + off, n_dev)}, device_id_type=MESH)
    pl.semaphore_wait(barrier, n_dev - 1)

    parts = [pltpu.make_async_remote_copy(src_ref=s, dst_ref=d, send_sem=part_send.at[i], recv_sem=part_recv.at[i], device_id={'sp': partner}, device_id_type=MESH)
             for i, (s, d) in enumerate(((at_ref, at_par), (gy_ref.at[:, other], gy_par)))]
    for cp in parts:
        cp.start()

    def rs_copy(ch, s):
        return pltpu.make_async_remote_copy(src_ref=rs.at[ch, s], dst_ref=rs.at[ch, s + 1], send_sem=rs_send.at[ch, s], recv_sem=rs_recv.at[ch, s],
                                            device_id={'sp': right}, device_id_type=MESH)

    n_tile = 256

    def ring_step(ch, s):
        owner = lax.rem(chip - step_dir * (1 + s) + 2 * n_chips, n_chips)
        row_at = pl.ds(pl.multiple_of(owner * chunk, chunk), chunk)

        def tile(t, carry):
            col = pl.multiple_of(t * n_tile, n_tile)
            in_half = pl.multiple_of(ch * sub + col, n_tile)
            term = dot_nn(at_own[row_at, :], gy_own[:, pl.ds(pl.multiple_of(core * half + in_half, n_tile), n_tile)])
            term = term + dot_nn(at_par[row_at, :], gy_par[:, pl.ds(in_half, n_tile)])

            @pl.when(s == 0)
            def _():
                rs[ch, s, :, pl.ds(col, n_tile)] = term

            @pl.when(s > 0)
            def _():
                rs[ch, s, :, pl.ds(col, n_tile)] += term

            return carry

        lax.fori_loop(0, sub // n_tile, tile, 0)

    def ring(i):
        ch, s = lax.rem(i, 2), i // 2

        @pl.when(s > 0)
        def _():
            rs_copy(ch, s - 1).wait_recv()

        ring_step(ch, s)

        @pl.when(s < N_SLOTS - 1)
        def _():
            rs_copy(ch, s).start()

    def y_remote(off):
        dest = lax.rem(me + off, n_dev)
        return pltpu.make_async_remote_copy(src_ref=a_seq.at[dest], dst_ref=a_home.at[me], send_sem=y_send.at[off], recv_sem=y_recv.at[off],
                                            device_id={'sp': dest}, device_id_type=MESH)

    y_own = pltpu.make_async_copy(a_seq.at[me], a_home.at[me], y_loc)
    for off in range(1, n_dev):
        y_remote(off).start()
    y_own.start()

    def finish_out(ch):
        keep = pl.ds(pl.multiple_of(core * own_rows, own_rows), own_rows)
        give = pl.ds(pl.multiple_of((1 - core) * own_rows, own_rows), own_rows)
        cols = pl.ds(pl.multiple_of(core * half + ch * sub, sub), sub)
        loc = pltpu.make_async_copy(rs.at[ch, N_SLOTS - 1, keep, :], gw_ref.at[:, cols], fin_loc.at[ch])
        rem = pltpu.make_async_remote_copy(src_ref=rs.at[ch, N_SLOTS - 1, give, :], dst_ref=gw_ref.at[:, cols], send_sem=fin_send.at[ch], recv_sem=fin_recv.at[ch],
                                           device_id={'sp': partner}, device_id_type=MESH)
        return loc, rem

    scale = HEAD_DIM ** -0.5
    scale2 = LOG2E * scale

    def dv_copy(h, slot):
        cols = pl.ds(pl.multiple_of(h * HEAD_DIM, HEAD_DIM), HEAD_DIM)
        return pltpu.make_async_copy(dvb.at[slot], dv_ref.at[:, cols], dv_sem.at[slot])

    def head(h, carry):
        slot = lax.rem(h, 2)
        cols = pl.ds(pl.multiple_of(h * HEAD_DIM, HEAD_DIM), HEAD_DIM)
        in_pair = pl.ds(pl.multiple_of(slot * HEAD_DIM, HEAD_DIM), HEAD_DIM)

        @pl.when(slot == 0)
        def _():
            def do_tile(t, c2):
                ra = pl.ds(pl.multiple_of(t * 256, 256), 256)
                dob[ra, :] = dot_nt(gy_own[ra, :], wo[pl.ds(pl.multiple_of(h * HEAD_DIM, 2 * HEAD_DIM), 2 * HEAD_DIM), :]).astype(jnp.bfloat16)
                return c2

            lax.fori_loop(0, rows // 256, do_tile, 0)

        for cp in head_copies(h, slot):
            cp.wait()

        @pl.when(h + 1 < n_heads)
        def _():
            for cp in head_copies(h + 1, 1 - slot):
                cp.start()

        dk_acc[...] = jnp.zeros_like(dk_acc)
        dv_acc[...] = jnp.zeros_like(dv_acc)
        for start in range(0, rows, Q_BLOCK):
            stop = start + Q_BLOCK
            q_blk = hbuf[slot, 0, start:stop, :]
            do_blk = dob[start:stop, in_pair]
            lse = lse_ref[h, :, start:stop]
            k_all = hbuf[slot, 1, 0:stop, :]
            p = jnp.exp2(dot_nt(k_all, q_blk) * scale2 - lse)
            key_i = lax.broadcasted_iota(jnp.int32, (Q_BLOCK, Q_BLOCK), 0)
            qry_i = lax.broadcasted_iota(jnp.int32, (Q_BLOCK, Q_BLOCK), 1)
            p_diag = jnp.where(key_i <= qry_i, p[start:stop, :], 0.0)
            p = jnp.concatenate([p[0:start, :], p_diag], axis=0) if start else p_diag
            dp = dot_nt(hbuf[slot, 2, 0:stop, :], do_blk)
            delta = jnp.sum(p * dp, axis=0, keepdims=True)
            ds = (p * (dp - delta) * scale).astype(jnp.bfloat16)
            dv_acc[0:stop, :] += dot_nn(p.astype(jnp.bfloat16), do_blk)
            dk_acc[0:stop, :] += dot_nn(ds, q_blk)
            dqk[0, start:stop, cols] = dot_tn(k_all, ds).T.astype(jnp.bfloat16)
        dqk[1, :, cols] = dk_acc[...].astype(jnp.bfloat16)

        @pl.when(h >= 2)
        def _():
            dv_copy(h, slot).wait()

        dvb[slot] = dv_acc[...].astype(jnp.bfloat16)
        dv_copy(h, slot).start()

        ring_from = n_heads - 6

        @pl.when(jnp.logical_and(h >= ring_from, lax.rem(h - ring_from, 2) == 1))
        def _():
            ring(2 + (h - ring_from) // 2)

        return carry

    loads[0].wait()
    loads[1].wait()
    for cp in parts:
        cp.wait_recv()
    for i in range(2):
        ring(i)
    loads[2].wait()
    lax.fori_loop(0, n_heads, head, 0)
    for slot in range(2):
        dv_copy(0, slot).wait()

    for off in range(1, n_dev):
        y_remote(off).wait()
    y_own.wait()

    def home_in(b, slot):
        return (pltpu.make_async_copy(a_home.at[b], ahb.at[slot], ax_sem.at[slot, 0]), pltpu.make_async_copy(x_home.at[b], xhb.at[slot], ax_sem.at[slot, 1]))

    def y_copy(b, slot):
        return pltpu.make_async_copy(yb.at[slot], y_out.at[b], yo_sem.at[slot])

    def y_rows(b, carry):
        slot = lax.rem(b, 2)
        for cp in home_in(b, slot):
            cp.wait()

        @pl.when(b + 1 < n_dev)
        def _():
            for cp in home_in(b + 1, 1 - slot):
                cp.start()

        @pl.when(b >= 2)
        def _():
            y_copy(b, slot).wait()

        yb[slot] = (xhb[slot].astype(jnp.float32) + dot_nn(ahb[slot], wo[...])).astype(jnp.bfloat16)
        y_copy(b, slot).start()
        return carry

    def raw_copy(i, b, slot):
        src = (q1_ref, k1_ref)[i]
        return pltpu.make_async_copy(src.at[pl.ds(pl.multiple_of(b * piece, piece), piece), :], rawb.at[slot], raw_sem.at[slot])

    for i, t_ref in ((0, tq_ref), (1, tk_ref)):
        t_ref[...] = jnp.zeros_like(t_ref)
        raw_copy(i, 0, 0).start()

        def norm_rows(b, carry):
            slot = lax.rem(b, 2)
            raw_copy(i, b, slot).wait()

            @pl.when(b + 1 < n_dev)
            def _():
                raw_copy(i, b + 1, 1 - slot).start()

            at = pl.ds(pl.multiple_of(b * piece, piece), piece)
            inv = row_inv(rawb[slot])
            cos_t, sin_t = cs_ref[at, 0:HEAD_DIM], cs_ref[at, HEAD_DIM:2 * HEAD_DIM]
            total = jnp.zeros((piece, HEAD_DIM), jnp.float32)
            for c in range(0, d_model, HEAD_DIM):
                d_u = dqk[i, at, c:c + HEAD_DIM].astype(jnp.float32)
                d_n = d_u * cos_t - pltpu.roll(d_u, HEAD_DIM // 2, 1) * sin_t
                hat = rawb[slot, :, c:c + HEAD_DIM] * inv
                t_ref[:, c:c + HEAD_DIM] += jnp.sum(d_n * hat, axis=0, keepdims=True)
                d_n = d_n * g_ref[i + 1:i + 2, c:c + HEAD_DIM].astype(jnp.float32)
                total = total + d_n * hat
                tmp[:, c:c + HEAD_DIM] = d_n
                nrm[:, c:c + HEAD_DIM] = hat
            mean = jnp.sum(total, axis=-1, keepdims=True) * (1.0 / d_model)
            for c in range(0, d_model, HEAD_DIM):
                dqk[i, at, c:c + HEAD_DIM] = (inv * (tmp[:, c:c + HEAD_DIM] - nrm[:, c:c + HEAD_DIM] * mean)).astype(jnp.bfloat16)
            return carry

        lax.fori_loop(0, n_dev, norm_rows, 0)
        pltpu.make_async_copy(dqk.at[i], (dq_ref, dk_ref)[i], dqk_sem.at[i]).start()
        if i == 0:
            ring(jnp.int32(5))
            for cp in home_in(0, 0):
                cp.start()
            lax.fori_loop(0, n_dev, y_rows, 0)

    for ch in range(2):
        ring(jnp.int32(6 + ch))
        for cp in finish_out(ch):
            cp.start()
    for slot in range(2):
        y_copy(0, slot).wait()
    for cp in parts:
        cp.wait_send()
    for ch in range(2):
        for s in range(N_SLOTS - 1):
            rs_copy(ch, s).wait_send()
    for i in range(2):
        pltpu.make_async_copy(dqk.at[i], (dq_ref, dk_ref)[i], dqk_sem.at[i]).wait()
    for ch in range(2):
        loc, rem = finish_out(ch)
        loc.wait()
        rem.wait()


def middle(n_dev, a_seq, x_home, a_t, gy, w_out, q_rot, k_rot, v_val, q1, k1, cos_sin, lse, gains):
    rows, d_model = gy.shape
    piece, chunk, own_rows, sub = rows // n_dev, d_model // (n_dev // 2), d_model // n_dev, d_model // 4
    hbm = pl.BlockSpec(memory_space=pl.ANY)
    vmem = pl.BlockSpec(memory_space=pltpu.VMEM)
    f32, bf16 = jnp.float32, jnp.bfloat16
    act = jax.ShapeDtypeStruct((rows, d_model), bf16)
    vec = jax.ShapeDtypeStruct((1, d_model), f32)
    dma = pltpu.SemaphoreType.DMA
    return pl.pallas_call(
        functools.partial(middle_kernel, n_dev),
        out_shape=(jax.ShapeDtypeStruct((n_dev, piece, d_model), bf16), jax.ShapeDtypeStruct((n_dev, piece, d_model), bf16), jax.ShapeDtypeStruct((own_rows, d_model), f32), act, act, act, vec, vec),
        in_specs=[hbm] * 10 + [vmem] * 3,
        out_specs=(hbm,) * 6 + (vmem,) * 2,
        scratch_shapes=[
            pltpu.VMEM((d_model, d_model), bf16), pltpu.VMEM((d_model, rows), bf16), pltpu.VMEM((d_model, rows), bf16),
            pltpu.VMEM((rows, d_model), bf16), pltpu.VMEM((rows, d_model // 2), bf16),
            pltpu.VMEM((2, N_SLOTS, chunk, sub), f32), pltpu.VMEM((2, rows, d_model), bf16),
            pltpu.VMEM((2, 3, rows, HEAD_DIM), bf16), pltpu.VMEM((2, rows, HEAD_DIM), bf16), pltpu.VMEM((rows, 2 * HEAD_DIM), bf16),
            pltpu.VMEM((rows, HEAD_DIM), f32), pltpu.VMEM((rows, HEAD_DIM), f32),
            pltpu.VMEM((2, piece, d_model), f32), pltpu.VMEM((piece, d_model), f32), pltpu.VMEM((piece, d_model), f32),
            pltpu.VMEM((2, piece, d_model), bf16), pltpu.VMEM((2, piece, d_model), bf16), pltpu.VMEM((2, piece, d_model), bf16),
            dma((3,)), dma((n_dev,)), dma((n_dev,)), dma, dma((2,)), dma((2,)), dma((2, 3)), dma((2, 3)), dma((2, 3)), dma((2,)), dma((2,)), dma((2,)),
            dma((2,)), dma((2,)), dma((2,)), dma((2, 2)), dma((2,)),
        ],
        compiler_params=pltpu.CompilerParams(collective_id=2, has_side_effects=True, vmem_limit_bytes=67043328),
        cost_estimate=pl.CostEstimate(flops=12 * rows * rows * d_model, bytes_accessed=64 * 1024 * 1024, transcendentals=0),
        name="middle",
    )(a_seq.reshape(n_dev, piece, d_model), x_home, a_t, gy, w_out, q_rot, k_rot, v_val, q1, k1, cos_sin, lse, gains)


N_SLOTS = 4


def tail_kernel(n_dev, ht_ref, htp_ref, dy_v, dy_k, dy_q, w_v, w_k, w_q, x_ref, gy_ref, gn_ref, tq_ref, tk_ref,
                gw_v, gw_k, gw_q, gx_ref, gain_ref,
                ht_own, ht_par, dy_own, dy_par, rs, dh, wbuf, xbuf, gybuf, n_acc, gsend, grecv,
                load_sem, part_send, part_recv, rs_send, rs_recv, w_sem, xy_sem, gx_send, gx_recv, gx_loc,
                gain_send, gain_recv, fin_loc, fin_send, fin_recv):
    me = lax.axis_index('sp')
    chip, core = me // 2, me % 2
    n_chips = n_dev // 2
    step_dir = 1 - 2 * core
    partner = me + step_dir
    right = 2 * lax.rem(chip + step_dir + n_chips, n_chips) + core
    rows, d_model = x_ref.shape
    half = d_model // 2
    piece = rows // n_dev
    chunk = d_model // n_chips
    own_rows = d_model // n_dev
    dys, ws, gws = (dy_v, dy_k, dy_q), (w_v, w_k, w_q), (gw_v, gw_k, gw_q)
    mine = pl.ds(pl.multiple_of(core * half, half), half)
    other = pl.ds(pl.multiple_of((1 - core) * half, half), half)

    loads = [pltpu.make_async_copy(dys[i], dy_own.at[i], load_sem.at[i]) for i in range(3)]
    loads[1:1] = [pltpu.make_async_copy(ht_ref, ht_own, load_sem.at[3]), pltpu.make_async_copy(htp_ref, ht_par, load_sem.at[4])]
    for cp in loads:
        cp.start()

    barrier = pltpu.get_barrier_semaphore()
    for off in range(1, n_dev):
        pl.semaphore_signal(barrier, inc=1, device_id={'sp': lax.rem(me + off, n_dev)}, device_id_type=MESH)
    pl.semaphore_wait(barrier, n_dev - 1)

    def to_partner(src, dst, idx):
        return pltpu.make_async_remote_copy(src_ref=src, dst_ref=dst, send_sem=part_send.at[idx], recv_sem=part_recv.at[idx],
                                            device_id={'sp': partner}, device_id_type=MESH)

    parts = [to_partner(dys[i].at[:, other], dy_par.at[i], i) for i in range(3)]
    for cp in parts:
        cp.start()

    def rs_copy(w, s):
        return pltpu.make_async_remote_copy(src_ref=rs.at[w, s], dst_ref=rs.at[w, s + 1], send_sem=rs_send.at[w, s], recv_sem=rs_recv.at[w, s],
                                            device_id={'sp': right}, device_id_type=MESH)

    n_tile = 256

    def ring_step(w, s):
        owner = lax.rem(chip - step_dir * (1 + s) + 2 * n_chips, n_chips)
        row_at = pl.multiple_of(owner * chunk, chunk)

        def tile(t, carry):
            col = pl.multiple_of(t * n_tile, n_tile)
            term = dot_nn(ht_own[pl.ds(row_at, chunk), :], dy_own[w, :, pl.ds(pl.multiple_of(core * half + col, n_tile), n_tile)])
            term = term + dot_nn(ht_par[pl.ds(row_at, chunk), :], dy_par[w, :, pl.ds(col, n_tile)])

            @pl.when(s == 0)
            def _():
                rs[w, s, :, pl.ds(col, n_tile)] = term

            @pl.when(s > 0)
            def _():
                rs[w, s, :, pl.ds(col, n_tile)] += term

            return carry

        lax.fori_loop(0, half // n_tile, tile, 0)

    def w_copy(i, n, slot):
        return pltpu.make_async_copy(ws[i].at[pl.ds(pl.multiple_of(n * n_tile, n_tile), n_tile), :], wbuf.at[slot, i], w_sem.at[slot, i])

    def dh_block(n):
        slot = lax.rem(n, 2)
        for i in range(3):
            w_copy(i, n, slot).wait()

        @pl.when(n + 1 < d_model // n_tile)
        def _():
            for i in range(3):
                w_copy(i, n + 1, 1 - slot).start()

        m_tile = 256

        def tile(t, carry):
            at = pl.ds(pl.multiple_of(t * m_tile, m_tile), m_tile)
            total = dot_nt(dy_own[0, at, :], wbuf[slot, 0]) + dot_nt(dy_own[1, at, :], wbuf[slot, 1]) + dot_nt(dy_own[2, at, :], wbuf[slot, 2])
            dh[at, pl.ds(pl.multiple_of(n * n_tile, n_tile), n_tile)] = total.astype(jnp.bfloat16)
            return carry

        lax.fori_loop(0, rows // m_tile, tile, 0)

    def xy_copies(p, slot):
        at = pl.ds(pl.multiple_of(p * piece, piece), piece)
        return (pltpu.make_async_copy(x_ref.at[at, :], xbuf.at[slot], xy_sem.at[slot, 0]),
                pltpu.make_async_copy(gy_ref.at[at, :], gybuf.at[slot], xy_sem.at[slot, 1]))

    def gx_remote(off):
        dest = lax.rem(me + off, n_dev)
        at = pl.ds(pl.multiple_of(dest * piece, piece), piece)
        return pltpu.make_async_remote_copy(src_ref=dh.at[at, :], dst_ref=gx_ref.at[me], send_sem=gx_send.at[off], recv_sem=gx_recv.at[off],
                                            device_id={'sp': dest}, device_id_type=MESH)

    def gx_own():
        at = pl.ds(pl.multiple_of(me * piece, piece), piece)
        return pltpu.make_async_copy(dh.at[at, :], gx_ref.at[me], gx_loc)

    def gain_copy(off):
        dest = lax.rem(me + off, n_dev)
        return pltpu.make_async_remote_copy(src_ref=gsend.at[dest], dst_ref=grecv.at[off], send_sem=gain_send.at[off], recv_sem=gain_recv.at[off],
                                            device_id={'sp': dest}, device_id_type=MESH)

    def grad_x_pieces():
        n_acc[...] = jnp.zeros_like(n_acc)
        for cp in xy_copies(0, 0):
            cp.start()

        def one(p, carry):
            slot = lax.rem(p, 2)
            for cp in xy_copies(p, slot):
                cp.wait()

            @pl.when(p + 1 < n_dev)
            def _():
                for cp in xy_copies(p + 1, 1 - slot):
                    cp.start()

            at = pl.ds(pl.multiple_of(p * piece, piece), piece)
            sub = 32

            def rows_of(j, c2):
                ra = pl.ds(pl.multiple_of(j * sub, sub), sub)
                rb = pl.ds(pl.multiple_of(p * piece + j * sub, sub), sub)
                x_f = xbuf[slot, ra, :].astype(jnp.float32)
                inv = row_inv(x_f)
                hat = x_f * inv
                d_h = dh[rb, :].astype(jnp.float32)
                n_acc[...] += jnp.sum(d_h * hat, axis=0, keepdims=True)
                d_n = d_h * gn_ref[0:1, :].astype(jnp.float32)
                mean = jnp.mean(d_n * hat, axis=-1, keepdims=True)
                out = gybuf[slot, ra, :].astype(jnp.float32) + inv * (d_n - hat * mean)
                dh[rb, :] = out.astype(jnp.bfloat16)
                return c2

            lax.fori_loop(0, piece // sub, rows_of, 0)
            return carry

        lax.fori_loop(0, n_dev, one, 0)
        for off in range(1, n_dev):
            gx_remote(off).start()
        gx_own().start()
        for d in range(n_dev):
            gsend[d] = jnp.zeros(gsend.shape[1:], jnp.float32)
            cols = slice(d * own_rows, (d + 1) * own_rows)
            gsend[d, 0:1, :] = n_acc[:, cols]
            gsend[d, 1:2, :] = tq_ref[:, cols]
            gsend[d, 2:3, :] = tk_ref[:, cols]
        for off in range(1, n_dev):
            gain_copy(off).start()

    def finish_out(w):
        keep = pl.ds(pl.multiple_of(core * own_rows, own_rows), own_rows)
        give = pl.ds(pl.multiple_of((1 - core) * own_rows, own_rows), own_rows)
        loc = pltpu.make_async_copy(rs.at[w, N_SLOTS - 1, keep, :], gws[w].at[:, mine], fin_loc.at[w])
        rem = pltpu.make_async_remote_copy(src_ref=rs.at[w, N_SLOTS - 1, give, :], dst_ref=gws[w].at[:, mine], send_sem=fin_send.at[w], recv_sem=fin_recv.at[w],
                                           device_id={'sp': partner}, device_id_type=MESH)
        return loc, rem

    for cp in loads[:3]:
        cp.wait()
    for i in range(3):
        w_copy(i, 0, 0).start()
    n_blocks = d_model // n_tile
    dh_from = 2

    def main(it, carry):
        s, w = it // 3, lax.rem(it, 3)

        @pl.when(s == 0)
        def _():
            pltpu.make_async_remote_copy(src_ref=dy_v.at[:, other], dst_ref=dy_par.at[w], send_sem=part_send.at[w], recv_sem=part_recv.at[w],
                                         device_id={'sp': partner}, device_id_type=MESH).wait_recv()

        @pl.when(jnp.logical_and(s == 0, w > 0))
        def _():
            pltpu.make_async_copy(dy_v, dy_own.at[w], load_sem.at[w]).wait()

        @pl.when(s > 0)
        def _():
            rs_copy(w, s - 1).wait_recv()

        ring_step(w, s)

        @pl.when(s < N_SLOTS - 1)
        def _():
            rs_copy(w, s).start()

        for j in range(2):
            blk_i = 2 * (it - dh_from) + j

            @pl.when(jnp.logical_and(blk_i >= 0, blk_i < n_blocks))
            def _():
                dh_block(blk_i)

        @pl.when(it == dh_from + n_blocks // 2)
        def _():
            grad_x_pieces()

        for i in range(3):
            @pl.when(jnp.logical_and(s == N_SLOTS - 1, w == i))
            def _():
                for cp in finish_out(i):
                    cp.start()

        return carry

    lax.fori_loop(0, 3 * N_SLOTS, main, 0)

    for cp in parts:
        cp.wait_send()

    def drain(it, carry):
        rs_copy(lax.rem(it, 3), it // 3).wait_send()
        return carry

    lax.fori_loop(0, 3 * (N_SLOTS - 1), drain, 0)
    for off in range(1, n_dev):
        gain_copy(off).wait()
    total = gsend[me]
    for off in range(1, n_dev):
        total = total + grecv[off]
    gain_ref[...] = total
    for off in range(1, n_dev):
        gx_remote(off).wait()
    gx_own().wait()
    for i in range(3):
        loc, rem = finish_out(i)
        loc.wait()
        rem.wait()


def tail(n_dev, ht, ht_par, dys, ws, x_bf, gy, gains, t_q, t_k):
    rows, d_model = x_bf.shape
    half, chunk, own_rows, piece = d_model // 2, d_model // (n_dev // 2), d_model // n_dev, rows // n_dev
    hbm = pl.BlockSpec(memory_space=pl.ANY)
    vmem = pl.BlockSpec(memory_space=pltpu.VMEM)
    f32, bf16 = jnp.float32, jnp.bfloat16
    gw = jax.ShapeDtypeStruct((own_rows, d_model), f32)
    dma = pltpu.SemaphoreType.DMA
    return pl.pallas_call(
        functools.partial(tail_kernel, n_dev),
        out_shape=(gw, gw, gw, jax.ShapeDtypeStruct((n_dev, piece, d_model), bf16), jax.ShapeDtypeStruct((8, own_rows), f32)),
        in_specs=[hbm] * 10 + [vmem] * 3,
        out_specs=(hbm,) * 4 + (vmem,),
        scratch_shapes=[
            pltpu.VMEM((d_model, rows), bf16), pltpu.VMEM((d_model, rows), bf16),
            pltpu.VMEM((3, rows, d_model), bf16), pltpu.VMEM((3, rows, half), bf16),
            pltpu.VMEM((3, N_SLOTS, chunk, half), f32),
            pltpu.VMEM((rows, d_model), bf16),
            pltpu.VMEM((2, 3, 256, d_model), bf16),
            pltpu.VMEM((2, piece, d_model), bf16), pltpu.VMEM((2, piece, d_model), bf16),
            pltpu.VMEM((1, d_model), f32), pltpu.VMEM((n_dev, 8, own_rows), f32), pltpu.VMEM((n_dev, 8, own_rows), f32),
            dma((5,)), dma((3,)), dma((3,)), dma((3, 3)), dma((3, 3)), dma((2, 3)), dma((2, 2)),
            dma((n_dev,)), dma((n_dev,)), dma, dma((n_dev,)), dma((n_dev,)), dma((3,)), dma((3,)), dma((3,)),
        ],
        compiler_params=pltpu.CompilerParams(collective_id=0, has_side_effects=True, vmem_limit_bytes=67043328),
        cost_estimate=pl.CostEstimate(flops=12 * rows * d_model * d_model, bytes_accessed=64 * 1024 * 1024, transcendentals=0),
        name="tail",
    )(ht, ht_par, *dys, *ws, x_bf, gy, gains, t_q, t_k)


def solution(mesh):
    n_dev = mesh.shape['sp']

    def device_step(x_loc, gy_loc, pos_loc, g_norm, w_query, w_key, w_value, w_out, g_query, g_key):
        n_batch, loc_len, d_model = x_loc.shape
        rows = n_batch * loc_len
        gains = jnp.stack([g_norm, g_query, g_key])
        x_bf, gy, cos_sin, q_rot, k_rot, v_val, h_t, h_t_par, q1, k1, attended, a_t, lse = front(n_dev, x_loc, gy_loc, pos_loc, gains, w_query, w_key, w_value)
        gy = gy.reshape(rows, d_model)
        y_out, _, grad_wo, dq_bf, dk_bf, d_v, t_q, t_k = middle(n_dev, attended, x_loc, a_t, gy, w_out, q_rot, k_rot, v_val, q1, k1, cos_sin, lse, gains)
        grad_wv, grad_wk, grad_wq, grad_x, sums = tail(n_dev, h_t, h_t_par, (d_v, dk_bf, dq_bf), (w_value, w_key, w_query), x_bf, gy, gains, t_q, t_k)
        return y_out, grad_x, sums[0], grad_wq, grad_wk, grad_wv, grad_wo, sums[1], sums[2]

    seq_spec = P('dp', 'sp', None)
    mat_rep = P(None, None)
    vec_rep = P(None)
    row_spec = P(('dp', 'sp'), None)
    vec_spec = P(('dp', 'sp'))
    return jax.shard_map(device_step, mesh=mesh, in_specs=(seq_spec, seq_spec, P('dp', 'sp'), vec_rep, mat_rep, mat_rep, mat_rep, mat_rep, vec_rep, vec_rep), out_specs=(seq_spec, seq_spec, vec_spec, row_spec, row_spec, row_spec, row_spec, vec_spec, vec_spec), check_vma=False)
```

```python
import functools
import math
import jax
import jax.numpy as jnp
import numpy as np
from jax import lax
from jax.experimental import pallas as pl
from jax.experimental.pallas import tpu as pltpu
from jax.sharding import PartitionSpec as P

HEAD_DIM = 128
NORM_EPS = 1e-5
ROPE_BASE = 10000.0
NEG_BIG = -1e30
LOG2E = math.log2(math.e)
Q_BLOCK = 256


def rope_table(n_pos):
    half_dim = HEAD_DIM // 2
    inv_freq = (ROPE_BASE ** (-np.arange(half_dim) * (2.0 / HEAD_DIM))).astype(np.float32)
    angles = (np.arange(n_pos, dtype=np.float32)[:, None] * inv_freq).astype(np.float64)
    rest = np.concatenate([np.cos(angles), np.sin(angles)], axis=1).astype(np.float32)
    parts = []
    for _ in range(3):
        part = rest.astype(jnp.bfloat16)
        parts.append(part)
        rest = rest - part.astype(np.float32)
    return jnp.asarray(np.stack(parts))


def dot_nn(a, b):
    return lax.dot_general(a, b, (((1,), (0,)), ((), ())), preferred_element_type=jnp.float32)


def dot_nt(a, b):
    return lax.dot_general(a, b, (((1,), (1,)), ((), ())), preferred_element_type=jnp.float32)


def dot_tn(a, b):
    return lax.dot_general(a, b, (((0,), (0,)), ((), ())), preferred_element_type=jnp.float32)


def attend_head(seq_len, load_q, load_k, load_v, store):
    scale2 = LOG2E * HEAD_DIM ** -0.5
    for start in range(0, seq_len, Q_BLOCK):
        stop = start + Q_BLOCK
        q_blk = load_q(start, stop)
        s_diag = dot_nt(load_k(start, stop), q_blk)
        key_i = lax.broadcasted_iota(jnp.int32, s_diag.shape, 0)
        qry_i = lax.broadcasted_iota(jnp.int32, s_diag.shape, 1)
        s_diag = jnp.where(key_i <= qry_i, s_diag, NEG_BIG)
        m = jnp.max(s_diag, axis=0, keepdims=True)
        if start:
            s_past = dot_nt(load_k(0, start), q_blk)
            m = jnp.maximum(m, jnp.max(s_past, axis=0, keepdims=True))
        m2 = m * scale2
        p_diag = jnp.exp2(s_diag * scale2 - m2)
        l = jnp.sum(p_diag, axis=0, keepdims=True)
        acc = dot_tn(load_v(start, stop), p_diag.astype(jnp.bfloat16))
        if start:
            p_past = jnp.exp2(s_past * scale2 - m2)
            l = l + jnp.sum(p_past, axis=0, keepdims=True)
            acc = acc + dot_tn(load_v(0, start), p_past.astype(jnp.bfloat16))
        store(start, stop, acc / l, m2 + jnp.log2(l))


MESH = pl.DeviceIdType.MESH
ROW_BLOCK = 256


def row_inv(values):
    return lax.rsqrt(jnp.mean(values * values, axis=-1, keepdims=True) + NORM_EPS)


def front_kernel(n_dev, x_loc, gy_loc, pos_loc, tab_ref, g_ref, wq_ref, wk_ref, wv_ref,
                 x_seq, gy_seq, cs_ref, q_ref, k_ref, v_ref, ht_ref, ht_par, q1_ref, k1_ref, a_ref, at_ref, lse_ref,
                 xv, posv, wbuf, csb, qb, kb, vb, htb, q1b, k1b, ab, atb,
                 w_sem, x_send, x_recv, g_send, g_recv, p_send, p_recv, own_sem, xs_sem, out_sem, hp_send, hp_recv, a_sem):
    me = lax.axis_index('sp')
    chip, core = me // 2, me % 2
    n_chips = n_dev // 2
    piece = x_loc.shape[1]
    blk = 2 * piece
    n_pos = tab_ref.shape[1]
    d_model = x_loc.shape[2]

    for cp in [pltpu.make_async_copy(w, wbuf.at[i], w_sem.at[i]) for i, w in enumerate((wv_ref, wq_ref, wk_ref))]:
        cp.start()
    mine = pl.ds(pl.multiple_of(me * piece, piece), piece)
    own = [pltpu.make_async_copy(x_loc.at[me], xv.at[mine, :], own_sem.at[0]), pltpu.make_async_copy(pos_loc.at[me], posv.at[me], own_sem.at[1])]
    own_gy = pltpu.make_async_copy(gy_loc.at[me], gy_seq.at[me], own_sem.at[2])
    for cp in own + [own_gy]:
        cp.start()

    barrier = pltpu.get_barrier_semaphore()
    for off in range(1, n_dev):
        pl.semaphore_signal(barrier, inc=1, device_id={'sp': lax.rem(me + off, n_dev)}, device_id_type=MESH)
    pl.semaphore_wait(barrier, n_dev - 1)

    sends = []
    dests = [2 * chip + 1 - core]
    for hop in (1, n_chips - 1, 2):
        dests += [2 * lax.rem(chip + hop, n_chips) + lax.rem(core + flip, 2) for flip in range(2)]
    for i, dest in enumerate(dests):
        sends.append(pltpu.make_async_remote_copy(src_ref=pos_loc.at[dest], dst_ref=posv.at[me], send_sem=p_send.at[i], recv_sem=p_recv.at[me],
                                                  device_id={'sp': dest}, device_id_type=MESH))
        sends.append(pltpu.make_async_remote_copy(src_ref=x_loc.at[dest], dst_ref=xv.at[mine, :], send_sem=x_send.at[i], recv_sem=x_recv.at[me],
                                                  device_id={'sp': dest}, device_id_type=MESH))
    gy_sends = [pltpu.make_async_remote_copy(src_ref=gy_loc.at[dest], dst_ref=gy_seq.at[me], send_sem=g_send.at[i], recv_sem=g_recv.at[me],
                                             device_id={'sp': dest}, device_id_type=MESH) for i, dest in enumerate(dests)]
    for cp in sends + gy_sends:
        cp.start()

    def arrival(src):
        at = pl.ds(pl.multiple_of(src * piece, piece), piece)
        return (pltpu.make_async_remote_copy(src_ref=x_loc.at[src], dst_ref=xv.at[at, :], send_sem=x_send.at[0], recv_sem=x_recv.at[src],
                                             device_id={'sp': src}, device_id_type=MESH),
                pltpu.make_async_remote_copy(src_ref=pos_loc.at[src], dst_ref=posv.at[src], send_sem=p_send.at[0], recv_sem=p_recv.at[src],
                                             device_id={'sp': src}, device_id_type=MESH))

    def outs(at, slot):
        rows = pl.ds(pl.multiple_of(at, blk), blk)
        pairs = [(csb.at[slot], cs_ref.at[rows, :]), (qb.at[rows, :], q_ref.at[rows, :]), (kb.at[rows, :], k_ref.at[rows, :]), (vb.at[rows, :], v_ref.at[rows, :]),
                 (htb.at[slot], ht_ref.at[:, rows]), (q1b.at[slot], q1_ref.at[rows, :]), (k1b.at[slot], k1_ref.at[rows, :])]
        return [pltpu.make_async_copy(s, d, out_sem.at[slot, i]) for i, (s, d) in enumerate(pairs)]

    def ht_send(at, slot, b):
        cols = pl.ds(pl.multiple_of(at, blk), blk)
        return pltpu.make_async_remote_copy(src_ref=htb.at[slot], dst_ref=ht_par.at[:, cols], send_sem=hp_send.at[slot], recv_sem=hp_recv.at[b],
                                            device_id={'sp': 2 * chip + 1 - core}, device_id_type=MESH)

    def x_out(src_chip):
        rows = pl.ds(pl.multiple_of(src_chip * blk, blk), blk)
        return pltpu.make_async_copy(xv.at[rows, :], x_seq.at[rows, :], xs_sem.at[src_chip])

    def block(b, carry):
        hop = b + (b // 2) * (5 - 2 * b)
        src_chip = lax.rem(chip + hop, n_chips)
        at = pl.multiple_of(src_chip * blk, blk)
        slot = lax.rem(b, 2)

        @pl.when(b == 0)
        def _():
            for cp in own:
                cp.wait()
            for cp in arrival(2 * chip + 1 - core):
                cp.wait_recv()

        @pl.when(b > 0)
        def _():
            for e in range(2):
                for cp in arrival(2 * src_chip + e):
                    cp.wait_recv()

        x_out(src_chip).start()

        @pl.when(b >= 2)
        def _():
            for cp in outs(at, slot):
                cp.wait()
            ht_send(at, slot, b).wait_send()

        for e in range(2):
            hot = (lax.broadcasted_iota(jnp.int32, (n_pos, piece), 0) == posv[2 * src_chip + e]).astype(jnp.bfloat16)
            table = (dot_tn(hot, tab_ref[0]) + dot_tn(hot, tab_ref[1])) + dot_tn(hot, tab_ref[2])
            swapped = pltpu.roll(table, HEAD_DIM // 2, 1)
            low = lax.broadcasted_iota(jnp.int32, table.shape, 1) < HEAD_DIM // 2
            csb[slot, e * piece:(e + 1) * piece, 0:HEAD_DIM] = jnp.where(low, table, swapped)
            csb[slot, e * piece:(e + 1) * piece, HEAD_DIM:2 * HEAD_DIM] = jnp.where(low, -swapped, table)
        x_f = xv[pl.ds(at, blk), :].astype(jnp.float32)
        hidden = (x_f * row_inv(x_f) * g_ref[0:1, :].astype(jnp.float32)).astype(jnp.bfloat16)
        htb[slot] = hidden.T

        @pl.when(b == 0)
        def _():
            for i, w in enumerate((wv_ref, wq_ref, wk_ref)):
                pltpu.make_async_copy(w, wbuf.at[i], w_sem.at[i]).wait()

        vb[pl.ds(at, blk), :] = dot_nn(hidden, wbuf[0]).astype(jnp.bfloat16)
        cos_t, sin_t = csb[slot, :, 0:HEAD_DIM], csb[slot, :, HEAD_DIM:2 * HEAD_DIM]
        for i, raw_ref, out_ref in ((1, q1b, qb), (2, k1b, kb)):
            raw_ref[slot] = dot_nn(hidden, wbuf[i])
            inv = row_inv(raw_ref[slot])
            for c in range(0, d_model, HEAD_DIM):
                u = raw_ref[slot, :, c:c + HEAD_DIM] * inv * g_ref[i:i + 1, c:c + HEAD_DIM].astype(jnp.float32)
                out_ref[pl.ds(at, blk), c:c + HEAD_DIM] = (u * cos_t + pltpu.roll(u, HEAD_DIM // 2, 1) * sin_t).astype(jnp.bfloat16)
        for cp in outs(at, slot):
            cp.start()
        ht_send(at, slot, b).start()
        return carry

    lax.fori_loop(0, n_chips, block, 0)

    def a_copies(h, slot):
        cols = pl.ds(pl.multiple_of(h * HEAD_DIM, HEAD_DIM), HEAD_DIM)
        return (pltpu.make_async_copy(ab.at[slot], a_ref.at[:, cols], a_sem.at[slot, 0]), pltpu.make_async_copy(atb.at[slot], at_ref.at[cols, :], a_sem.at[slot, 1]))

    def head(h, carry):
        slot = lax.rem(h, 2)
        cols = pl.ds(pl.multiple_of(h * HEAD_DIM, HEAD_DIM), HEAD_DIM)

        @pl.when(h >= 2)
        def _():
            for cp in a_copies(h, slot):
                cp.wait()

        def store(start, stop, out, lse):
            atb[slot, :, start:stop] = out.astype(jnp.bfloat16)
            ab[slot, start:stop, :] = out.T.astype(jnp.bfloat16)
            lse_ref[h, :, start:stop] = lse

        attend_head(n_dev * piece, lambda i, j: qb[i:j, cols], lambda i, j: kb[i:j, cols], lambda i, j: vb[i:j, cols], store)
        for cp in a_copies(h, slot):
            cp.start()
        return carry

    lax.fori_loop(0, d_model // HEAD_DIM, head, 0)
    for slot in range(2):
        for cp in outs(0, slot) + list(a_copies(0, slot)):
            cp.wait()
        ht_send(0, slot, 0).wait_send()
    for i in range(n_chips):
        x_out(i).wait()
        ht_send(0, 0, i).wait_recv()
    for cp in sends:
        cp.wait_send()
    own_gy.wait()
    for i, cp in enumerate(gy_sends):
        cp.wait_send()
        src = dests[i]
        pltpu.make_async_remote_copy(src_ref=gy_loc.at[src], dst_ref=gy_seq.at[src], send_sem=g_send.at[0], recv_sem=g_recv.at[src],
                                     device_id={'sp': src}, device_id_type=MESH).wait_recv()


def front(n_dev, x_loc, gy_loc, pos_loc, gains, w_query, w_key, w_value):
    n_batch, piece, d_model = x_loc.shape
    rows, blk = n_batch * piece, 2 * piece
    hbm = pl.BlockSpec(memory_space=pl.ANY)
    vmem = pl.BlockSpec(memory_space=pltpu.VMEM)
    bf16, f32 = jnp.bfloat16, jnp.float32
    act = jax.ShapeDtypeStruct((rows, d_model), bf16)
    raw = jax.ShapeDtypeStruct((rows, d_model), f32)
    turned = jax.ShapeDtypeStruct((d_model, rows), bf16)
    dma = pltpu.SemaphoreType.DMA
    whole = pltpu.VMEM((rows, d_model), bf16)
    return pl.pallas_call(
        functools.partial(front_kernel, n_dev),
        out_shape=(act, jax.ShapeDtypeStruct(x_loc.shape, bf16), jax.ShapeDtypeStruct((rows, 2 * HEAD_DIM), f32), act, act, act, turned, turned, raw, raw, act, turned,
                   jax.ShapeDtypeStruct((d_model // HEAD_DIM, 1, rows), f32)),
        in_specs=[hbm] * 3 + [vmem] * 2 + [hbm] * 3,
        out_specs=(hbm,) * 12 + (vmem,),
        scratch_shapes=[
            pltpu.VMEM((rows, d_model), bf16), pltpu.VMEM((n_dev, 1, piece), jnp.int32), pltpu.VMEM((3, d_model, d_model), bf16),
            pltpu.VMEM((2, blk, 2 * HEAD_DIM), f32), whole, whole, whole, pltpu.VMEM((2, d_model, blk), bf16),
            pltpu.VMEM((2, blk, d_model), f32), pltpu.VMEM((2, blk, d_model), f32),
            pltpu.VMEM((2, rows, HEAD_DIM), bf16), pltpu.VMEM((2, HEAD_DIM, rows), bf16),
            dma((3,)), dma((n_dev,)), dma((n_dev,)), dma((n_dev,)), dma((n_dev,)), dma((n_dev,)), dma((n_dev,)), dma((3,)), dma((n_dev // 2,)), dma((2, 7)), dma((2,)), dma((n_dev // 2,)), dma((2, 2)),
        ],
        compiler_params=pltpu.CompilerParams(collective_id=1, has_side_effects=True, vmem_limit_bytes=67043328),
        cost_estimate=pl.CostEstimate(flops=6 * rows * d_model * d_model, bytes_accessed=60 * 1024 * 1024, transcendentals=0),
        name="front",
    )(x_loc, gy_loc, pos_loc[:, None, :], rope_table(rows), gains, w_query, w_key, w_value)


def middle_kernel(n_dev, a_seq, x_home, at_ref, gy_ref, wo_ref, q_ref, k_ref, v_ref, q1_ref, k1_ref, cs_ref, lse_ref, g_ref,
                  y_out, a_home, gw_ref, dq_ref, dk_ref, dv_ref, tq_ref, tk_ref,
                  wo, at_own, at_par, gy_own, gy_par, rs, dqk, hbuf, dvb, dob, dk_acc, dv_acc, rawb, tmp, nrm, ahb, xhb, yb,
                  load_sem, y_send, y_recv, y_loc, part_send, part_recv, rs_send, rs_recv, h_sem, dv_sem, raw_sem, dqk_sem,
                  fin_loc, fin_send, fin_recv, ax_sem, yo_sem):
    me = lax.axis_index('sp')
    chip, core = me // 2, me % 2
    n_chips = n_dev // 2
    step_dir = 1 - 2 * core
    partner = me + step_dir
    right = 2 * lax.rem(chip + step_dir + n_chips, n_chips) + core
    rows, d_model = gy_ref.shape
    n_heads = d_model // HEAD_DIM
    half, sub = d_model // 2, d_model // 4
    piece, chunk, own_rows = rows // n_dev, d_model // n_chips, d_model // n_dev
    other = pl.ds(pl.multiple_of((1 - core) * half, half), half)

    loads = [pltpu.make_async_copy(s, d, load_sem.at[i]) for i, (s, d) in enumerate(((at_ref, at_own), (gy_ref, gy_own), (wo_ref, wo)))]
    for cp in loads:
        cp.start()

    def head_copies(h, slot):
        cols = pl.ds(pl.multiple_of(h * HEAD_DIM, HEAD_DIM), HEAD_DIM)
        return [pltpu.make_async_copy(r.at[:, cols], hbuf.at[slot, i], h_sem.at[slot, i]) for i, r in enumerate((q_ref, k_ref, v_ref))]

    for cp in head_copies(0, 0):
        cp.start()

    barrier = pltpu.get_barrier_semaphore()
    for off in range(1, n_dev):
        pl.semaphore_signal(barrier, inc=1, device_id={'sp': lax.rem(me + off, n_dev)}, device_id_type=MESH)
    pl.semaphore_wait(barrier, n_dev - 1)

    parts = [pltpu.make_async_remote_copy(src_ref=s, dst_ref=d, send_sem=part_send.at[i], recv_sem=part_recv.at[i], device_id={'sp': partner}, device_id_type=MESH)
             for i, (s, d) in enumerate(((at_ref, at_par), (gy_ref.at[:, other], gy_par)))]
    for cp in parts:
        cp.start()

    def rs_copy(ch, s):
        return pltpu.make_async_remote_copy(src_ref=rs.at[ch, s], dst_ref=rs.at[ch, s + 1], send_sem=rs_send.at[ch, s], recv_sem=rs_recv.at[ch, s],
                                            device_id={'sp': right}, device_id_type=MESH)

    n_tile = 256

    def ring_step(ch, s):
        owner = lax.rem(chip - step_dir * (1 + s) + 2 * n_chips, n_chips)
        row_at = pl.ds(pl.multiple_of(owner * chunk, chunk), chunk)

        def tile(t, carry):
            col = pl.multiple_of(t * n_tile, n_tile)
            in_half = pl.multiple_of(ch * sub + col, n_tile)
            term = dot_nn(at_own[row_at, :], gy_own[:, pl.ds(pl.multiple_of(core * half + in_half, n_tile), n_tile)])
            term = term + dot_nn(at_par[row_at, :], gy_par[:, pl.ds(in_half, n_tile)])

            @pl.when(s == 0)
            def _():
                rs[ch, s, :, pl.ds(col, n_tile)] = term

            @pl.when(s > 0)
            def _():
                rs[ch, s, :, pl.ds(col, n_tile)] += term

            return carry

        lax.fori_loop(0, sub // n_tile, tile, 0)

    def ring(i):
        ch, s = lax.rem(i, 2), i // 2

        @pl.when(s > 0)
        def _():
            rs_copy(ch, s - 1).wait_recv()

        ring_step(ch, s)

        @pl.when(s < N_SLOTS - 1)
        def _():
            rs_copy(ch, s).start()

    def y_remote(off):
        dest = lax.rem(me + off, n_dev)
        return pltpu.make_async_remote_copy(src_ref=a_seq.at[dest], dst_ref=a_home.at[me], send_sem=y_send.at[off], recv_sem=y_recv.at[off],
                                            device_id={'sp': dest}, device_id_type=MESH)

    y_own = pltpu.make_async_copy(a_seq.at[me], a_home.at[me], y_loc)
    for off in range(1, n_dev):
        y_remote(off).start()
    y_own.start()

    def finish_out(ch):
        keep = pl.ds(pl.multiple_of(core * own_rows, own_rows), own_rows)
        give = pl.ds(pl.multiple_of((1 - core) * own_rows, own_rows), own_rows)
        cols = pl.ds(pl.multiple_of(core * half + ch * sub, sub), sub)
        loc = pltpu.make_async_copy(rs.at[ch, N_SLOTS - 1, keep, :], gw_ref.at[:, cols], fin_loc.at[ch])
        rem = pltpu.make_async_remote_copy(src_ref=rs.at[ch, N_SLOTS - 1, give, :], dst_ref=gw_ref.at[:, cols], send_sem=fin_send.at[ch], recv_sem=fin_recv.at[ch],
                                           device_id={'sp': partner}, device_id_type=MESH)
        return loc, rem

    scale = HEAD_DIM ** -0.5
    scale2 = LOG2E * scale

    def dv_copy(h, slot):
        cols = pl.ds(pl.multiple_of(h * HEAD_DIM, HEAD_DIM), HEAD_DIM)
        return pltpu.make_async_copy(dvb.at[slot], dv_ref.at[:, cols], dv_sem.at[slot])

    def head(h, carry):
        slot = lax.rem(h, 2)
        cols = pl.ds(pl.multiple_of(h * HEAD_DIM, HEAD_DIM), HEAD_DIM)
        in_pair = pl.ds(pl.multiple_of(slot * HEAD_DIM, HEAD_DIM), HEAD_DIM)

        @pl.when(slot == 0)
        def _():
            def do_tile(t, c2):
                ra = pl.ds(pl.multiple_of(t * 256, 256), 256)
                dob[ra, :] = dot_nt(gy_own[ra, :], wo[pl.ds(pl.multiple_of(h * HEAD_DIM, 2 * HEAD_DIM), 2 * HEAD_DIM), :]).astype(jnp.bfloat16)
                return c2

            lax.fori_loop(0, rows // 256, do_tile, 0)

        for cp in head_copies(h, slot):
            cp.wait()

        @pl.when(h + 1 < n_heads)
        def _():
            for cp in head_copies(h + 1, 1 - slot):
                cp.start()

        dk_acc[...] = jnp.zeros_like(dk_acc)
        dv_acc[...] = jnp.zeros_like(dv_acc)
        for start in range(0, rows, Q_BLOCK):
            stop = start + Q_BLOCK
            q_blk = hbuf[slot, 0, start:stop, :]
            do_blk = dob[start:stop, in_pair]
            lse = lse_ref[h, :, start:stop]
            k_all = hbuf[slot, 1, 0:stop, :]
            p = jnp.exp2(dot_nt(k_all, q_blk) * scale2 - lse)
            key_i = lax.broadcasted_iota(jnp.int32, (Q_BLOCK, Q_BLOCK), 0)
            qry_i = lax.broadcasted_iota(jnp.int32, (Q_BLOCK, Q_BLOCK), 1)
            p_diag = jnp.where(key_i <= qry_i, p[start:stop, :], 0.0)
            p = jnp.concatenate([p[0:start, :], p_diag], axis=0) if start else p_diag
            dp = dot_nt(hbuf[slot, 2, 0:stop, :], do_blk)
            delta = jnp.sum(p * dp, axis=0, keepdims=True)
            ds = (p * (dp - delta) * scale).astype(jnp.bfloat16)
            dv_acc[0:stop, :] += dot_nn(p.astype(jnp.bfloat16), do_blk)
            dk_acc[0:stop, :] += dot_nn(ds, q_blk)
            dqk[0, start:stop, cols] = dot_tn(k_all, ds).T.astype(jnp.bfloat16)
        dqk[1, :, cols] = dk_acc[...].astype(jnp.bfloat16)

        @pl.when(h >= 2)
        def _():
            dv_copy(h, slot).wait()

        dvb[slot] = dv_acc[...].astype(jnp.bfloat16)
        dv_copy(h, slot).start()

        ring_from = n_heads - 5

        @pl.when(jnp.logical_or(h == ring_from, h == ring_from + 3))
        def _():
            ring(2 + (h - ring_from) // 3)

        return carry

    loads[0].wait()
    loads[1].wait()
    for cp in parts:
        cp.wait_recv()
    for i in range(2):
        ring(i)
    loads[2].wait()
    lax.fori_loop(0, n_heads, head, 0)
    for slot in range(2):
        dv_copy(0, slot).wait()

    for off in range(1, n_dev):
        y_remote(off).wait()
    y_own.wait()

    def home_in(b, slot):
        two = pl.ds(2 * b, 2)
        return (pltpu.make_async_copy(a_home.at[two], ahb.at[slot], ax_sem.at[slot, 0]), pltpu.make_async_copy(x_home.at[two], xhb.at[slot], ax_sem.at[slot, 1]))

    def y_copy(b, slot):
        return pltpu.make_async_copy(yb.at[slot], y_out.at[pl.ds(2 * b, 2)], yo_sem.at[slot])

    def y_rows(b, carry):
        slot = lax.rem(b, 2)
        for cp in home_in(b, slot):
            cp.wait()

        @pl.when(b + 1 < n_chips)
        def _():
            for cp in home_in(b + 1, 1 - slot):
                cp.start()

        @pl.when(b >= 2)
        def _():
            y_copy(b, slot).wait()

        o_proj = dot_nn(ahb[slot].reshape(2 * piece, d_model), wo[...])
        yb[slot] = (xhb[slot].astype(jnp.float32) + o_proj.reshape(2, piece, d_model)).astype(jnp.bfloat16)
        y_copy(b, slot).start()
        return carry

    def raw_copy(i, b, slot):
        src = (q1_ref, k1_ref)[i]
        return pltpu.make_async_copy(src.at[pl.ds(pl.multiple_of(b * piece, piece), piece), :], rawb.at[slot], raw_sem.at[slot])

    for cp in home_in(0, 0):
        cp.start()
    for i, t_ref in ((0, tq_ref), (1, tk_ref)):
        t_ref[...] = jnp.zeros_like(t_ref)
        raw_copy(i, 0, 0).start()

        def norm_rows(b, carry):
            slot = lax.rem(b, 2)
            raw_copy(i, b, slot).wait()

            @pl.when(b + 1 < n_dev)
            def _():
                raw_copy(i, b + 1, 1 - slot).start()

            at = pl.ds(pl.multiple_of(b * piece, piece), piece)
            inv = row_inv(rawb[slot])
            cos_t, sin_t = cs_ref[at, 0:HEAD_DIM], cs_ref[at, HEAD_DIM:2 * HEAD_DIM]
            total = jnp.zeros((piece, HEAD_DIM), jnp.float32)
            for c in range(0, d_model, HEAD_DIM):
                d_u = dqk[i, at, c:c + HEAD_DIM].astype(jnp.float32)
                d_n = d_u * cos_t - pltpu.roll(d_u, HEAD_DIM // 2, 1) * sin_t
                hat = rawb[slot, :, c:c + HEAD_DIM] * inv
                t_ref[:, c:c + HEAD_DIM] += jnp.sum(d_n * hat, axis=0, keepdims=True)
                d_n = d_n * g_ref[i + 1:i + 2, c:c + HEAD_DIM].astype(jnp.float32)
                total = total + d_n * hat
                tmp[:, c:c + HEAD_DIM] = d_n
                nrm[:, c:c + HEAD_DIM] = hat
            mean = jnp.sum(total, axis=-1, keepdims=True) * (1.0 / d_model)
            for c in range(0, d_model, HEAD_DIM):
                dqk[i, at, c:c + HEAD_DIM] = (inv * (tmp[:, c:c + HEAD_DIM] - nrm[:, c:c + HEAD_DIM] * mean)).astype(jnp.bfloat16)
            return carry

        lax.fori_loop(0, n_dev, norm_rows, 0)
        pltpu.make_async_copy(dqk.at[i], (dq_ref, dk_ref)[i], dqk_sem.at[i]).start()
        if i == 0:
            ring(jnp.int32(4))
            lax.fori_loop(0, n_chips // 2, y_rows, 0)
            ring(jnp.int32(5))
            lax.fori_loop(n_chips // 2, n_chips, y_rows, 0)

    for ch in range(2):
        ring(jnp.int32(6 + ch))
        for cp in finish_out(ch):
            cp.start()
    for slot in range(2):
        y_copy(0, slot).wait()
    for cp in parts:
        cp.wait_send()
    for ch in range(2):
        for s in range(N_SLOTS - 1):
            rs_copy(ch, s).wait_send()
    for i in range(2):
        pltpu.make_async_copy(dqk.at[i], (dq_ref, dk_ref)[i], dqk_sem.at[i]).wait()
    for ch in range(2):
        loc, rem = finish_out(ch)
        loc.wait()
        rem.wait()


def middle(n_dev, a_seq, x_home, a_t, gy, w_out, q_rot, k_rot, v_val, q1, k1, cos_sin, lse, gains):
    rows, d_model = gy.shape
    piece, chunk, own_rows, sub = rows // n_dev, d_model // (n_dev // 2), d_model // n_dev, d_model // 4
    hbm = pl.BlockSpec(memory_space=pl.ANY)
    vmem = pl.BlockSpec(memory_space=pltpu.VMEM)
    f32, bf16 = jnp.float32, jnp.bfloat16
    act = jax.ShapeDtypeStruct((rows, d_model), bf16)
    vec = jax.ShapeDtypeStruct((1, d_model), f32)
    dma = pltpu.SemaphoreType.DMA
    return pl.pallas_call(
        functools.partial(middle_kernel, n_dev),
        out_shape=(jax.ShapeDtypeStruct((n_dev, piece, d_model), bf16), jax.ShapeDtypeStruct((n_dev, piece, d_model), bf16), jax.ShapeDtypeStruct((own_rows, d_model), f32), act, act, act, vec, vec),
        in_specs=[hbm] * 10 + [vmem] * 3,
        out_specs=(hbm,) * 6 + (vmem,) * 2,
        scratch_shapes=[
            pltpu.VMEM((d_model, d_model), bf16), pltpu.VMEM((d_model, rows), bf16), pltpu.VMEM((d_model, rows), bf16),
            pltpu.VMEM((rows, d_model), bf16), pltpu.VMEM((rows, d_model // 2), bf16),
            pltpu.VMEM((2, N_SLOTS, chunk, sub), f32), pltpu.VMEM((2, rows, d_model), bf16),
            pltpu.VMEM((2, 3, rows, HEAD_DIM), bf16), pltpu.VMEM((2, rows, HEAD_DIM), bf16), pltpu.VMEM((rows, 2 * HEAD_DIM), bf16),
            pltpu.VMEM((rows, HEAD_DIM), f32), pltpu.VMEM((rows, HEAD_DIM), f32),
            pltpu.VMEM((2, piece, d_model), f32), pltpu.VMEM((piece, d_model), f32), pltpu.VMEM((piece, d_model), f32),
            pltpu.VMEM((2, 2, piece, d_model), bf16), pltpu.VMEM((2, 2, piece, d_model), bf16), pltpu.VMEM((2, 2, piece, d_model), bf16),
            dma((3,)), dma((n_dev,)), dma((n_dev,)), dma, dma((2,)), dma((2,)), dma((2, 3)), dma((2, 3)), dma((2, 3)), dma((2,)), dma((2,)), dma((2,)),
            dma((2,)), dma((2,)), dma((2,)), dma((2, 2)), dma((2,)),
        ],
        compiler_params=pltpu.CompilerParams(collective_id=2, has_side_effects=True, vmem_limit_bytes=67043328),
        cost_estimate=pl.CostEstimate(flops=12 * rows * rows * d_model, bytes_accessed=64 * 1024 * 1024, transcendentals=0),
        name="middle",
    )(a_seq.reshape(n_dev, piece, d_model), x_home, a_t, gy, w_out, q_rot, k_rot, v_val, q1, k1, cos_sin, lse, gains)


N_SLOTS = 4


def tail_kernel(n_dev, ht_ref, htp_ref, dy_v, dy_k, dy_q, w_v, w_k, w_q, x_ref, gy_ref, gn_ref, tq_ref, tk_ref,
                gw_v, gw_k, gw_q, gx_ref, gain_ref,
                ht_own, ht_par, dy_own, dy_par, rs, dh, wbuf, xbuf, gybuf, n_acc, gsend, grecv,
                load_sem, part_send, part_recv, rs_send, rs_recv, w_sem, xy_sem, gx_send, gx_recv, gx_loc,
                gain_send, gain_recv, fin_loc, fin_send, fin_recv):
    me = lax.axis_index('sp')
    chip, core = me // 2, me % 2
    n_chips = n_dev // 2
    step_dir = 1 - 2 * core
    partner = me + step_dir
    right = 2 * lax.rem(chip + step_dir + n_chips, n_chips) + core
    rows, d_model = x_ref.shape
    half = d_model // 2
    piece = rows // n_dev
    chunk = d_model // n_chips
    own_rows = d_model // n_dev
    dys, ws, gws = (dy_v, dy_k, dy_q), (w_v, w_k, w_q), (gw_v, gw_k, gw_q)
    mine = pl.ds(pl.multiple_of(core * half, half), half)
    other = pl.ds(pl.multiple_of((1 - core) * half, half), half)

    loads = [pltpu.make_async_copy(dys[i], dy_own.at[i], load_sem.at[i]) for i in range(3)]
    loads[1:1] = [pltpu.make_async_copy(ht_ref, ht_own, load_sem.at[3]), pltpu.make_async_copy(htp_ref, ht_par, load_sem.at[4])]
    for cp in loads:
        cp.start()

    barrier = pltpu.get_barrier_semaphore()
    for off in range(1, n_dev):
        pl.semaphore_signal(barrier, inc=1, device_id={'sp': lax.rem(me + off, n_dev)}, device_id_type=MESH)
    pl.semaphore_wait(barrier, n_dev - 1)

    def to_partner(src, dst, idx):
        return pltpu.make_async_remote_copy(src_ref=src, dst_ref=dst, send_sem=part_send.at[idx], recv_sem=part_recv.at[idx],
                                            device_id={'sp': partner}, device_id_type=MESH)

    parts = [to_partner(dys[i].at[:, other], dy_par.at[i], i) for i in range(3)]
    for cp in parts:
        cp.start()

    def rs_copy(w, s):
        return pltpu.make_async_remote_copy(src_ref=rs.at[w, s], dst_ref=rs.at[w, s + 1], send_sem=rs_send.at[w, s], recv_sem=rs_recv.at[w, s],
                                            device_id={'sp': right}, device_id_type=MESH)

    n_tile = 256

    def ring_step(w, s):
        owner = lax.rem(chip - step_dir * (1 + s) + 2 * n_chips, n_chips)
        row_at = pl.multiple_of(owner * chunk, chunk)

        def tile(t, carry):
            col = pl.multiple_of(t * n_tile, n_tile)
            term = dot_nn(ht_own[pl.ds(row_at, chunk), :], dy_own[w, :, pl.ds(pl.multiple_of(core * half + col, n_tile), n_tile)])
            term = term + dot_nn(ht_par[pl.ds(row_at, chunk), :], dy_par[w, :, pl.ds(col, n_tile)])

            @pl.when(s == 0)
            def _():
                rs[w, s, :, pl.ds(col, n_tile)] = term

            @pl.when(s > 0)
            def _():
                rs[w, s, :, pl.ds(col, n_tile)] += term

            return carry

        lax.fori_loop(0, half // n_tile, tile, 0)

    def w_copy(i, n, slot):
        return pltpu.make_async_copy(ws[i].at[pl.ds(pl.multiple_of(n * n_tile, n_tile), n_tile), :], wbuf.at[slot, i], w_sem.at[slot, i])

    def dh_block(n):
        slot = lax.rem(n, 2)
        for i in range(3):
            w_copy(i, n, slot).wait()

        @pl.when(n + 1 < d_model // n_tile)
        def _():
            for i in range(3):
                w_copy(i, n + 1, 1 - slot).start()

        m_tile = 256

        def tile(t, carry):
            at = pl.ds(pl.multiple_of(t * m_tile, m_tile), m_tile)
            total = dot_nt(dy_own[0, at, :], wbuf[slot, 0]) + dot_nt(dy_own[1, at, :], wbuf[slot, 1]) + dot_nt(dy_own[2, at, :], wbuf[slot, 2])
            dh[at, pl.ds(pl.multiple_of(n * n_tile, n_tile), n_tile)] = total.astype(jnp.bfloat16)
            return carry

        lax.fori_loop(0, rows // m_tile, tile, 0)

    def xy_copies(p, slot):
        at = pl.ds(pl.multiple_of(p * piece, piece), piece)
        return (pltpu.make_async_copy(x_ref.at[at, :], xbuf.at[slot], xy_sem.at[slot, 0]),
                pltpu.make_async_copy(gy_ref.at[at, :], gybuf.at[slot], xy_sem.at[slot, 1]))

    def gx_remote(off):
        dest = lax.rem(me + off, n_dev)
        at = pl.ds(pl.multiple_of(dest * piece, piece), piece)
        return pltpu.make_async_remote_copy(src_ref=dh.at[at, :], dst_ref=gx_ref.at[me], send_sem=gx_send.at[off], recv_sem=gx_recv.at[off],
                                            device_id={'sp': dest}, device_id_type=MESH)

    def gx_own():
        at = pl.ds(pl.multiple_of(me * piece, piece), piece)
        return pltpu.make_async_copy(dh.at[at, :], gx_ref.at[me], gx_loc)

    def gain_copy(off):
        dest = lax.rem(me + off, n_dev)
        return pltpu.make_async_remote_copy(src_ref=gsend.at[dest], dst_ref=grecv.at[off], send_sem=gain_send.at[off], recv_sem=gain_recv.at[off],
                                            device_id={'sp': dest}, device_id_type=MESH)

    def grad_x_pieces():
        n_acc[...] = jnp.zeros_like(n_acc)
        for cp in xy_copies(0, 0):
            cp.start()

        def one(p, carry):
            slot = lax.rem(p, 2)
            for cp in xy_copies(p, slot):
                cp.wait()

            @pl.when(p + 1 < n_dev)
            def _():
                for cp in xy_copies(p + 1, 1 - slot):
                    cp.start()

            at = pl.ds(pl.multiple_of(p * piece, piece), piece)
            sub = 32

            def rows_of(j, c2):
                ra = pl.ds(pl.multiple_of(j * sub, sub), sub)
                rb = pl.ds(pl.multiple_of(p * piece + j * sub, sub), sub)
                x_f = xbuf[slot, ra, :].astype(jnp.float32)
                inv = row_inv(x_f)
                hat = x_f * inv
                d_h = dh[rb, :].astype(jnp.float32)
                n_acc[...] += jnp.sum(d_h * hat, axis=0, keepdims=True)
                d_n = d_h * gn_ref[0:1, :].astype(jnp.float32)
                mean = jnp.mean(d_n * hat, axis=-1, keepdims=True)
                out = gybuf[slot, ra, :].astype(jnp.float32) + inv * (d_n - hat * mean)
                dh[rb, :] = out.astype(jnp.bfloat16)
                return c2

            lax.fori_loop(0, piece // sub, rows_of, 0)
            return carry

        lax.fori_loop(0, n_dev, one, 0)
        for off in range(1, n_dev):
            gx_remote(off).start()
        gx_own().start()
        for d in range(n_dev):
            gsend[d] = jnp.zeros(gsend.shape[1:], jnp.float32)
            cols = slice(d * own_rows, (d + 1) * own_rows)
            gsend[d, 0:1, :] = n_acc[:, cols]
            gsend[d, 1:2, :] = tq_ref[:, cols]
            gsend[d, 2:3, :] = tk_ref[:, cols]
        for off in range(1, n_dev):
            gain_copy(off).start()

    def finish_out(w):
        keep = pl.ds(pl.multiple_of(core * own_rows, own_rows), own_rows)
        give = pl.ds(pl.multiple_of((1 - core) * own_rows, own_rows), own_rows)
        loc = pltpu.make_async_copy(rs.at[w, N_SLOTS - 1, keep, :], gws[w].at[:, mine], fin_loc.at[w])
        rem = pltpu.make_async_remote_copy(src_ref=rs.at[w, N_SLOTS - 1, give, :], dst_ref=gws[w].at[:, mine], send_sem=fin_send.at[w], recv_sem=fin_recv.at[w],
                                           device_id={'sp': partner}, device_id_type=MESH)
        return loc, rem

    for cp in loads[:3]:
        cp.wait()
    for i in range(3):
        w_copy(i, 0, 0).start()
    n_blocks = d_model // n_tile
    dh_from = 2

    def main(it, carry):
        s, w = it // 3, lax.rem(it, 3)

        @pl.when(s == 0)
        def _():
            pltpu.make_async_remote_copy(src_ref=dy_v.at[:, other], dst_ref=dy_par.at[w], send_sem=part_send.at[w], recv_sem=part_recv.at[w],
                                         device_id={'sp': partner}, device_id_type=MESH).wait_recv()

        @pl.when(jnp.logical_and(s == 0, w > 0))
        def _():
            pltpu.make_async_copy(dy_v, dy_own.at[w], load_sem.at[w]).wait()

        @pl.when(s > 0)
        def _():
            rs_copy(w, s - 1).wait_recv()

        ring_step(w, s)

        @pl.when(s < N_SLOTS - 1)
        def _():
            rs_copy(w, s).start()

        for j in range(2):
            blk_i = 2 * (it - dh_from) + j

            @pl.when(jnp.logical_and(blk_i >= 0, blk_i < n_blocks))
            def _():
                dh_block(blk_i)

        @pl.when(it == dh_from + n_blocks // 2)
        def _():
            grad_x_pieces()

        for i in range(3):
            @pl.when(jnp.logical_and(s == N_SLOTS - 1, w == i))
            def _():
                for cp in finish_out(i):
                    cp.start()

        return carry

    lax.fori_loop(0, 3 * N_SLOTS, main, 0)

    for cp in parts:
        cp.wait_send()

    def drain(it, carry):
        rs_copy(lax.rem(it, 3), it // 3).wait_send()
        return carry

    lax.fori_loop(0, 3 * (N_SLOTS - 1), drain, 0)
    for off in range(1, n_dev):
        gain_copy(off).wait()
    total = gsend[me]
    for off in range(1, n_dev):
        total = total + grecv[off]
    gain_ref[...] = total
    for off in range(1, n_dev):
        gx_remote(off).wait()
    gx_own().wait()
    for i in range(3):
        loc, rem = finish_out(i)
        loc.wait()
        rem.wait()


def tail(n_dev, ht, ht_par, dys, ws, x_bf, gy, gains, t_q, t_k):
    rows, d_model = x_bf.shape
    half, chunk, own_rows, piece = d_model // 2, d_model // (n_dev // 2), d_model // n_dev, rows // n_dev
    hbm = pl.BlockSpec(memory_space=pl.ANY)
    vmem = pl.BlockSpec(memory_space=pltpu.VMEM)
    f32, bf16 = jnp.float32, jnp.bfloat16
    gw = jax.ShapeDtypeStruct((own_rows, d_model), f32)
    dma = pltpu.SemaphoreType.DMA
    return pl.pallas_call(
        functools.partial(tail_kernel, n_dev),
        out_shape=(gw, gw, gw, jax.ShapeDtypeStruct((n_dev, piece, d_model), bf16), jax.ShapeDtypeStruct((8, own_rows), f32)),
        in_specs=[hbm] * 10 + [vmem] * 3,
        out_specs=(hbm,) * 4 + (vmem,),
        scratch_shapes=[
            pltpu.VMEM((d_model, rows), bf16), pltpu.VMEM((d_model, rows), bf16),
            pltpu.VMEM((3, rows, d_model), bf16), pltpu.VMEM((3, rows, half), bf16),
            pltpu.VMEM((3, N_SLOTS, chunk, half), f32),
            pltpu.VMEM((rows, d_model), bf16),
            pltpu.VMEM((2, 3, 256, d_model), bf16),
            pltpu.VMEM((2, piece, d_model), bf16), pltpu.VMEM((2, piece, d_model), bf16),
            pltpu.VMEM((1, d_model), f32), pltpu.VMEM((n_dev, 8, own_rows), f32), pltpu.VMEM((n_dev, 8, own_rows), f32),
            dma((5,)), dma((3,)), dma((3,)), dma((3, 3)), dma((3, 3)), dma((2, 3)), dma((2, 2)),
            dma((n_dev,)), dma((n_dev,)), dma, dma((n_dev,)), dma((n_dev,)), dma((3,)), dma((3,)), dma((3,)),
        ],
        compiler_params=pltpu.CompilerParams(collective_id=0, has_side_effects=True, vmem_limit_bytes=67043328),
        cost_estimate=pl.CostEstimate(flops=12 * rows * d_model * d_model, bytes_accessed=64 * 1024 * 1024, transcendentals=0),
        name="tail",
    )(ht, ht_par, *dys, *ws, x_bf, gy, gains, t_q, t_k)


def solution(mesh):
    n_dev = mesh.shape['sp']

    def device_step(x_loc, gy_loc, pos_loc, g_norm, w_query, w_key, w_value, w_out, g_query, g_key):
        n_batch, loc_len, d_model = x_loc.shape
        rows = n_batch * loc_len
        gains = jnp.stack([g_norm, g_query, g_key])
        x_bf, gy, cos_sin, q_rot, k_rot, v_val, h_t, h_t_par, q1, k1, attended, a_t, lse = front(n_dev, x_loc, gy_loc, pos_loc, gains, w_query, w_key, w_value)
        gy = gy.reshape(rows, d_model)
        y_out, _, grad_wo, dq_bf, dk_bf, d_v, t_q, t_k = middle(n_dev, attended, x_loc, a_t, gy, w_out, q_rot, k_rot, v_val, q1, k1, cos_sin, lse, gains)
        grad_wv, grad_wk, grad_wq, grad_x, sums = tail(n_dev, h_t, h_t_par, (d_v, dk_bf, dq_bf), (w_value, w_key, w_query), x_bf, gy, gains, t_q, t_k)
        return y_out, grad_x, sums[0], grad_wq, grad_wk, grad_wv, grad_wo, sums[1], sums[2]

    seq_spec = P('dp', 'sp', None)
    mat_rep = P(None, None)
    vec_rep = P(None)
    row_spec = P(('dp', 'sp'), None)
    vec_spec = P(('dp', 'sp'))
    return jax.shard_map(device_step, mesh=mesh, in_specs=(seq_spec, seq_spec, P('dp', 'sp'), vec_rep, mat_rep, mat_rep, mat_rep, mat_rep, vec_rep, vec_rep), out_specs=(seq_spec, seq_spec, vec_spec, row_spec, row_spec, row_spec, row_spec, vec_spec, vec_spec), check_vma=False)
```

```python
import functools
import math
import jax
import jax.numpy as jnp
import numpy as np
from jax import lax
from jax.experimental import pallas as pl
from jax.experimental.pallas import tpu as pltpu
from jax.sharding import PartitionSpec as P

HEAD_DIM = 128
NORM_EPS = 1e-5
ROPE_BASE = 10000.0
NEG_BIG = -1e30
LOG2E = math.log2(math.e)
Q_BLOCK = 256


def rope_table(n_pos):
    half_dim = HEAD_DIM // 2
    inv_freq = (ROPE_BASE ** (-np.arange(half_dim) * (2.0 / HEAD_DIM))).astype(np.float32)
    angles = (np.arange(n_pos, dtype=np.float32)[:, None] * inv_freq).astype(np.float64)
    rest = np.concatenate([np.cos(angles), np.sin(angles)], axis=1).astype(np.float32)
    parts = []
    for _ in range(3):
        part = rest.astype(jnp.bfloat16)
        parts.append(part)
        rest = rest - part.astype(np.float32)
    return jnp.asarray(np.stack(parts))


def dot_nn(a, b):
    return lax.dot_general(a, b, (((1,), (0,)), ((), ())), preferred_element_type=jnp.float32)


def dot_nt(a, b):
    return lax.dot_general(a, b, (((1,), (1,)), ((), ())), preferred_element_type=jnp.float32)


def dot_tn(a, b):
    return lax.dot_general(a, b, (((0,), (0,)), ((), ())), preferred_element_type=jnp.float32)


def attend_head(seq_len, load_q, load_k, load_v, store):
    scale2 = LOG2E * HEAD_DIM ** -0.5
    for start in range(0, seq_len, Q_BLOCK):
        stop = start + Q_BLOCK
        q_blk = load_q(start, stop)
        s_diag = dot_nt(load_k(start, stop), q_blk)
        key_i = lax.broadcasted_iota(jnp.int32, s_diag.shape, 0)
        qry_i = lax.broadcasted_iota(jnp.int32, s_diag.shape, 1)
        s_diag = jnp.where(key_i <= qry_i, s_diag, NEG_BIG)
        m = jnp.max(s_diag, axis=0, keepdims=True)
        if start:
            s_past = dot_nt(load_k(0, start), q_blk)
            m = jnp.maximum(m, jnp.max(s_past, axis=0, keepdims=True))
        m2 = m * scale2
        p_diag = jnp.exp2(s_diag * scale2 - m2)
        l = jnp.sum(p_diag, axis=0, keepdims=True)
        acc = dot_tn(load_v(start, stop), p_diag.astype(jnp.bfloat16))
        if start:
            p_past = jnp.exp2(s_past * scale2 - m2)
            l = l + jnp.sum(p_past, axis=0, keepdims=True)
            acc = acc + dot_tn(load_v(0, start), p_past.astype(jnp.bfloat16))
        store(start, stop, acc / l, m2 + jnp.log2(l))


MESH = pl.DeviceIdType.MESH
ROW_BLOCK = 256


def row_inv(values):
    return lax.rsqrt(jnp.mean(values * values, axis=-1, keepdims=True) + NORM_EPS)


def front_kernel(n_dev, x_loc, gy_loc, pos_loc, tab_ref, g_ref, wq_ref, wk_ref, wv_ref,
                 x_seq, gy_seq, cs_ref, q_ref, k_ref, v_ref, ht_ref, ht_par, q1_ref, k1_ref, a_ref, at_ref, lse_ref,
                 xv, posv, wbuf, csb, qb, kb, vb, htb, q1b, k1b, ab, atb,
                 w_sem, x_send, x_recv, g_send, g_recv, p_send, p_recv, own_sem, xs_sem, out_sem, hp_send, hp_recv, a_sem):
    me = lax.axis_index('sp')
    chip, core = me // 2, me % 2
    n_chips = n_dev // 2
    piece = x_loc.shape[1]
    blk = 2 * piece
    n_pos = tab_ref.shape[1]
    d_model = x_loc.shape[2]

    for cp in [pltpu.make_async_copy(w, wbuf.at[i], w_sem.at[i]) for i, w in enumerate((wv_ref, wq_ref, wk_ref))]:
        cp.start()
    mine = pl.ds(pl.multiple_of(me * piece, piece), piece)
    own = [pltpu.make_async_copy(x_loc.at[me], xv.at[mine, :], own_sem.at[0]), pltpu.make_async_copy(pos_loc.at[me], posv.at[me], own_sem.at[1])]
    own_gy = pltpu.make_async_copy(gy_loc.at[me], gy_seq.at[me], own_sem.at[2])
    for cp in own + [own_gy]:
        cp.start()

    barrier = pltpu.get_barrier_semaphore()
    for off in range(1, n_dev):
        pl.semaphore_signal(barrier, inc=1, device_id={'sp': lax.rem(me + off, n_dev)}, device_id_type=MESH)
    pl.semaphore_wait(barrier, n_dev - 1)

    sends = []
    dests = [2 * chip + 1 - core]
    for hop in (1, n_chips - 1, 2):
        dests += [2 * lax.rem(chip + hop, n_chips) + lax.rem(core + flip, 2) for flip in range(2)]
    for i, dest in enumerate(dests):
        sends.append(pltpu.make_async_remote_copy(src_ref=pos_loc.at[dest], dst_ref=posv.at[me], send_sem=p_send.at[i], recv_sem=p_recv.at[me],
                                                  device_id={'sp': dest}, device_id_type=MESH))
        sends.append(pltpu.make_async_remote_copy(src_ref=x_loc.at[dest], dst_ref=xv.at[mine, :], send_sem=x_send.at[i], recv_sem=x_recv.at[me],
                                                  device_id={'sp': dest}, device_id_type=MESH))
    gy_sends = [pltpu.make_async_remote_copy(src_ref=gy_loc.at[dest], dst_ref=gy_seq.at[me], send_sem=g_send.at[i], recv_sem=g_recv.at[me],
                                             device_id={'sp': dest}, device_id_type=MESH) for i, dest in enumerate(dests)]
    for cp in sends + gy_sends:
        cp.start()

    def arrival(src):
        at = pl.ds(pl.multiple_of(src * piece, piece), piece)
        return (pltpu.make_async_remote_copy(src_ref=x_loc.at[src], dst_ref=xv.at[at, :], send_sem=x_send.at[0], recv_sem=x_recv.at[src],
                                             device_id={'sp': src}, device_id_type=MESH),
                pltpu.make_async_remote_copy(src_ref=pos_loc.at[src], dst_ref=posv.at[src], send_sem=p_send.at[0], recv_sem=p_recv.at[src],
                                             device_id={'sp': src}, device_id_type=MESH))

    def outs(at, slot):
        rows = pl.ds(pl.multiple_of(at, blk), blk)
        pairs = [(csb.at[slot], cs_ref.at[rows, :]), (qb.at[rows, :], q_ref.at[rows, :]), (kb.at[rows, :], k_ref.at[rows, :]), (vb.at[rows, :], v_ref.at[rows, :]),
                 (htb.at[slot], ht_ref.at[:, rows]), (q1b.at[slot], q1_ref.at[rows, :]), (k1b.at[slot], k1_ref.at[rows, :])]
        return [pltpu.make_async_copy(s, d, out_sem.at[slot, i]) for i, (s, d) in enumerate(pairs)]

    def ht_send(at, slot, b):
        cols = pl.ds(pl.multiple_of(at, blk), blk)
        return pltpu.make_async_remote_copy(src_ref=htb.at[slot], dst_ref=ht_par.at[:, cols], send_sem=hp_send.at[slot], recv_sem=hp_recv.at[b],
                                            device_id={'sp': 2 * chip + 1 - core}, device_id_type=MESH)

    def x_out(src_chip):
        rows = pl.ds(pl.multiple_of(src_chip * blk, blk), blk)
        return pltpu.make_async_copy(xv.at[rows, :], x_seq.at[rows, :], xs_sem.at[src_chip])

    def block(b, carry):
        hop = b + (b // 2) * (5 - 2 * b)
        src_chip = lax.rem(chip + hop, n_chips)
        at = pl.multiple_of(src_chip * blk, blk)
        slot = lax.rem(b, 2)

        @pl.when(b == 0)
        def _():
            for cp in own:
                cp.wait()
            for cp in arrival(2 * chip + 1 - core):
                cp.wait_recv()

        @pl.when(b > 0)
        def _():
            for e in range(2):
                for cp in arrival(2 * src_chip + e):
                    cp.wait_recv()

        x_out(src_chip).start()

        @pl.when(b >= 2)
        def _():
            for cp in outs(at, slot):
                cp.wait()
            ht_send(at, slot, b).wait_send()

        for e in range(2):
            hot = (lax.broadcasted_iota(jnp.int32, (n_pos, piece), 0) == posv[2 * src_chip + e]).astype(jnp.bfloat16)
            table = (dot_tn(hot, tab_ref[0]) + dot_tn(hot, tab_ref[1])) + dot_tn(hot, tab_ref[2])
            swapped = pltpu.roll(table, HEAD_DIM // 2, 1)
            low = lax.broadcasted_iota(jnp.int32, table.shape, 1) < HEAD_DIM // 2
            csb[slot, e * piece:(e + 1) * piece, 0:HEAD_DIM] = jnp.where(low, table, swapped)
            csb[slot, e * piece:(e + 1) * piece, HEAD_DIM:2 * HEAD_DIM] = jnp.where(low, -swapped, table)
        x_f = xv[pl.ds(at, blk), :].astype(jnp.float32)
        hidden = (x_f * row_inv(x_f) * g_ref[0:1, :].astype(jnp.float32)).astype(jnp.bfloat16)
        htb[slot] = hidden.T

        @pl.when(b == 0)
        def _():
            for i, w in enumerate((wv_ref, wq_ref, wk_ref)):
                pltpu.make_async_copy(w, wbuf.at[i], w_sem.at[i]).wait()

        vb[pl.ds(at, blk), :] = dot_nn(hidden, wbuf[0]).astype(jnp.bfloat16)
        cos_t, sin_t = csb[slot, :, 0:HEAD_DIM], csb[slot, :, HEAD_DIM:2 * HEAD_DIM]
        for i, raw_ref, out_ref in ((1, q1b, qb), (2, k1b, kb)):
            raw_ref[slot] = dot_nn(hidden, wbuf[i])
            inv = row_inv(raw_ref[slot])
            for c in range(0, d_model, HEAD_DIM):
                u = raw_ref[slot, :, c:c + HEAD_DIM] * inv * g_ref[i:i + 1, c:c + HEAD_DIM].astype(jnp.float32)
                out_ref[pl.ds(at, blk), c:c + HEAD_DIM] = (u * cos_t + pltpu.roll(u, HEAD_DIM // 2, 1) * sin_t).astype(jnp.bfloat16)
        for cp in outs(at, slot):
            cp.start()
        ht_send(at, slot, b).start()
        return carry

    lax.fori_loop(0, n_chips, block, 0)

    def a_copies(h, slot):
        cols = pl.ds(pl.multiple_of(h * HEAD_DIM, HEAD_DIM), HEAD_DIM)
        return (pltpu.make_async_copy(ab.at[slot], a_ref.at[:, cols], a_sem.at[slot, 0]), pltpu.make_async_copy(atb.at[slot], at_ref.at[cols, :], a_sem.at[slot, 1]))

    def head(h, carry):
        slot = lax.rem(h, 2)
        cols = pl.ds(pl.multiple_of(h * HEAD_DIM, HEAD_DIM), HEAD_DIM)

        @pl.when(h >= 2)
        def _():
            for cp in a_copies(h, slot):
                cp.wait()

        def store(start, stop, out, lse):
            atb[slot, :, start:stop] = out.astype(jnp.bfloat16)
            ab[slot, start:stop, :] = out.T.astype(jnp.bfloat16)
            lse_ref[h, :, start:stop] = lse

        attend_head(n_dev * piece, lambda i, j: qb[i:j, cols], lambda i, j: kb[i:j, cols], lambda i, j: vb[i:j, cols], store)
        for cp in a_copies(h, slot):
            cp.start()
        return carry

    lax.fori_loop(0, d_model // HEAD_DIM, head, 0)
    for slot in range(2):
        for cp in outs(0, slot) + list(a_copies(0, slot)):
            cp.wait()
        ht_send(0, slot, 0).wait_send()
    for i in range(n_chips):
        x_out(i).wait()
        ht_send(0, 0, i).wait_recv()
    for cp in sends:
        cp.wait_send()
    own_gy.wait()
    for i, cp in enumerate(gy_sends):
        cp.wait_send()
        src = dests[i]
        pltpu.make_async_remote_copy(src_ref=gy_loc.at[src], dst_ref=gy_seq.at[src], send_sem=g_send.at[0], recv_sem=g_recv.at[src],
                                     device_id={'sp': src}, device_id_type=MESH).wait_recv()


def front(n_dev, x_loc, gy_loc, pos_loc, gains, w_query, w_key, w_value):
    n_batch, piece, d_model = x_loc.shape
    rows, blk = n_batch * piece, 2 * piece
    hbm = pl.BlockSpec(memory_space=pl.ANY)
    vmem = pl.BlockSpec(memory_space=pltpu.VMEM)
    bf16, f32 = jnp.bfloat16, jnp.float32
    act = jax.ShapeDtypeStruct((rows, d_model), bf16)
    raw = jax.ShapeDtypeStruct((rows, d_model), f32)
    turned = jax.ShapeDtypeStruct((d_model, rows), bf16)
    dma = pltpu.SemaphoreType.DMA
    whole = pltpu.VMEM((rows, d_model), bf16)
    return pl.pallas_call(
        functools.partial(front_kernel, n_dev),
        out_shape=(act, jax.ShapeDtypeStruct(x_loc.shape, bf16), jax.ShapeDtypeStruct((rows, 2 * HEAD_DIM), f32), act, act, act, turned, turned, raw, raw, act, turned,
                   jax.ShapeDtypeStruct((d_model // HEAD_DIM, 1, rows), f32)),
        in_specs=[hbm] * 3 + [vmem] * 2 + [hbm] * 3,
        out_specs=(hbm,) * 12 + (vmem,),
        scratch_shapes=[
            pltpu.VMEM((rows, d_model), bf16), pltpu.VMEM((n_dev, 1, piece), jnp.int32), pltpu.VMEM((3, d_model, d_model), bf16),
            pltpu.VMEM((2, blk, 2 * HEAD_DIM), f32), whole, whole, whole, pltpu.VMEM((2, d_model, blk), bf16),
            pltpu.VMEM((2, blk, d_model), f32), pltpu.VMEM((2, blk, d_model), f32),
            pltpu.VMEM((2, rows, HEAD_DIM), bf16), pltpu.VMEM((2, HEAD_DIM, rows), bf16),
            dma((3,)), dma((n_dev,)), dma((n_dev,)), dma((n_dev,)), dma((n_dev,)), dma((n_dev,)), dma((n_dev,)), dma((3,)), dma((n_dev // 2,)), dma((2, 7)), dma((2,)), dma((n_dev // 2,)), dma((2, 2)),
        ],
        compiler_params=pltpu.CompilerParams(collective_id=1, has_side_effects=True, vmem_limit_bytes=67043328),
        cost_estimate=pl.CostEstimate(flops=6 * rows * d_model * d_model, bytes_accessed=60 * 1024 * 1024, transcendentals=0),
        name="front",
    )(x_loc, gy_loc, pos_loc[:, None, :], rope_table(rows), gains, w_query, w_key, w_value)


def middle_kernel(n_dev, a_seq, at_ref, gy_ref, wo_ref, q_ref, k_ref, v_ref, q1_ref, k1_ref, cs_ref, lse_ref, g_ref,
                  a_home, gw_ref, dq_ref, dk_ref, dv_ref, tq_ref, tk_ref,
                  wo, at_own, at_par, gy_own, gy_par, rs, dqk, hbuf, dvb, dob, dk_acc, dv_acc, rawb, tmp, nrm,
                  load_sem, y_send, y_recv, y_loc, part_send, part_recv, rs_send, rs_recv, h_sem, dv_sem, raw_sem, dqk_sem,
                  fin_loc, fin_send, fin_recv):
    me = lax.axis_index('sp')
    chip, core = me // 2, me % 2
    n_chips = n_dev // 2
    step_dir = 1 - 2 * core
    partner = me + step_dir
    right = 2 * lax.rem(chip + step_dir + n_chips, n_chips) + core
    rows, d_model = gy_ref.shape
    n_heads = d_model // HEAD_DIM
    half, sub = d_model // 2, d_model // 4
    piece, chunk, own_rows = rows // n_dev, d_model // n_chips, d_model // n_dev
    other = pl.ds(pl.multiple_of((1 - core) * half, half), half)

    loads = [pltpu.make_async_copy(s, d, load_sem.at[i]) for i, (s, d) in enumerate(((at_ref, at_own), (gy_ref, gy_own), (wo_ref, wo)))]
    for cp in loads:
        cp.start()

    def head_copies(h, slot):
        cols = pl.ds(pl.multiple_of(h * HEAD_DIM, HEAD_DIM), HEAD_DIM)
        return [pltpu.make_async_copy(r.at[:, cols], hbuf.at[slot, i], h_sem.at[slot, i]) for i, r in enumerate((q_ref, k_ref, v_ref))]

    for cp in head_copies(0, 0):
        cp.start()

    barrier = pltpu.get_barrier_semaphore()
    for off in range(1, n_dev):
        pl.semaphore_signal(barrier, inc=1, device_id={'sp': lax.rem(me + off, n_dev)}, device_id_type=MESH)
    pl.semaphore_wait(barrier, n_dev - 1)

    parts = [pltpu.make_async_remote_copy(src_ref=s, dst_ref=d, send_sem=part_send.at[i], recv_sem=part_recv.at[i], device_id={'sp': partner}, device_id_type=MESH)
             for i, (s, d) in enumerate(((at_ref, at_par), (gy_ref.at[:, other], gy_par)))]
    for cp in parts:
        cp.start()

    def rs_copy(ch, s):
        return pltpu.make_async_remote_copy(src_ref=rs.at[ch, s], dst_ref=rs.at[ch, s + 1], send_sem=rs_send.at[ch, s], recv_sem=rs_recv.at[ch, s],
                                            device_id={'sp': right}, device_id_type=MESH)

    n_tile = 256

    def ring_step(ch, s):
        owner = lax.rem(chip - step_dir * (1 + s) + 2 * n_chips, n_chips)
        row_at = pl.ds(pl.multiple_of(owner * chunk, chunk), chunk)

        def tile(t, carry):
            col = pl.multiple_of(t * n_tile, n_tile)
            in_half = pl.multiple_of(ch * sub + col, n_tile)
            term = dot_nn(at_own[row_at, :], gy_own[:, pl.ds(pl.multiple_of(core * half + in_half, n_tile), n_tile)])
            term = term + dot_nn(at_par[row_at, :], gy_par[:, pl.ds(in_half, n_tile)])

            @pl.when(s == 0)
            def _():
                rs[ch, s, :, pl.ds(col, n_tile)] = term

            @pl.when(s > 0)
            def _():
                rs[ch, s, :, pl.ds(col, n_tile)] += term

            return carry

        lax.fori_loop(0, sub // n_tile, tile, 0)

    def ring(i):
        ch, s = lax.rem(i, 2), i // 2

        @pl.when(s > 0)
        def _():
            rs_copy(ch, s - 1).wait_recv()

        ring_step(ch, s)

        @pl.when(s < N_SLOTS - 1)
        def _():
            rs_copy(ch, s).start()

    def y_remote(off):
        dest = lax.rem(me + off, n_dev)
        return pltpu.make_async_remote_copy(src_ref=a_seq.at[dest], dst_ref=a_home.at[me], send_sem=y_send.at[off], recv_sem=y_recv.at[off],
                                            device_id={'sp': dest}, device_id_type=MESH)

    y_own = pltpu.make_async_copy(a_seq.at[me], a_home.at[me], y_loc)
    for off in range(1, n_dev):
        y_remote(off).start()
    y_own.start()

    def finish_out(ch):
        keep = pl.ds(pl.multiple_of(core * own_rows, own_rows), own_rows)
        give = pl.ds(pl.multiple_of((1 - core) * own_rows, own_rows), own_rows)
        cols = pl.ds(pl.multiple_of(core * half + ch * sub, sub), sub)
        loc = pltpu.make_async_copy(rs.at[ch, N_SLOTS - 1, keep, :], gw_ref.at[:, cols], fin_loc.at[ch])
        rem = pltpu.make_async_remote_copy(src_ref=rs.at[ch, N_SLOTS - 1, give, :], dst_ref=gw_ref.at[:, cols], send_sem=fin_send.at[ch], recv_sem=fin_recv.at[ch],
                                           device_id={'sp': partner}, device_id_type=MESH)
        return loc, rem

    scale = HEAD_DIM ** -0.5
    scale2 = LOG2E * scale

    def dv_copy(h, slot):
        cols = pl.ds(pl.multiple_of(h * HEAD_DIM, HEAD_DIM), HEAD_DIM)
        return pltpu.make_async_copy(dvb.at[slot], dv_ref.at[:, cols], dv_sem.at[slot])

    def head(h, carry):
        slot = lax.rem(h, 2)
        cols = pl.ds(pl.multiple_of(h * HEAD_DIM, HEAD_DIM), HEAD_DIM)
        in_pair = pl.ds(pl.multiple_of(slot * HEAD_DIM, HEAD_DIM), HEAD_DIM)

        @pl.when(slot == 0)
        def _():
            def do_tile(t, c2):
                ra = pl.ds(pl.multiple_of(t * 256, 256), 256)
                dob[ra, :] = dot_nt(gy_own[ra, :], wo[pl.ds(pl.multiple_of(h * HEAD_DIM, 2 * HEAD_DIM), 2 * HEAD_DIM), :]).astype(jnp.bfloat16)
                return c2

            lax.fori_loop(0, rows // 256, do_tile, 0)

        for cp in head_copies(h, slot):
            cp.wait()

        @pl.when(h + 1 < n_heads)
        def _():
            for cp in head_copies(h + 1, 1 - slot):
                cp.start()

        dk_acc[...] = jnp.zeros_like(dk_acc)
        dv_acc[...] = jnp.zeros_like(dv_acc)
        for start in range(0, rows, Q_BLOCK):
            stop = start + Q_BLOCK
            q_blk = hbuf[slot, 0, start:stop, :]
            do_blk = dob[start:stop, in_pair]
            lse = lse_ref[h, :, start:stop]
            k_all = hbuf[slot, 1, 0:stop, :]
            p = jnp.exp2(dot_nt(k_all, q_blk) * scale2 - lse)
            key_i = lax.broadcasted_iota(jnp.int32, (Q_BLOCK, Q_BLOCK), 0)
            qry_i = lax.broadcasted_iota(jnp.int32, (Q_BLOCK, Q_BLOCK), 1)
            p_diag = jnp.where(key_i <= qry_i, p[start:stop, :], 0.0)
            p = jnp.concatenate([p[0:start, :], p_diag], axis=0) if start else p_diag
            dp = dot_nt(hbuf[slot, 2, 0:stop, :], do_blk)
            delta = jnp.sum(p * dp, axis=0, keepdims=True)
            ds = (p * (dp - delta) * scale).astype(jnp.bfloat16)
            dv_acc[0:stop, :] += dot_nn(p.astype(jnp.bfloat16), do_blk)
            dk_acc[0:stop, :] += dot_nn(ds, q_blk)
            dqk[0, start:stop, cols] = dot_tn(k_all, ds).T.astype(jnp.bfloat16)
        dqk[1, :, cols] = dk_acc[...].astype(jnp.bfloat16)

        @pl.when(h >= 2)
        def _():
            dv_copy(h, slot).wait()

        dvb[slot] = dv_acc[...].astype(jnp.bfloat16)
        dv_copy(h, slot).start()

        ring_from = n_heads - 5

        @pl.when(jnp.logical_or(h == ring_from, h == ring_from + 3))
        def _():
            ring(2 + (h - ring_from) // 3)

        return carry

    loads[0].wait()
    loads[1].wait()
    for cp in parts:
        cp.wait_recv()
    for i in range(2):
        ring(i)
    loads[2].wait()
    lax.fori_loop(0, n_heads, head, 0)
    for slot in range(2):
        dv_copy(0, slot).wait()

    def raw_copy(i, b, slot):
        src = (q1_ref, k1_ref)[i]
        return pltpu.make_async_copy(src.at[pl.ds(pl.multiple_of(b * piece, piece), piece), :], rawb.at[slot], raw_sem.at[slot])

    for i, t_ref in ((0, tq_ref), (1, tk_ref)):
        t_ref[...] = jnp.zeros_like(t_ref)
        raw_copy(i, 0, 0).start()

        def norm_rows(b, carry):
            slot = lax.rem(b, 2)
            raw_copy(i, b, slot).wait()

            @pl.when(b + 1 < n_dev)
            def _():
                raw_copy(i, b + 1, 1 - slot).start()

            at = pl.ds(pl.multiple_of(b * piece, piece), piece)
            inv = row_inv(rawb[slot])
            cos_t, sin_t = cs_ref[at, 0:HEAD_DIM], cs_ref[at, HEAD_DIM:2 * HEAD_DIM]
            total = jnp.zeros((piece, HEAD_DIM), jnp.float32)
            for c in range(0, d_model, HEAD_DIM):
                d_u = dqk[i, at, c:c + HEAD_DIM].astype(jnp.float32)
                d_n = d_u * cos_t - pltpu.roll(d_u, HEAD_DIM // 2, 1) * sin_t
                hat = rawb[slot, :, c:c + HEAD_DIM] * inv
                t_ref[:, c:c + HEAD_DIM] += jnp.sum(d_n * hat, axis=0, keepdims=True)
                d_n = d_n * g_ref[i + 1:i + 2, c:c + HEAD_DIM].astype(jnp.float32)
                total = total + d_n * hat
                tmp[:, c:c + HEAD_DIM] = d_n
                nrm[:, c:c + HEAD_DIM] = hat
            mean = jnp.sum(total, axis=-1, keepdims=True) * (1.0 / d_model)
            for c in range(0, d_model, HEAD_DIM):
                dqk[i, at, c:c + HEAD_DIM] = (inv * (tmp[:, c:c + HEAD_DIM] - nrm[:, c:c + HEAD_DIM] * mean)).astype(jnp.bfloat16)
            return carry

        lax.fori_loop(0, n_dev, norm_rows, 0)
        pltpu.make_async_copy(dqk.at[i], (dq_ref, dk_ref)[i], dqk_sem.at[i]).start()
        if i == 0:
            ring(jnp.int32(4))
            ring(jnp.int32(5))

    for ch in range(2):
        ring(jnp.int32(6 + ch))
        for cp in finish_out(ch):
            cp.start()
    for cp in parts:
        cp.wait_send()
    for ch in range(2):
        for s in range(N_SLOTS - 1):
            rs_copy(ch, s).wait_send()
    for off in range(1, n_dev):
        y_remote(off).wait()
    y_own.wait()
    for i in range(2):
        pltpu.make_async_copy(dqk.at[i], (dq_ref, dk_ref)[i], dqk_sem.at[i]).wait()
    for ch in range(2):
        loc, rem = finish_out(ch)
        loc.wait()
        rem.wait()


def middle(n_dev, a_seq, a_t, gy, w_out, q_rot, k_rot, v_val, q1, k1, cos_sin, lse, gains):
    rows, d_model = gy.shape
    piece, chunk, own_rows, sub = rows // n_dev, d_model // (n_dev // 2), d_model // n_dev, d_model // 4
    hbm = pl.BlockSpec(memory_space=pl.ANY)
    vmem = pl.BlockSpec(memory_space=pltpu.VMEM)
    f32, bf16 = jnp.float32, jnp.bfloat16
    act = jax.ShapeDtypeStruct((rows, d_model), bf16)
    vec = jax.ShapeDtypeStruct((1, d_model), f32)
    dma = pltpu.SemaphoreType.DMA
    return pl.pallas_call(
        functools.partial(middle_kernel, n_dev),
        out_shape=(jax.ShapeDtypeStruct((n_dev, piece, d_model), bf16), jax.ShapeDtypeStruct((own_rows, d_model), f32), act, act, act, vec, vec),
        in_specs=[hbm] * 9 + [vmem] * 3,
        out_specs=(hbm,) * 5 + (vmem,) * 2,
        scratch_shapes=[
            pltpu.VMEM((d_model, d_model), bf16), pltpu.VMEM((d_model, rows), bf16), pltpu.VMEM((d_model, rows), bf16),
            pltpu.VMEM((rows, d_model), bf16), pltpu.VMEM((rows, d_model // 2), bf16),
            pltpu.VMEM((2, N_SLOTS, chunk, sub), f32), pltpu.VMEM((2, rows, d_model), bf16),
            pltpu.VMEM((2, 3, rows, HEAD_DIM), bf16), pltpu.VMEM((2, rows, HEAD_DIM), bf16), pltpu.VMEM((rows, 2 * HEAD_DIM), bf16),
            pltpu.VMEM((rows, HEAD_DIM), f32), pltpu.VMEM((rows, HEAD_DIM), f32),
            pltpu.VMEM((2, piece, d_model), f32), pltpu.VMEM((piece, d_model), f32), pltpu.VMEM((piece, d_model), f32),
            dma((3,)), dma((n_dev,)), dma((n_dev,)), dma, dma((2,)), dma((2,)), dma((2, 3)), dma((2, 3)), dma((2, 3)), dma((2,)), dma((2,)), dma((2,)),
            dma((2,)), dma((2,)), dma((2,)),
        ],
        compiler_params=pltpu.CompilerParams(collective_id=2, has_side_effects=True, vmem_limit_bytes=67043328),
        cost_estimate=pl.CostEstimate(flops=12 * rows * rows * d_model, bytes_accessed=64 * 1024 * 1024, transcendentals=0),
        name="middle",
    )(a_seq.reshape(n_dev, piece, d_model), a_t, gy, w_out, q_rot, k_rot, v_val, q1, k1, cos_sin, lse, gains)


N_SLOTS = 4


def tail_kernel(n_dev, ht_ref, htp_ref, dy_v, dy_k, dy_q, w_v, w_k, w_q, x_ref, gy_ref, ah_ref, xh_ref, wo_ref, gn_ref, tq_ref, tk_ref,
                gw_v, gw_k, gw_q, gx_ref, y_ref, gain_ref,
                ht_own, ht_par, dy_own, dy_par, rs, dh, wbuf, xbuf, gybuf, n_acc, gsend, grecv, wob, xhb, yhb,
                load_sem, part_send, part_recv, rs_send, rs_recv, w_sem, xy_sem, gx_send, gx_recv, gx_loc,
                gain_send, gain_recv, fin_loc, fin_send, fin_recv, home_sem):
    me = lax.axis_index('sp')
    chip, core = me // 2, me % 2
    n_chips = n_dev // 2
    step_dir = 1 - 2 * core
    partner = me + step_dir
    right = 2 * lax.rem(chip + step_dir + n_chips, n_chips) + core
    rows, d_model = x_ref.shape
    half = d_model // 2
    piece = rows // n_dev
    chunk = d_model // n_chips
    own_rows = d_model // n_dev
    dys, ws, gws = (dy_v, dy_k, dy_q), (w_v, w_k, w_q), (gw_v, gw_k, gw_q)
    mine = pl.ds(pl.multiple_of(core * half, half), half)
    other = pl.ds(pl.multiple_of((1 - core) * half, half), half)

    loads = [pltpu.make_async_copy(dys[i], dy_own.at[i], load_sem.at[i]) for i in range(3)]
    a_load = pltpu.make_async_copy(ah_ref, dh, home_sem.at[0])
    loads[1:1] = [pltpu.make_async_copy(ht_ref, ht_own, load_sem.at[3]), pltpu.make_async_copy(htp_ref, ht_par, load_sem.at[4])]
    for cp in loads:
        cp.start()

    barrier = pltpu.get_barrier_semaphore()
    for off in range(1, n_dev):
        pl.semaphore_signal(barrier, inc=1, device_id={'sp': lax.rem(me + off, n_dev)}, device_id_type=MESH)
    pl.semaphore_wait(barrier, n_dev - 1)

    def to_partner(src, dst, idx):
        return pltpu.make_async_remote_copy(src_ref=src, dst_ref=dst, send_sem=part_send.at[idx], recv_sem=part_recv.at[idx],
                                            device_id={'sp': partner}, device_id_type=MESH)

    parts = [to_partner(dys[i].at[:, other], dy_par.at[i], i) for i in range(3)]
    for cp in parts + [a_load]:
        cp.start()

    def rs_copy(w, s):
        return pltpu.make_async_remote_copy(src_ref=rs.at[w, s], dst_ref=rs.at[w, s + 1], send_sem=rs_send.at[w, s], recv_sem=rs_recv.at[w, s],
                                            device_id={'sp': right}, device_id_type=MESH)

    n_tile = 256

    def ring_step(w, s):
        owner = lax.rem(chip - step_dir * (1 + s) + 2 * n_chips, n_chips)
        row_at = pl.multiple_of(owner * chunk, chunk)

        def tile(t, carry):
            col = pl.multiple_of(t * n_tile, n_tile)
            term = dot_nn(ht_own[pl.ds(row_at, chunk), :], dy_own[w, :, pl.ds(pl.multiple_of(core * half + col, n_tile), n_tile)])
            term = term + dot_nn(ht_par[pl.ds(row_at, chunk), :], dy_par[w, :, pl.ds(col, n_tile)])

            @pl.when(s == 0)
            def _():
                rs[w, s, :, pl.ds(col, n_tile)] = term

            @pl.when(s > 0)
            def _():
                rs[w, s, :, pl.ds(col, n_tile)] += term

            return carry

        lax.fori_loop(0, half // n_tile, tile, 0)

    def dh_block(n):
        w_copies = [pltpu.make_async_copy(ws[i].at[pl.ds(pl.multiple_of(n * n_tile, n_tile), n_tile), :], wbuf.at[i], w_sem.at[i]) for i in range(3)]
        for cp in w_copies:
            cp.start()
        for cp in w_copies:
            cp.wait()

        m_tile = 256

        def tile(t, carry):
            at = pl.ds(pl.multiple_of(t * m_tile, m_tile), m_tile)
            total = dot_nt(dy_own[0, at, :], wbuf[0]) + dot_nt(dy_own[1, at, :], wbuf[1]) + dot_nt(dy_own[2, at, :], wbuf[2])
            dh[at, pl.ds(pl.multiple_of(n * n_tile, n_tile), n_tile)] = total.astype(jnp.bfloat16)
            return carry

        lax.fori_loop(0, rows // m_tile, tile, 0)

    def y_block(n, carry):
        cols = pl.ds(pl.multiple_of(n * n_tile, n_tile), n_tile)
        ins = [pltpu.make_async_copy(wo_ref.at[:, cols], wob, home_sem.at[1]), pltpu.make_async_copy(xh_ref.at[:, cols], xhb, home_sem.at[2])]
        for cp in ins:
            cp.start()
        for cp in ins:
            cp.wait()

        def tile(t, c2):
            at = pl.ds(pl.multiple_of(t * 256, 256), 256)
            yhb[at, :] = (xhb[at, :].astype(jnp.float32) + dot_nn(dh[at, :], wob[...])).astype(jnp.bfloat16)
            return c2

        lax.fori_loop(0, rows // 256, tile, 0)
        out = pltpu.make_async_copy(yhb, y_ref.at[:, cols], home_sem.at[3])
        out.start()
        out.wait()
        return carry

    def xy_copies(p, slot):
        at = pl.ds(pl.multiple_of(p * piece, piece), piece)
        return (pltpu.make_async_copy(x_ref.at[at, :], xbuf.at[slot], xy_sem.at[slot, 0]),
                pltpu.make_async_copy(gy_ref.at[at, :], gybuf.at[slot], xy_sem.at[slot, 1]))

    def gx_remote(off):
        dest = lax.rem(me + off, n_dev)
        at = pl.ds(pl.multiple_of(dest * piece, piece), piece)
        return pltpu.make_async_remote_copy(src_ref=dh.at[at, :], dst_ref=gx_ref.at[me], send_sem=gx_send.at[off], recv_sem=gx_recv.at[off],
                                            device_id={'sp': dest}, device_id_type=MESH)

    def gx_own():
        at = pl.ds(pl.multiple_of(me * piece, piece), piece)
        return pltpu.make_async_copy(dh.at[at, :], gx_ref.at[me], gx_loc)

    def gain_copy(off):
        dest = lax.rem(me + off, n_dev)
        return pltpu.make_async_remote_copy(src_ref=gsend.at[dest], dst_ref=grecv.at[off], send_sem=gain_send.at[off], recv_sem=gain_recv.at[off],
                                            device_id={'sp': dest}, device_id_type=MESH)

    def grad_x_pieces():
        n_acc[...] = jnp.zeros_like(n_acc)
        for cp in xy_copies(0, 0):
            cp.start()

        def one(p, carry):
            slot = lax.rem(p, 2)
            for cp in xy_copies(p, slot):
                cp.wait()

            @pl.when(p + 1 < n_dev)
            def _():
                for cp in xy_copies(p + 1, 1 - slot):
                    cp.start()

            at = pl.ds(pl.multiple_of(p * piece, piece), piece)
            sub = 32

            def rows_of(j, c2):
                ra = pl.ds(pl.multiple_of(j * sub, sub), sub)
                rb = pl.ds(pl.multiple_of(p * piece + j * sub, sub), sub)
                x_f = xbuf[slot, ra, :].astype(jnp.float32)
                inv = row_inv(x_f)
                hat = x_f * inv
                d_h = dh[rb, :].astype(jnp.float32)
                n_acc[...] += jnp.sum(d_h * hat, axis=0, keepdims=True)
                d_n = d_h * gn_ref[0:1, :].astype(jnp.float32)
                mean = jnp.mean(d_n * hat, axis=-1, keepdims=True)
                out = gybuf[slot, ra, :].astype(jnp.float32) + inv * (d_n - hat * mean)
                dh[rb, :] = out.astype(jnp.bfloat16)
                return c2

            lax.fori_loop(0, piece // sub, rows_of, 0)
            return carry

        lax.fori_loop(0, n_dev, one, 0)
        for off in range(1, n_dev):
            gx_remote(off).start()
        gx_own().start()
        for d in range(n_dev):
            gsend[d] = jnp.zeros(gsend.shape[1:], jnp.float32)
            cols = slice(d * own_rows, (d + 1) * own_rows)
            gsend[d, 0:1, :] = n_acc[:, cols]
            gsend[d, 1:2, :] = tq_ref[:, cols]
            gsend[d, 2:3, :] = tk_ref[:, cols]
        for off in range(1, n_dev):
            gain_copy(off).start()

    def finish_out(w):
        keep = pl.ds(pl.multiple_of(core * own_rows, own_rows), own_rows)
        give = pl.ds(pl.multiple_of((1 - core) * own_rows, own_rows), own_rows)
        loc = pltpu.make_async_copy(rs.at[w, N_SLOTS - 1, keep, :], gws[w].at[:, mine], fin_loc.at[w])
        rem = pltpu.make_async_remote_copy(src_ref=rs.at[w, N_SLOTS - 1, give, :], dst_ref=gws[w].at[:, mine], send_sem=fin_send.at[w], recv_sem=fin_recv.at[w],
                                           device_id={'sp': partner}, device_id_type=MESH)
        return loc, rem

    for cp in loads[:3]:
        cp.wait()
    n_blocks = d_model // n_tile
    dh_from = 3

    def main(it, carry):
        s, w = it // 3, lax.rem(it, 3)

        @pl.when(s == 0)
        def _():
            pltpu.make_async_remote_copy(src_ref=dy_v.at[:, other], dst_ref=dy_par.at[w], send_sem=part_send.at[w], recv_sem=part_recv.at[w],
                                         device_id={'sp': partner}, device_id_type=MESH).wait_recv()

        @pl.when(jnp.logical_and(s == 0, w > 0))
        def _():
            pltpu.make_async_copy(dy_v, dy_own.at[w], load_sem.at[w]).wait()

        @pl.when(s > 0)
        def _():
            rs_copy(w, s - 1).wait_recv()

        ring_step(w, s)

        @pl.when(s < N_SLOTS - 1)
        def _():
            rs_copy(w, s).start()

        @pl.when(it == 1)
        def _():
            a_load.wait()
            lax.fori_loop(0, n_blocks // 2, y_block, 0)

        @pl.when(it == 2)
        def _():
            lax.fori_loop(n_blocks // 2, n_blocks, y_block, 0)

        for j in range(2):
            blk_i = 2 * (it - dh_from) + j

            @pl.when(jnp.logical_and(blk_i >= 0, blk_i < n_blocks))
            def _():
                dh_block(blk_i)

        @pl.when(it == dh_from + n_blocks // 2)
        def _():
            grad_x_pieces()

        for i in range(3):
            @pl.when(jnp.logical_and(s == N_SLOTS - 1, w == i))
            def _():
                for cp in finish_out(i):
                    cp.start()

        return carry

    lax.fori_loop(0, 3 * N_SLOTS, main, 0)

    for cp in parts:
        cp.wait_send()

    def drain(it, carry):
        rs_copy(lax.rem(it, 3), it // 3).wait_send()
        return carry

    lax.fori_loop(0, 3 * (N_SLOTS - 1), drain, 0)
    for off in range(1, n_dev):
        gain_copy(off).wait()
    total = gsend[me]
    for off in range(1, n_dev):
        total = total + grecv[off]
    gain_ref[...] = total
    for off in range(1, n_dev):
        gx_remote(off).wait()
    gx_own().wait()
    for i in range(3):
        loc, rem = finish_out(i)
        loc.wait()
        rem.wait()


def tail(n_dev, ht, ht_par, dys, ws, x_bf, gy, a_home, x_home, w_out, gains, t_q, t_k):
    rows, d_model = x_bf.shape
    half, chunk, own_rows, piece = d_model // 2, d_model // (n_dev // 2), d_model // n_dev, rows // n_dev
    hbm = pl.BlockSpec(memory_space=pl.ANY)
    vmem = pl.BlockSpec(memory_space=pltpu.VMEM)
    f32, bf16 = jnp.float32, jnp.bfloat16
    gw = jax.ShapeDtypeStruct((own_rows, d_model), f32)
    dma = pltpu.SemaphoreType.DMA
    return pl.pallas_call(
        functools.partial(tail_kernel, n_dev),
        out_shape=(gw, gw, gw, jax.ShapeDtypeStruct((n_dev, piece, d_model), bf16), jax.ShapeDtypeStruct((rows, d_model), bf16), jax.ShapeDtypeStruct((8, own_rows), f32)),
        in_specs=[hbm] * 13 + [vmem] * 3,
        out_specs=(hbm,) * 5 + (vmem,),
        scratch_shapes=[
            pltpu.VMEM((d_model, rows), bf16), pltpu.VMEM((d_model, rows), bf16),
            pltpu.VMEM((3, rows, d_model), bf16), pltpu.VMEM((3, rows, half), bf16),
            pltpu.VMEM((3, N_SLOTS, chunk, half), f32),
            pltpu.VMEM((rows, d_model), bf16),
            pltpu.VMEM((3, 256, d_model), bf16),
            pltpu.VMEM((2, piece, d_model), bf16), pltpu.VMEM((2, piece, d_model), bf16),
            pltpu.VMEM((1, d_model), f32), pltpu.VMEM((n_dev, 8, own_rows), f32), pltpu.VMEM((n_dev, 8, own_rows), f32),
            pltpu.VMEM((d_model, 256), bf16), pltpu.VMEM((rows, 256), bf16), pltpu.VMEM((rows, 256), bf16),
            dma((5,)), dma((3,)), dma((3,)), dma((3, 3)), dma((3, 3)), dma((3,)), dma((2, 2)),
            dma((n_dev,)), dma((n_dev,)), dma, dma((n_dev,)), dma((n_dev,)), dma((3,)), dma((3,)), dma((3,)), dma((4,)),
        ],
        compiler_params=pltpu.CompilerParams(collective_id=0, has_side_effects=True, vmem_limit_bytes=67043328),
        cost_estimate=pl.CostEstimate(flops=12 * rows * d_model * d_model, bytes_accessed=64 * 1024 * 1024, transcendentals=0),
        name="tail",
    )(ht, ht_par, *dys, *ws, x_bf, gy, a_home, x_home, w_out, gains, t_q, t_k)


def solution(mesh):
    n_dev = mesh.shape['sp']

    def device_step(x_loc, gy_loc, pos_loc, g_norm, w_query, w_key, w_value, w_out, g_query, g_key):
        n_batch, loc_len, d_model = x_loc.shape
        rows = n_batch * loc_len
        gains = jnp.stack([g_norm, g_query, g_key])
        x_bf, gy, cos_sin, q_rot, k_rot, v_val, h_t, h_t_par, q1, k1, attended, a_t, lse = front(n_dev, x_loc, gy_loc, pos_loc, gains, w_query, w_key, w_value)
        gy = gy.reshape(rows, d_model)
        a_home, grad_wo, dq_bf, dk_bf, d_v, t_q, t_k = middle(n_dev, attended, a_t, gy, w_out, q_rot, k_rot, v_val, q1, k1, cos_sin, lse, gains)
        grad_wv, grad_wk, grad_wq, grad_x, y_out, sums = tail(n_dev, h_t, h_t_par, (d_v, dk_bf, dq_bf), (w_value, w_key, w_query), x_bf, gy,
                                                              a_home.reshape(rows, d_model), x_loc.reshape(rows, d_model), w_out, gains, t_q, t_k)
        y_out = y_out.reshape(n_batch, loc_len, d_model)
        return y_out, grad_x, sums[0], grad_wq, grad_wk, grad_wv, grad_wo, sums[1], sums[2]

    seq_spec = P('dp', 'sp', None)
    mat_rep = P(None, None)
    vec_rep = P(None)
    row_spec = P(('dp', 'sp'), None)
    vec_spec = P(('dp', 'sp'))
    return jax.shard_map(device_step, mesh=mesh, in_specs=(seq_spec, seq_spec, P('dp', 'sp'), vec_rep, mat_rep, mat_rep, mat_rep, mat_rep, vec_rep, vec_rep), out_specs=(seq_spec, seq_spec, vec_spec, row_spec, row_spec, row_spec, row_spec, vec_spec, vec_spec), check_vma=False)
```
